32 devices in a mesh: data: 4 (over y, z), dap: 8 (over x, core).
Axes of the slice: x: 4, y: 2, z: 2, core: 2. Of those that a mesh axis runs over, the one named last changes fastest.
The devices are a block of a 4x4x8 slice.
Arguments:
- pair_act: float32 [1024, 256, 128], P(('data', 'dap')), parts along dimension 0
- pair_mask: int32 [1024, 256], P(('data', 'dap')), parts along dimension 0
- msa_act: bfloat16 [512, 1024, 256], P(None, ('data', 'dap')), parts along dimension 1
- opm_norm: float32 [2, 256], replicated
- opm_proj: bfloat16 [256, 64], replicated
- opm_out: bfloat16 [1024, 128], replicated
- opm_bias: float32 [128], replicated
- tri_norm: float32 [2, 2, 128], replicated
- tri_proj: bfloat16 [2, 128, 512], replicated
- tri_gate: bfloat16 [2, 128, 128], replicated
- tri_xnorm: float32 [2, 2, 128], replicated
- tri_out: bfloat16 [2, 128, 128], replicated
Outputs:
- output: float32 [1024, 256, 128], P(('data', 'dap')), parts along dimension 0
There are 4 independent parts. The reference program is written for one: setup_inputs(seed, part) draws one part's arguments, and reference() takes and returns one part's arrays. A program takes and returns all parts, laid end to end along the dimension named above; an argument that names none is the same for every part.
All inputs are finite; a program needn't handle non-finite values.
Results may differ from the reference program's by a relative error of at most 0.00337041.
Values are sent between devices in bfloat16 or wider.
A program may use at most 768 MiB of HBM per device.

```python
import jax
import jax.numpy as jnp
from jax import lax

RESIDUES = 256
PAIR_DIM = 128
TRI_DIM = 128
MSA_DIM = 256
OPM_DIM = 32
MSA_DEPTH = 512
ROW_BLOCK = 32
NUM_BLOCKS = RESIDUES // ROW_BLOCK
LN_EPS = 1e-5


def layer_norm(values, norm_scale, norm_shift):
    row_mean = jnp.mean(values, axis=-1, keepdims=True)
    centered = values - row_mean
    row_var = jnp.mean(centered * centered, axis=-1, keepdims=True)
    return (centered * lax.rsqrt(row_var + LN_EPS) * norm_scale + norm_shift).astype(jnp.bfloat16)


def outer_product_mean(msa_act, opm_norm, opm_proj, opm_out, opm_bias):
    msa_norm = layer_norm(msa_act.astype(jnp.float32), opm_norm[0], opm_norm[1])
    proj_all = jnp.dot(msa_norm.reshape(MSA_DEPTH * RESIDUES, MSA_DIM), opm_proj, preferred_element_type=jnp.float32)
    proj_all = proj_all.astype(jnp.bfloat16).reshape(MSA_DEPTH, RESIDUES, 2 * OPM_DIM)
    left_proj = proj_all[:, :, :OPM_DIM].astype(jnp.float32)
    right_proj = proj_all[:, :, OPM_DIM:].astype(jnp.float32)
    left_blocks = jnp.moveaxis(left_proj.reshape(MSA_DEPTH, NUM_BLOCKS, ROW_BLOCK, OPM_DIM), 1, 0)

    def block_update(left_blk):
        outer_prod = jnp.einsum("sip,sjq->ijpq", left_blk, right_proj) / MSA_DEPTH
        outer_flat = outer_prod.astype(jnp.bfloat16).reshape(ROW_BLOCK * RESIDUES, OPM_DIM * OPM_DIM)
        return jnp.dot(outer_flat, opm_out, preferred_element_type=jnp.float32).reshape(ROW_BLOCK, RESIDUES, PAIR_DIM)

    opm_update = lax.map(block_update, left_blocks).reshape(RESIDUES, RESIDUES, PAIR_DIM)
    return opm_update + opm_bias


def triangle_update(pair_act, mask_f, norm_pair, w_proj, w_gate, norm_mix, w_out, incoming):
    pair_blocks = pair_act.reshape(NUM_BLOCKS, ROW_BLOCK, RESIDUES, PAIR_DIM)
    mask_blocks = mask_f.reshape(NUM_BLOCKS, ROW_BLOCK, RESIDUES, 1)

    def project(blk_args):
        pair_blk, mask_blk = blk_args
        pair_norm = layer_norm(pair_blk, norm_pair[0], norm_pair[1])
        proj_all = jnp.dot(pair_norm.reshape(ROW_BLOCK * RESIDUES, PAIR_DIM), w_proj, preferred_element_type=jnp.float32)
        proj_all = proj_all.reshape(ROW_BLOCK, RESIDUES, 4 * TRI_DIM)
        left_act = mask_blk * jax.nn.sigmoid(proj_all[:, :, TRI_DIM:2 * TRI_DIM]) * proj_all[:, :, :TRI_DIM]
        right_act = mask_blk * jax.nn.sigmoid(proj_all[:, :, 3 * TRI_DIM:]) * proj_all[:, :, 2 * TRI_DIM:3 * TRI_DIM]
        return left_act.astype(jnp.bfloat16), right_act.astype(jnp.bfloat16)

    left_all, right_all = lax.map(project, (pair_blocks, mask_blocks))
    left_all = left_all.reshape(RESIDUES, RESIDUES, TRI_DIM)
    right_all = right_all.reshape(RESIDUES, RESIDUES, TRI_DIM)
    if incoming:
        left_all = jnp.swapaxes(left_all, 0, 1)
        right_all = jnp.swapaxes(right_all, 0, 1)
    right_wide = right_all.astype(jnp.float32)
    left_blocks = left_all.reshape(NUM_BLOCKS, ROW_BLOCK, RESIDUES, TRI_DIM)

    def combine(blk_args):
        pair_blk, left_blk = blk_args
        mixed_act = jnp.einsum("ikc,jkc->ijc", left_blk.astype(jnp.float32), right_wide).astype(jnp.bfloat16)
        mixed_norm = layer_norm(mixed_act.astype(jnp.float32), norm_mix[0], norm_mix[1])
        update = jnp.dot(mixed_norm.reshape(ROW_BLOCK * RESIDUES, TRI_DIM), w_out, preferred_element_type=jnp.float32)
        pair_norm = layer_norm(pair_blk, norm_pair[0], norm_pair[1])
        gate_act = jax.nn.sigmoid(jnp.dot(pair_norm.reshape(ROW_BLOCK * RESIDUES, PAIR_DIM), w_gate, preferred_element_type=jnp.float32))
        return pair_blk + (gate_act * update).reshape(ROW_BLOCK, RESIDUES, PAIR_DIM)

    return lax.map(combine, (pair_blocks, left_blocks)).reshape(RESIDUES, RESIDUES, PAIR_DIM)


def setup_inputs(seed: int = 0, part: int = 0) -> dict:
    part_keys = jax.random.split(jax.random.fold_in(jax.random.key(seed), part), 5)
    shared_keys = jax.random.split(jax.random.key(seed + 1), 12)

    def scaled_normal(key_w, shape_w, fan_in):
        return (jax.random.normal(key_w, shape_w, jnp.float32) * fan_in ** -0.5).astype(jnp.bfloat16)

    pair_act = jax.random.normal(part_keys[0], (RESIDUES, RESIDUES, PAIR_DIM), jnp.float32)
    valid_len = jax.random.randint(part_keys[1], (), RESIDUES - RESIDUES // 8, RESIDUES - RESIDUES // 32 + 1)
    positions = jnp.arange(RESIDUES)
    in_range = positions < valid_len
    kept_entries = jax.random.randint(part_keys[2], (RESIDUES, RESIDUES), 0, 32) != 0
    pair_mask = (in_range[:, None] & in_range[None, :] & kept_entries).astype(jnp.int32)
    profile = jax.random.normal(part_keys[3], (RESIDUES, MSA_DIM), jnp.float32)
    msa_noise = jax.random.normal(part_keys[4], (MSA_DEPTH, RESIDUES, MSA_DIM), jnp.float32)
    msa_act = (profile[None] + 0.75 * msa_noise).astype(jnp.bfloat16)
    opm_norm = jnp.stack([1.0 + 0.3 * jax.random.normal(shared_keys[0], (MSA_DIM,), jnp.float32), 0.3 * jax.random.normal(shared_keys[1], (MSA_DIM,), jnp.float32)])
    opm_proj = scaled_normal(shared_keys[2], (MSA_DIM, 2 * OPM_DIM), MSA_DIM)
    opm_out = scaled_normal(shared_keys[3], (OPM_DIM * OPM_DIM, PAIR_DIM), OPM_DIM * OPM_DIM)
    opm_bias = 0.5 * jax.random.normal(shared_keys[4], (PAIR_DIM,), jnp.float32)
    tri_norm = jnp.concatenate([1.0 + 0.3 * jax.random.normal(shared_keys[5], (2, 1, PAIR_DIM), jnp.float32), 0.3 * jax.random.normal(shared_keys[6], (2, 1, PAIR_DIM), jnp.float32)], axis=1)
    tri_proj = scaled_normal(shared_keys[7], (2, PAIR_DIM, 4 * TRI_DIM), PAIR_DIM)
    tri_gate = scaled_normal(shared_keys[8], (2, PAIR_DIM, PAIR_DIM), PAIR_DIM)
    tri_xnorm = jnp.concatenate([1.0 + 0.3 * jax.random.normal(shared_keys[9], (2, 1, TRI_DIM), jnp.float32), 0.3 * jax.random.normal(shared_keys[10], (2, 1, TRI_DIM), jnp.float32)], axis=1)
    tri_out = scaled_normal(shared_keys[11], (2, TRI_DIM, PAIR_DIM), TRI_DIM)
    return {"pair_act": pair_act, "pair_mask": pair_mask, "msa_act": msa_act, "opm_norm": opm_norm, "opm_proj": opm_proj, "opm_out": opm_out, "opm_bias": opm_bias, "tri_norm": tri_norm, "tri_proj": tri_proj, "tri_gate": tri_gate, "tri_xnorm": tri_xnorm, "tri_out": tri_out}


def reference(pair_act, pair_mask, msa_act, opm_norm, opm_proj, opm_out, opm_bias, tri_norm, tri_proj, tri_gate, tri_xnorm, tri_out):
    mask_f = pair_mask.astype(jnp.float32)
    pair_zero = pair_act + outer_product_mean(msa_act, opm_norm, opm_proj, opm_out, opm_bias)
    pair_one = triangle_update(pair_zero, mask_f, tri_norm[0], tri_proj[0], tri_gate[0], tri_xnorm[0], tri_out[0], False)
    return triangle_update(pair_one, mask_f, tri_norm[1], tri_proj[1], tri_gate[1], tri_xnorm[1], tri_out[1], True)
```

```python
import functools

import jax
import jax.numpy as jnp
from jax import lax
from jax.experimental import pallas as pl
from jax.experimental.pallas import tpu as pltpu
from jax.sharding import PartitionSpec as P

LN_EPS = 1e-5
LANES = 128
MESH = pl.DeviceIdType.MESH


def norm_over(values, norm_scale, norm_shift, norm_axis):
    chan_mean = jnp.mean(values, axis=norm_axis, keepdims=True)
    centered = values - chan_mean
    chan_var = jnp.mean(centered * centered, axis=norm_axis, keepdims=True)
    return (centered * lax.rsqrt(chan_var + LN_EPS) * norm_scale + norm_shift).astype(jnp.bfloat16)


def outer_product_mean(value_a7, opm_norm, opm_proj, opm_out, opm_bias):
    value_a9 = value_a7.shape[0]
    opm_dim = opm_proj.shape[1] // 2
    value_a8 = norm_over(value_a7.astype(jnp.float32), opm_norm[0], opm_norm[1], -1)
    proj_all = jnp.einsum("srm,mp->srp", value_a8, opm_proj, preferred_element_type=jnp.float32).astype(jnp.bfloat16)
    right_full = lax.all_gather(proj_all[:, :, opm_dim:], "dap", axis=1, tiled=True)
    outer_prod = jnp.einsum("sip,sjq->ijpq", proj_all[:, :, :opm_dim], right_full, preferred_element_type=jnp.float32) / value_a9
    local_rows = outer_prod.shape[0]
    residues = outer_prod.shape[1]
    outer_flat = outer_prod.astype(jnp.bfloat16).reshape(local_rows, residues, opm_dim * opm_dim)
    return jnp.einsum("ijf,fz->ijz", outer_flat, opm_out, preferred_element_type=jnp.float32) + opm_bias


def _col(v, n):
    return jnp.broadcast_to(v.astype(jnp.float32)[:, None], (v.shape[0], n))


def _norm_rows(v, scale, shift):
    mean = jnp.mean(v, axis=0, keepdims=True)
    cen = v - mean
    var = jnp.mean(cen * cen, axis=0, keepdims=True)
    return (cen * lax.rsqrt(var + LN_EPS) * scale + shift).astype(jnp.bfloat16)


def _entry_barrier(me, n):
    barrier = pltpu.get_barrier_semaphore()
    for s in range(1, n):
        pl.semaphore_signal(barrier, inc=1, device_id={"dap": lax.rem(me + s, n)}, device_id_type=MESH)
    pl.semaphore_wait(barrier, n - 1)


def _tri_kernel(n, incoming, z_hbm, mask_ref, w_ref, wout_ref, nrm_ref, o_hbm,
                zb, gb, st, snd, ra, rb, xs, xr, tb, ob, zsem, osem, ss_ab, rs_ab, ss_x, rs_x):
    me = lax.axis_index("dap")
    rows, chan, cols = zb.shape
    ch_rows = snd.shape[3]
    chunks = rows // ch_rows
    cown = chan // n
    halves = cols // LANES
    pst = st.shape[2] // ch_rows
    pxt = tb.shape[1] // chan
    slot = ch_rows

    def zcopy(ch):
        at = pl.ds(ch * ch_rows, ch_rows)
        return pltpu.make_async_copy(z_hbm.at[at], zb.at[at], zsem.at[ch])

    def ab_copy(t, ch, src, dst):
        buf = rb if t else ra
        return pltpu.make_async_remote_copy(
            src_ref=snd.at[t, ch, pl.ds(pl.multiple_of(dst * cown, cown), cown)],
            dst_ref=buf.at[src, :, pl.ds(ch * slot, slot)],
            send_sem=ss_ab.at[t, ch, dst], recv_sem=rs_ab.at[t, ch, src],
            device_id={"dap": dst}, device_id_type=MESH)

    def x_copy(ch, src, dst):
        return pltpu.make_async_remote_copy(
            src_ref=xs.at[ch, dst], dst_ref=xr.at[ch, pl.ds(pl.multiple_of(src * cown, cown), cown)],
            send_sem=ss_x.at[ch, dst], recv_sem=rs_x.at[ch, src],
            device_id={"dap": dst}, device_id_type=MESH)

    for ch in range(chunks):
        zcopy(ch).start()
    _entry_barrier(me, n)

    scale, shift = nrm_ref[0], nrm_ref[1]
    xscale, xshift = nrm_ref[2], nrm_ref[3]

    for ch in range(chunks):
        zcopy(ch).wait()

        @pl.loop(0, ch_rows)
        def _(i, ch=ch):
            r = ch * ch_rows + i
            y = _norm_rows(zb[r], scale, shift)
            q = jnp.dot(w_ref[...], y, preferred_element_type=jnp.float32)
            m = mask_ref[pl.ds(r, 1), :]
            a = m * jax.nn.sigmoid(q[chan:2 * chan]) * q[:chan]
            b = m * jax.nn.sigmoid(q[3 * chan:4 * chan]) * q[2 * chan:3 * chan]
            gb[r] = jax.nn.sigmoid(q[4 * chan:])
            at = pl.ds(pl.multiple_of(i * pst, 8), chan)
            for h in range(halves):
                st[0, h, at, :] = a[:, h * LANES:(h + 1) * LANES]
                st[1, h, at, :] = b[:, h * LANES:(h + 1) * LANES]

        @pl.loop(0, chan, unroll=8)
        def _(c, ch=ch):
            for t in range(2):
                for h in range(halves):
                    snd[t, ch, c, :, h * LANES:(h + 1) * LANES] = st[t, h, pl.ds(c, ch_rows, stride=pst), :].astype(jnp.bfloat16)

        own = pl.ds(pl.multiple_of(me * cown, cown), cown)
        if incoming:
            order = ((1, ch), (0, ch))
        else:
            order = ((1, ch),) if ch < chunks - 1 else ((1, ch),) + tuple((0, k) for k in range(chunks))
        for t, k in order:
            for s in range(1, n):
                ab_copy(t, k, me, lax.rem(me + s, n)).start()
        ra[me, :, ch * slot:(ch + 1) * slot] = snd[0, ch, own]
        rb[me, :, ch * slot:(ch + 1) * slot] = snd[1, ch, own]

    def wait_ab(t, ch):
        for s in range(1, n):
            ab_copy(t, ch, lax.rem(me + s, n), me).wait_recv()

    def send_x(ch):
        for s in range(1, n):
            x_copy(ch, me, lax.rem(me + s, n)).start()
        xr[ch, pl.ds(pl.multiple_of(me * cown, cown), cown)] = xs[ch, me]

    for ch in range(chunks):
        wait_ab(1, ch)
    if incoming:
        for ch in range(chunks):
            wait_ab(0, ch)

        @pl.loop(0, cown)
        def _(c):
            x = lax.dot_general(ra[:, c].reshape(n * rows, cols), rb[:, c].reshape(n * rows, cols),
                                (((0,), (0,)), ((), ())), preferred_element_type=jnp.float32)
            x = x.astype(jnp.bfloat16).reshape(n, chunks, ch_rows, cols)
            for ch in range(chunks):
                xs[ch, :, c] = x[:, ch]
        for ch in range(chunks):
            send_x(ch)
    else:
        for ch in range(chunks):
            wait_ab(0, ch)

            @pl.loop(0, cown)
            def _(c, ch=ch):
                x = lax.dot_general(ra[:, c, ch * slot:(ch + 1) * slot].reshape(n * ch_rows, cols),
                                    rb[:, c].reshape(n * rows, cols),
                                    (((1,), (1,)), ((), ())), preferred_element_type=jnp.float32)
                xs[ch, :, c] = x.astype(jnp.bfloat16).reshape(n, ch_rows, cols)
            send_x(ch)

    for ch in range(chunks):
        for s in range(1, n):
            x_copy(ch, lax.rem(me + s, n), me).wait_recv()

        @pl.loop(0, chan, unroll=8)
        def _(c, ch=ch):
            at = pl.ds(pl.multiple_of(c * pxt, 8), ch_rows)
            for h in range(halves):
                tb[h, at, :] = xr[ch, c, :, h * LANES:(h + 1) * LANES].astype(jnp.float32)

        @pl.loop(0, ch_rows)
        def _(i, ch=ch):
            r = ch * ch_rows + i
            x = jnp.concatenate([tb[h, pl.ds(i, chan, stride=pxt), :] for h in range(halves)], axis=1)
            xn = _norm_rows(x, xscale, xshift)
            upd = jnp.dot(wout_ref[...], xn, preferred_element_type=jnp.float32)
            ob[r] = zb[r] + gb[r] * upd
        at = pl.ds(ch * ch_rows, ch_rows)
        pltpu.make_async_copy(ob.at[at], o_hbm.at[at], osem.at[ch]).start()

    for ch in range(chunks):
        at = pl.ds(ch * ch_rows, ch_rows)
        pltpu.make_async_copy(ob.at[at], o_hbm.at[at], osem.at[ch]).wait()
        for s in range(1, n):
            dst = lax.rem(me + s, n)
            ab_copy(0, ch, me, dst).wait_send()
            ab_copy(1, ch, me, dst).wait_send()
            x_copy(ch, me, dst).wait_send()


def _tri_call(n, incoming, z_cm, mask_f, w_proj, w_gate, norm_pair, norm_mix, w_out):
    rows, chan, cols = z_cm.shape
    cown = chan // n
    chunks = 2
    ch_rows = rows // chunks
    halves = cols // LANES
    w_all = jnp.concatenate([w_proj, w_gate], axis=1).T
    nrm = jnp.stack([_col(norm_pair[0], cols), _col(norm_pair[1], cols), _col(norm_mix[0], cols), _col(norm_mix[1], cols)])
    vm = pl.BlockSpec(memory_space=pltpu.VMEM)
    hbm = pl.BlockSpec(memory_space=pl.ANY)
    return pl.pallas_call(
        functools.partial(_tri_kernel, n, incoming),
        out_shape=jax.ShapeDtypeStruct(z_cm.shape, jnp.float32),
        in_specs=[hbm, vm, vm, vm, vm],
        out_specs=hbm,
        scratch_shapes=[
            pltpu.VMEM((rows, chan, cols), jnp.float32),
            pltpu.VMEM((rows, chan, cols), jnp.float32),
            pltpu.VMEM((2, halves, ch_rows * (chan + 8), LANES), jnp.float32),
            pltpu.VMEM((2, chunks, chan, ch_rows, cols), jnp.bfloat16),
            pltpu.VMEM((n, cown, rows, cols), jnp.bfloat16),
            pltpu.VMEM((n, cown, rows, cols), jnp.bfloat16),
            pltpu.VMEM((chunks, n, cown, ch_rows, cols), jnp.bfloat16),
            pltpu.VMEM((chunks, chan, ch_rows, cols), jnp.bfloat16),
            pltpu.VMEM((halves, chan * (ch_rows + 8), LANES), jnp.float32),
            pltpu.VMEM((rows, chan, cols), jnp.float32),
            pltpu.SemaphoreType.DMA((chunks,)),
            pltpu.SemaphoreType.DMA((chunks,)),
            pltpu.SemaphoreType.DMA((2, chunks, n)),
            pltpu.SemaphoreType.DMA((2, chunks, n)),
            pltpu.SemaphoreType.DMA((chunks, n)),
            pltpu.SemaphoreType.DMA((chunks, n)),
        ],
        compiler_params=pltpu.CompilerParams(collective_id=2 if incoming else 1, has_side_effects=True, vmem_limit_bytes=60 * 1024 * 1024),
        name="tri_in" if incoming else "tri_out",
    )(z_cm, mask_f, w_all, w_out.T, nrm)


def solution(mesh):
    row_spec = P(("data", "dap"), None, None)
    mask_spec = P(("data", "dap"), None)
    array_b8 = P(None, ("data", "dap"), None)
    replicated = P()

    def local_program(pair_loc, mask_loc, value_a7, opm_norm, opm_proj, opm_out, opm_bias, tri_norm, tri_proj, tri_gate, tri_xnorm, tri_out):
        n = lax.axis_size("dap")
        mask_f = mask_loc.astype(jnp.float32)
        pair_zero = pair_loc + outer_product_mean(value_a7, opm_norm, opm_proj, opm_out, opm_bias)
        z = jnp.swapaxes(pair_zero, 1, 2)
        for t in range(2):
            z = _tri_call(n, t == 1, z, mask_f, tri_proj[t], tri_gate[t], tri_norm[t], tri_xnorm[t], tri_out[t])
        return jnp.swapaxes(z, 1, 2)

    return jax.shard_map(local_program, mesh=mesh, in_specs=(row_spec, mask_spec, array_b8) + (replicated,) * 9, out_specs=row_spec, check_vma=False)
```

```python
import functools

import jax
import jax.numpy as jnp
from jax import lax
from jax.experimental import pallas as pl
from jax.experimental.pallas import tpu as pltpu
from jax.sharding import PartitionSpec as P

LN_EPS = 1e-5
LANES = 128
MESH = pl.DeviceIdType.MESH


def _col(v, n):
    return jnp.broadcast_to(v.astype(jnp.float32)[:, None], (v.shape[0], n))


def _norm_rows(v, scale, shift):
    mean = jnp.mean(v, axis=0, keepdims=True)
    cen = v - mean
    var = jnp.mean(cen * cen, axis=0, keepdims=True)
    return (cen * lax.rsqrt(var + LN_EPS) * scale + shift).astype(jnp.bfloat16)


def _entry_barrier(me, n):
    barrier = pltpu.get_barrier_semaphore()
    for s in range(1, n):
        pl.semaphore_signal(barrier, inc=1, device_id={"dap": lax.rem(me + s, n)}, device_id_type=MESH)
    pl.semaphore_wait(barrier, n - 1)


def _tri_kernel(n, incoming, z_hbm, mask_ref, w_ref, wout_ref, nrm_ref, o_hbm,
                zb, gb, st, snd, ra, rb, xs, xr, tb, ob, zsem, osem, ss_ab, rs_ab, ss_x, rs_x):
    me = lax.axis_index("dap")
    rows, chan, cols = zb.shape
    ch_rows = snd.shape[3]
    chunks = rows // ch_rows
    cown = chan // n
    halves = cols // LANES
    pst = st.shape[2] // ch_rows
    pxt = tb.shape[1] // chan

    def zcopy(ch):
        at = pl.ds(ch * ch_rows, ch_rows)
        return pltpu.make_async_copy(z_hbm.at[at], zb.at[at], zsem.at[ch])

    def ab_copy(t, ch, src, dst):
        buf = rb if t else ra
        return pltpu.make_async_remote_copy(
            src_ref=snd.at[t, ch, pl.ds(pl.multiple_of(dst * cown, cown), cown)],
            dst_ref=buf.at[ch, src],
            send_sem=ss_ab.at[t, ch, dst], recv_sem=rs_ab.at[t, ch, src],
            device_id={"dap": dst}, device_id_type=MESH)

    def x_copy(ch, src, dst):
        return pltpu.make_async_remote_copy(
            src_ref=xs.at[ch, dst], dst_ref=xr.at[ch, pl.ds(pl.multiple_of(src * cown, cown), cown)],
            send_sem=ss_x.at[ch, dst], recv_sem=rs_x.at[ch, src],
            device_id={"dap": dst}, device_id_type=MESH)

    for ch in range(chunks):
        zcopy(ch).start()
    _entry_barrier(me, n)

    scale, shift = nrm_ref[0], nrm_ref[1]
    xscale, xshift = nrm_ref[2], nrm_ref[3]

    for ch in range(chunks):
        zcopy(ch).wait()

        @pl.loop(0, ch_rows)
        def _(i, ch=ch):
            r = ch * ch_rows + i
            y = _norm_rows(zb[r], scale, shift)
            q = jnp.dot(w_ref[...], y, preferred_element_type=jnp.float32)
            m = mask_ref[pl.ds(r, 1), :]
            a = m * jax.nn.sigmoid(q[chan:2 * chan]) * q[:chan]
            b = m * jax.nn.sigmoid(q[3 * chan:4 * chan]) * q[2 * chan:3 * chan]
            gb[r] = jax.nn.sigmoid(q[4 * chan:])
            at = pl.ds(pl.multiple_of(i * pst, 8), chan)
            for h in range(halves):
                st[0, h, at, :] = a[:, h * LANES:(h + 1) * LANES]
                st[1, h, at, :] = b[:, h * LANES:(h + 1) * LANES]

        @pl.loop(0, chan, unroll=8)
        def _(c, ch=ch):
            for t in range(2):
                for h in range(halves):
                    snd[t, ch, c, :, h * LANES:(h + 1) * LANES] = st[t, h, pl.ds(c, ch_rows, stride=pst), :].astype(jnp.bfloat16)

        own = pl.ds(pl.multiple_of(me * cown, cown), cown)
        if incoming:
            order = ((1, ch), (0, ch))
        else:
            order = ((1, ch),) if ch < chunks - 1 else ((1, ch),) + tuple((0, k) for k in range(chunks))
        for t, k in order:
            for s in range(1, n):
                ab_copy(t, k, me, lax.rem(me + s, n)).start()
        ra[ch, me] = snd[0, ch, own]
        rb[ch, me] = snd[1, ch, own]

    def wait_ab(t, ch):
        for s in range(1, n):
            ab_copy(t, ch, lax.rem(me + s, n), me).wait_recv()

    def send_x(ch):
        for s in range(1, n):
            x_copy(ch, me, lax.rem(me + s, n)).start()
        xr[ch, pl.ds(pl.multiple_of(me * cown, cown), cown)] = xs[ch, me]

    for ch in range(chunks):
        wait_ab(1, ch)
    if incoming:
        for ch in range(chunks):
            wait_ab(0, ch)

        @pl.loop(0, cown)
        def _(c):
            x = lax.dot_general(ra[:, :, c].reshape(n * rows, cols), rb[:, :, c].reshape(n * rows, cols),
                                (((0,), (0,)), ((), ())), preferred_element_type=jnp.float32)
            x = x.astype(jnp.bfloat16).reshape(chunks, n, ch_rows, cols)
            for ch in range(chunks):
                xs[ch, :, c] = x[ch]
        for ch in range(chunks):
            send_x(ch)
    else:
        for ch in range(chunks):
            wait_ab(0, ch)

            @pl.loop(0, cown)
            def _(c, ch=ch):
                x = lax.dot_general(ra[ch, :, c].reshape(n * ch_rows, cols),
                                    rb[:, :, c].reshape(n * rows, cols),
                                    (((1,), (1,)), ((), ())), preferred_element_type=jnp.float32)
                xs[ch, :, c] = x.astype(jnp.bfloat16).reshape(n, ch_rows, cols)
            send_x(ch)

    for ch in range(chunks):
        for s in range(1, n):
            x_copy(ch, lax.rem(me + s, n), me).wait_recv()

        @pl.loop(0, chan, unroll=8)
        def _(c, ch=ch):
            at = pl.ds(pl.multiple_of(c * pxt, 8), ch_rows)
            for h in range(halves):
                tb[h, at, :] = xr[ch, c, :, h * LANES:(h + 1) * LANES].astype(jnp.float32)

        @pl.loop(0, ch_rows)
        def _(i, ch=ch):
            r = ch * ch_rows + i
            x = jnp.concatenate([tb[h, pl.ds(i, chan, stride=pxt), :] for h in range(halves)], axis=1)
            xn = _norm_rows(x, xscale, xshift)
            upd = jnp.dot(wout_ref[...], xn, preferred_element_type=jnp.float32)
            new = zb[r] + gb[r] * upd
            if incoming:
                ob[r] = new.T.reshape(chunks, n, cols // (chunks * n), chan).swapaxes(0, 1).reshape(cols, chan)
            else:
                ob[r] = new
        at = pl.ds(ch * ch_rows, ch_rows)
        pltpu.make_async_copy(ob.at[at], o_hbm.at[at], osem.at[ch]).start()

    for ch in range(chunks):
        at = pl.ds(ch * ch_rows, ch_rows)
        pltpu.make_async_copy(ob.at[at], o_hbm.at[at], osem.at[ch]).wait()
        for s in range(1, n):
            dst = lax.rem(me + s, n)
            ab_copy(0, ch, me, dst).wait_send()
            ab_copy(1, ch, me, dst).wait_send()
            x_copy(ch, me, dst).wait_send()


def _tri_call(n, incoming, z_cm, mask_f, w_proj, w_gate, norm_pair, norm_mix, w_out):
    rows, chan, cols = z_cm.shape
    cown = chan // n
    chunks = 2
    ch_rows = rows // chunks
    halves = cols // LANES
    out_block = (rows, cols, chan) if incoming else z_cm.shape
    w_all = jnp.concatenate([w_proj, w_gate], axis=1).T
    nrm = jnp.stack([_col(norm_pair[0], cols), _col(norm_pair[1], cols), _col(norm_mix[0], cols), _col(norm_mix[1], cols)])
    vm = pl.BlockSpec(memory_space=pltpu.VMEM)
    hbm = pl.BlockSpec(memory_space=pl.ANY)
    return pl.pallas_call(
        functools.partial(_tri_kernel, n, incoming),
        out_shape=jax.ShapeDtypeStruct(out_block, jnp.float32),
        in_specs=[hbm, vm, vm, vm, vm],
        out_specs=hbm,
        scratch_shapes=[
            pltpu.VMEM((rows, chan, cols), jnp.float32),
            pltpu.VMEM((rows, chan, cols), jnp.float32),
            pltpu.VMEM((2, halves, ch_rows * (chan + 8), LANES), jnp.float32),
            pltpu.VMEM((2, chunks, chan, ch_rows, cols), jnp.bfloat16),
            pltpu.VMEM((chunks, n, cown, ch_rows, cols), jnp.bfloat16),
            pltpu.VMEM((chunks, n, cown, ch_rows, cols), jnp.bfloat16),
            pltpu.VMEM((chunks, n, cown, ch_rows, cols), jnp.bfloat16),
            pltpu.VMEM((chunks, chan, ch_rows, cols), jnp.bfloat16),
            pltpu.VMEM((halves, chan * (ch_rows + 8), LANES), jnp.float32),
            pltpu.VMEM(out_block, jnp.float32),
            pltpu.SemaphoreType.DMA((chunks,)),
            pltpu.SemaphoreType.DMA((chunks,)),
            pltpu.SemaphoreType.DMA((2, chunks, n)),
            pltpu.SemaphoreType.DMA((2, chunks, n)),
            pltpu.SemaphoreType.DMA((chunks, n)),
            pltpu.SemaphoreType.DMA((chunks, n)),
        ],
        compiler_params=pltpu.CompilerParams(collective_id=2 if incoming else 1, has_side_effects=True, vmem_limit_bytes=60 * 1024 * 1024),
        name="tri_in" if incoming else "tri_out",
    )(z_cm, mask_f, w_all, w_out.T, nrm)


def _opm_kernel(n, z_hbm, msa_hbm, nrm_ref, proj_ref, wt_ref, bias_ref, o_hbm,
                mb, ub, at_b, bt, ball, obuf, zi, zo, msem, zsem, osem, ss, rs):
    me = lax.axis_index("dap")
    depth, grp, mdim = mb.shape[1:]
    rows = zi.shape[0]
    groups = rows // grp
    chunks, odim, lanes = ball.shape[:3]
    jrows = lanes // n
    per = jrows // grp
    qh = odim // 2
    pst = bt.shape[1] // jrows
    tiles = depth // LANES
    part = me + 1 - 2 * lax.rem(me, 2)
    right, left, opp = lax.rem(me + 2, n), lax.rem(me + n - 2, n), lax.rem(me + 4, n)

    def mcopy(g):
        return pltpu.make_async_copy(msa_hbm.at[:, pl.ds(g * grp, grp)], mb.at[g % 2], msem.at[g % 2])

    def block(c, h, src):
        return ball.at[c, h * qh:(h + 1) * qh, pl.ds(pl.multiple_of(src * jrows, jrows), jrows)]

    def send(c, h, src, k, dst):
        return pltpu.make_async_remote_copy(
            src_ref=block(c, h, src), dst_ref=block(c, h, src), send_sem=ss.at[c, h, k], recv_sem=rs.at[c, h, src],
            device_id={"dap": dst}, device_id_type=MESH)

    def arrived(c, h, src):
        send(c, h, src, 0, part).wait_recv()

    mcopy(0).start()
    mcopy(1).start()
    zcopy = pltpu.make_async_copy(z_hbm, zi, zsem.at[0])
    zcopy.start()
    _entry_barrier(me, n)

    scale, shift = nrm_ref[0:1, :], nrm_ref[1:2, :]
    sb = 32

    def project(c):
        for k in range(per):
            g = c * per + k
            mcopy(g).wait()

            @pl.loop(0, depth // sb)
            def _(b, g=g):
                x = mb[g % 2, pl.ds(b * sb, sb)].astype(jnp.float32).reshape(sb * grp, mdim)
                mean = jnp.mean(x, axis=1, keepdims=True)
                cen = x - mean
                var = jnp.mean(cen * cen, axis=1, keepdims=True)
                y = (cen * lax.rsqrt(var + LN_EPS) * scale + shift).astype(jnp.bfloat16)
                ub[pl.ds(pl.multiple_of(b * (sb * grp), sb * grp), sb * grp), :] = jnp.dot(y, proj_ref[...], preferred_element_type=jnp.float32)
            if g + 2 < groups:
                mcopy(g + 2).start()

            @pl.loop(0, grp)
            def _(i, g=g, k=k):
                v = ub[pl.ds(i, depth, stride=grp), :].T
                r = g * grp + i
                at_b[pl.ds(pl.multiple_of(r * odim, odim), odim), :] = v[:odim].astype(jnp.bfloat16)
                row = pl.multiple_of((k * grp + i) * pst, 8)
                for t in range(tiles):
                    bt[t, pl.ds(row, odim), :] = v[odim:2 * odim, t * LANES:(t + 1) * LANES]

        @pl.loop(0, odim, unroll=4)
        def _(q):
            for t in range(tiles):
                ball[c, q, pl.ds(pl.multiple_of(me * jrows, jrows), jrows), t * LANES:(t + 1) * LANES] = (
                    bt[t, pl.ds(q, jrows, stride=pst), :].astype(jnp.bfloat16))

    def send_own(c):
        for h in (0, 1):
            send(c, h, me, 0, right).start()
            send(c, 1 - h, me, 1, left).start()
        for h in (0, 1):
            send(c, h, me, 2, part).start()

    def forward_far(c):
        arrived(c, 0, left)
        send(c, 0, left, 3, right).start()
        send(c, 0, left, 4, part).start()
        arrived(c, 1, right)
        send(c, 1, right, 3, left).start()
        send(c, 1, right, 4, part).start()

    def forward_near(c):
        arrived(c, 1, left)
        send(c, 1, left, 5, part).start()
        arrived(c, 0, right)
        send(c, 0, right, 5, part).start()

    def forward_opp(c):
        for h in (0, 1):
            arrived(c, h, opp)
            send(c, h, opp, 6, part).start()

    def partner_all(c):
        for d in (0, 2, 4, 6):
            src = lax.rem(part + d, n)
            for h in (0, 1):
                arrived(c, h, src)

    def outer(c, lo, hi):
        @pl.loop(lo, hi)
        def _(b):
            rhs = ball[c, pl.ds(b * 2, 2)].reshape(2 * lanes, depth)
            o = lax.dot_general(at_b[...], rhs, (((1,), (1,)), ((), ())), preferred_element_type=jnp.float32)
            o = (o * (1.0 / depth)).astype(jnp.bfloat16)
            for t in range(2):
                obuf[b * 2 + t] = o[:, t * lanes:(t + 1) * lanes]

    def mix(c, lo, hi):
        @pl.loop(lo, hi)
        def _(i):
            rhs = obuf[:, pl.ds(pl.multiple_of(i * odim, odim), odim), :].reshape(odim * odim, lanes)
            upd = jnp.dot(wt_ref[...], rhs, preferred_element_type=jnp.float32)
            zt = zi[i].reshape(n, chunks, jrows, zi.shape[2])[:, c].reshape(lanes, zi.shape[2]).T
            zo[i, :, c * lanes:(c + 1) * lanes] = zt + (upd + bias_ref[...])

    blocks = odim // 2
    project(0)
    send_own(0)
    project(1)
    forward_far(0)
    send_own(1)
    forward_near(0)
    forward_opp(0)
    partner_all(0)
    outer(0, 0, blocks // 2)
    forward_far(1)
    outer(0, blocks // 2, blocks)
    zcopy.wait()
    forward_near(1)
    mix(0, 0, rows)
    forward_opp(1)
    partner_all(1)
    outer(1, 0, blocks)
    half = rows // 2
    for k in range(2):
        mix(1, k * half, (k + 1) * half)
        pltpu.make_async_copy(zo.at[pl.ds(k * half, half)], o_hbm.at[pl.ds(k * half, half)], osem.at[k]).start()
    for k in range(2):
        pltpu.make_async_copy(zo.at[pl.ds(k * half, half)], o_hbm.at[pl.ds(k * half, half)], osem.at[k]).wait()
    for c in range(chunks):
        for h in (0, 1):
            for k, src in ((0, me), (1, me), (2, me), (3, left if h == 0 else right), (4, left if h == 0 else right),
                           (5, right if h == 0 else left), (6, opp)):
                send(c, h, src, k, part).wait_send()


def _opm_call(n, pair_loc, msa, opm_norm, opm_proj, opm_out, opm_bias):
    rows, cols, chan = pair_loc.shape
    depth, _, mdim = msa.shape
    odim = opm_proj.shape[1] // 2
    grp = 8
    chunks = 2
    lanes = cols // chunks
    proj = jnp.pad(opm_proj, ((0, 0), (0, LANES - 2 * odim)))
    wt = opm_out.reshape(odim, odim, chan).transpose(2, 1, 0).reshape(chan, odim * odim)
    vm = pl.BlockSpec(memory_space=pltpu.VMEM)
    hbm = pl.BlockSpec(memory_space=pl.ANY)
    jrows = lanes // n
    return pl.pallas_call(
        functools.partial(_opm_kernel, n),
        out_shape=jax.ShapeDtypeStruct((rows, chan, cols), jnp.float32),
        in_specs=[hbm, hbm, vm, vm, vm, vm],
        out_specs=hbm,
        scratch_shapes=[
            pltpu.VMEM((2, depth, grp, mdim), jnp.bfloat16),
            pltpu.VMEM((depth * grp, LANES), jnp.float32),
            pltpu.VMEM((rows * odim, depth), jnp.bfloat16),
            pltpu.VMEM((depth // LANES, jrows * (odim + 8), LANES), jnp.float32),
            pltpu.VMEM((chunks, odim, lanes, depth), jnp.bfloat16),
            pltpu.VMEM((odim, rows * odim, lanes), jnp.bfloat16),
            pltpu.VMEM((rows, cols, chan), jnp.float32),
            pltpu.VMEM((rows, chan, cols), jnp.float32),
            pltpu.SemaphoreType.DMA((2,)),
            pltpu.SemaphoreType.DMA((1,)),
            pltpu.SemaphoreType.DMA((2,)),
            pltpu.SemaphoreType.DMA((chunks, 2, 7)),
            pltpu.SemaphoreType.DMA((chunks, 2, n)),
        ],
        compiler_params=pltpu.CompilerParams(collective_id=3, has_side_effects=True, vmem_limit_bytes=60 * 1024 * 1024),
        name="opm",
    )(pair_loc, msa, opm_norm, proj, wt, _col(opm_bias, lanes))


def solution(mesh):
    row_spec = P(("data", "dap"), None, None)
    mask_spec = P(("data", "dap"), None)
    array_b8 = P(None, ("data", "dap"), None)
    replicated = P()

    def local_program(pair_loc, mask_loc, value_a7, opm_norm, opm_proj, opm_out, opm_bias, tri_norm, tri_proj, tri_gate, tri_xnorm, tri_out):
        n = lax.axis_size("dap")
        rows, cols = mask_loc.shape
        mask_f = mask_loc.astype(jnp.float32).reshape(rows, n, 2, cols // (2 * n)).swapaxes(1, 2).reshape(rows, cols)
        z = _opm_call(n, pair_loc, value_a7, opm_norm, opm_proj, opm_out, opm_bias)
        for t in range(2):
            z = _tri_call(n, t == 1, z, mask_f, tri_proj[t], tri_gate[t], tri_norm[t], tri_xnorm[t], tri_out[t])
        return z

    return jax.shard_map(local_program, mesh=mesh, in_specs=(row_spec, mask_spec, array_b8) + (replicated,) * 9, out_specs=row_spec, check_vma=False)
```

```python
import functools

import jax
import jax.numpy as jnp
from jax import lax
from jax.experimental import pallas as pl
from jax.experimental.pallas import tpu as pltpu
from jax.sharding import PartitionSpec as P

LN_EPS = 1e-5
LANES = 128
TILE = 16
MESH = pl.DeviceIdType.MESH


def _norm_rows(v, scale, shift):
    mean = jnp.mean(v, axis=0, keepdims=True)
    cen = v - mean
    var = jnp.mean(cen * cen, axis=0, keepdims=True)
    return (cen * lax.rsqrt(var + LN_EPS) * scale + shift).astype(jnp.bfloat16)


def _column(row, n):
    return jnp.broadcast_to(row, (n, row.shape[1])).T


def _kernel(n, z_hbm, mask_ref, msa_hbm, onrm_ref, oproj_ref, oout_ref, obias_ref, nrm_ref, proj_ref, gate_ref, xnrm_ref, out_ref, o_hbm,
            mb, fb, at_b, ball, obuf, zi, zb, gb, st, snd, ra, rb, xs, xr, mk, wt, wa, wo, nc, bc,
            msem, zsem, osem, ss, rs, ss_ab, rs_ab, ss_x, rs_x):
    me = lax.axis_index("dap")
    depth, grp, mdim = mb.shape[1:]
    rows, cols, chan = zi.shape
    chunks, odim, lanes = ball.shape[:3]
    jrows = lanes // n
    groups = rows // grp
    per = jrows // grp
    qh = odim // 2
    cown = chan // n
    blocks = odim // 2
    tiles = depth // LANES
    bst, pst, pxt = odim + 8, chan + 8, jrows + 8
    part = me + 1 - 2 * lax.rem(me, 2)
    right, left, opp = lax.rem(me + 2, n), lax.rem(me + n - 2, n), lax.rem(me + 4, n)

    def mcopy(g):
        return pltpu.make_async_copy(msa_hbm.at[:, pl.ds(g * grp, grp)], mb.at[g % 2], msem.at[g % 2])

    mcopy(0).start()
    mcopy(1).start()
    zcopy = pltpu.make_async_copy(z_hbm, zi, zsem.at[0])
    zcopy.start()
    barrier = pltpu.get_barrier_semaphore()
    for s in range(1, n):
        pl.semaphore_signal(barrier, inc=1, device_id={"dap": lax.rem(me + s, n)}, device_id_type=MESH)
    pl.semaphore_wait(barrier, n - 1)

    def block(c, h, src):
        return ball.at[c, h * qh:(h + 1) * qh, pl.ds(pl.multiple_of(src * jrows, jrows), jrows)]

    def send(c, h, src, k, dst):
        return pltpu.make_async_remote_copy(
            src_ref=block(c, h, src), dst_ref=block(c, h, src), send_sem=ss.at[c, h, k], recv_sem=rs.at[c, h, src],
            device_id={"dap": dst}, device_id_type=MESH)

    def arrived(c, h, src):
        send(c, h, src, 0, part).wait_recv()

    oscale, oshift = onrm_ref[0:1, :], onrm_ref[1:2, :]
    sb = 64

    def project(c):
        for k in range(per):
            g = c * per + k
            mcopy(g).wait()

            @pl.loop(0, depth // sb)
            def _(b, g=g):
                x = mb[g % 2, pl.ds(b * sb, sb)].astype(jnp.float32).reshape(sb * grp, mdim)
                mean = jnp.mean(x, axis=1, keepdims=True)
                cen = x - mean
                var = jnp.mean(cen * cen, axis=1, keepdims=True)
                y = (cen * lax.rsqrt(var + LN_EPS) * oscale + oshift).astype(jnp.bfloat16)
                at = pl.ds(pl.multiple_of(b * (sb * grp), sb * grp), sb * grp)
                fb[at, :2 * odim] = jnp.dot(y, oproj_ref[...], preferred_element_type=jnp.float32)
            if g + 2 < groups:
                mcopy(g + 2).start()

            @pl.loop(0, grp)
            def _(i, g=g, k=k):
                v = fb[pl.ds(i, depth, stride=grp), :].T
                r = g * grp + i
                at_b[pl.ds(pl.multiple_of(r * odim, odim), odim), :] = v[:odim].astype(jnp.bfloat16)
                for t in range(tiles):
                    row = pl.multiple_of(t * (jrows * bst) + (k * grp + i) * bst, 8)
                    st[pl.ds(row, odim), :] = v[odim:2 * odim, t * LANES:(t + 1) * LANES]

        @pl.loop(0, odim, unroll=4)
        def _(q):
            for t in range(tiles):
                ball[c, q, pl.ds(pl.multiple_of(me * jrows, jrows), jrows), t * LANES:(t + 1) * LANES] = (
                    st[pl.ds(t * (jrows * bst) + q, jrows, stride=bst), :].astype(jnp.bfloat16))

    def send_own(c):
        for h in (0, 1):
            send(c, h, me, 0, right).start()
            send(c, 1 - h, me, 1, left).start()
        for h in (0, 1):
            send(c, h, me, 2, part).start()

    def forward_far(c):
        arrived(c, 0, left)
        send(c, 0, left, 3, right).start()
        send(c, 0, left, 4, part).start()
        arrived(c, 1, right)
        send(c, 1, right, 3, left).start()
        send(c, 1, right, 4, part).start()

    def forward_near(c):
        arrived(c, 1, left)
        send(c, 1, left, 5, part).start()
        arrived(c, 0, right)
        send(c, 0, right, 5, part).start()

    def forward_opp(c):
        for h in (0, 1):
            arrived(c, h, opp)
            send(c, h, opp, 6, part).start()

    def partner_all(c):
        for d in (0, 2, 4, 6):
            for h in (0, 1):
                arrived(c, h, lax.rem(part + d, n))

    def outer(c, lo, hi):
        @pl.loop(lo, hi)
        def _(b):
            rhs = ball[c, pl.ds(b * 2, 2)].reshape(2 * lanes, depth)
            o = lax.dot_general(at_b[...], rhs, (((1,), (1,)), ((), ())), preferred_element_type=jnp.float32)
            o = (o * (1.0 / depth)).astype(jnp.bfloat16)
            nt = rows * odim // TILE
            for t in range(2):
                obuf[b, t * nt:(t + 1) * nt] = o[:, t * lanes:(t + 1) * lanes].reshape(nt, TILE, lanes)

    def mix(c):
        @pl.loop(0, rows)
        def _(i):
            nt, w = rows * odim // TILE, odim // TILE
            rhs = jnp.stack([obuf[:, pl.ds(t * nt + i * w, w)] for t in range(2)], axis=1).reshape(odim * odim, lanes)
            upd = jnp.dot(wt[...], rhs, preferred_element_type=jnp.float32)
            zt = zi[i].reshape(n, chunks, jrows, chan)[:, c].reshape(lanes, chan).T
            zb[i, :, c * lanes:(c + 1) * lanes] = zt + (upd + bc[...])

    def prepare():
        rid = lax.broadcasted_iota(jnp.int32, (cols, cols), 0)
        cid = lax.broadcasted_iota(jnp.int32, (cols, cols), 1)
        two = chunks * jrows
        place = ((rid // jrows) % chunks) * lanes + (rid // two) * jrows + rid % jrows
        perm = (cid == place).astype(jnp.float32).astype(jnp.bfloat16)
        mk[...] = jnp.dot(mask_ref[...].astype(jnp.float32).astype(jnp.bfloat16), perm, preferred_element_type=jnp.float32)
        bc[...] = _column(obias_ref[...], lanes)
        for t in range(2):
            for k in range(2):
                nc[t, k] = _column(nrm_ref[t, k:k + 1, :], lanes)
                nc[t, 2 + k] = _column(xnrm_ref[t, k:k + 1, :], lanes)
            for k in range(4):
                wa[t, k * chan:(k + 1) * chan] = proj_ref[t, :, k * chan:(k + 1) * chan].astype(jnp.float32).T.astype(jnp.bfloat16)
            wa[t, 4 * chan:] = gate_ref[t].astype(jnp.float32).T.astype(jnp.bfloat16)
            wo[t] = out_ref[t].astype(jnp.float32).T.astype(jnp.bfloat16)
        fb[:odim * odim, :] = oout_ref[...].astype(jnp.float32)

        @pl.loop(0, odim * odim // LANES)
        def _(b):
            m = LANES // odim
            v = jnp.concatenate([fb[pl.ds(b * m + k, odim, stride=odim), :] for k in range(m)], axis=0)
            wt[:, pl.ds(pl.multiple_of(b * LANES, LANES), LANES)] = v.T.astype(jnp.bfloat16)

    def piece_rows(u, pieces):
        @pl.loop(0, jrows)
        def _(i):
            at = [(r0 + i, h * lanes) for r0, h in pieces]
            z = jnp.concatenate([zb[r, :, h:h + lanes] for r, h in at], axis=1)
            m = jnp.concatenate([mk[pl.ds(r, 1), :][:, h:h + lanes] for r, h in at], axis=1)
            scale = jnp.concatenate([nc[u, 0]] * 2, axis=1)
            shift = jnp.concatenate([nc[u, 1]] * 2, axis=1)
            q = jnp.dot(wa[u], _norm_rows(z, scale, shift), preferred_element_type=jnp.float32)
            ab = (m * jax.nn.sigmoid(q[chan:2 * chan]) * q[:chan], m * jax.nn.sigmoid(q[3 * chan:4 * chan]) * q[2 * chan:3 * chan])
            g = jax.nn.sigmoid(q[4 * chan:])
            for s, (r, h) in enumerate(at):
                gb[r, :, h:h + lanes] = g[:, s * lanes:(s + 1) * lanes]
                for t in range(2):
                    st[pl.ds(pl.multiple_of((t * 2 + s) * (jrows * pst) + i * pst, 8), chan), :] = ab[t][:, s * lanes:(s + 1) * lanes]

    def turn(p):
        @pl.loop(0, chan, unroll=8)
        def _(c):
            for t in range(2):
                for s in range(2):
                    snd[t, p, s, c] = st[pl.ds((t * 2 + s) * (jrows * pst) + c, jrows, stride=pst), :].astype(jnp.bfloat16)

    own = pl.ds(pl.multiple_of(me * cown, cown), cown)

    def landing(u, t, p, s, src):
        if u == 0:
            return (rb if t else ra).at[p, s, src]
        return obuf.at[t * 4 + p * 2 + s, pl.ds(pl.multiple_of(src * cown, cown), cown)]

    def ab_copy(u, t, p, s, src, dst):
        return pltpu.make_async_remote_copy(
            src_ref=snd.at[t, p, s, pl.ds(pl.multiple_of(dst * cown, cown), cown)], dst_ref=landing(u, t, p, s, src),
            send_sem=ss_ab.at[u, t, p, s, dst], recv_sem=rs_ab.at[u, t, p, s, src],
            device_id={"dap": dst}, device_id_type=MESH)

    def ab_send(u, t, p, s):
        for d in range(1, n):
            ab_copy(u, t, p, s, me, lax.rem(me + d, n)).start()
        landing(u, t, p, s, me)[...] = snd[t, p, s, own]

    def ab_wait(u, t, p, s):
        for d in range(1, n):
            ab_copy(u, t, p, s, lax.rem(me + d, n), me).wait_recv()

    def x_copy(u, p, src, dst):
        return pltpu.make_async_remote_copy(
            src_ref=xs.at[p, dst], dst_ref=xr.at[p, pl.ds(pl.multiple_of(src * cown, cown), cown)],
            send_sem=ss_x.at[u, p, dst], recv_sem=rs_x.at[u, p, src],
            device_id={"dap": dst}, device_id_type=MESH)

    def x_send(u, p):
        for d in range(1, n):
            x_copy(u, p, me, lax.rem(me + d, n)).start()
        xr[p, own] = xs[p, me]

    def x_wait(u, p):
        for d in range(1, n):
            x_copy(u, p, lax.rem(me + d, n), me).wait_recv()

    def sent(u):
        for d in range(1, n):
            dst = lax.rem(me + d, n)
            for t in range(2):
                for p in range(2):
                    for s in range(2):
                        ab_copy(u, t, p, s, me, dst).wait_send()

    def x_sent(u):
        for d in range(1, n):
            for p in range(2):
                x_copy(u, p, me, lax.rem(me + d, n)).wait_send()

    def x_out(p):
        @pl.loop(0, cown)
        def _(c):
            a = jnp.concatenate([ra[h, p, :, c].reshape(lanes, lanes) for h in range(2)], axis=1)
            b = jnp.concatenate([rb[h, :, :, c].reshape(cols, lanes) for h in range(2)], axis=1)
            x = lax.dot_general(a, b, (((1,), (1,)), ((), ())), preferred_element_type=jnp.float32)
            xs[p, :, c] = x.astype(jnp.bfloat16).reshape(n, jrows, cols)

    def x_in():
        @pl.loop(0, cown)
        def _(c):
            a, b = (jnp.concatenate([
                jnp.concatenate([obuf[t * 4 + p * 2 + s, src * cown + c] for p in range(2) for src in range(n)], axis=0)
                for s in range(2)], axis=1) for t in range(2))
            x = lax.dot_general(a, b, (((0,), (0,)), ((), ())), preferred_element_type=jnp.float32)
            x = x.astype(jnp.bfloat16).reshape(2, n, jrows, cols)
            for p in range(2):
                xs[p, :, c] = x[p]

    def finish(u, p):
        half = chan * pxt

        @pl.loop(0, chan, unroll=8)
        def _(c):
            for h in range(2):
                fb[pl.ds(pl.multiple_of(h * half + c * pxt, 8), jrows), :] = xr[p, c, :, h * lanes:(h + 1) * lanes].astype(jnp.float32)

        @pl.loop(0, jrows)
        def _(i):
            r = p * jrows + i
            x = jnp.concatenate([fb[pl.ds(h * half + i, chan, stride=pxt), :] for h in range(2)], axis=1)
            xscale = jnp.concatenate([nc[u, 2]] * 2, axis=1)
            xshift = jnp.concatenate([nc[u, 3]] * 2, axis=1)
            upd = jnp.dot(wo[u], _norm_rows(x, xscale, xshift), preferred_element_type=jnp.float32)
            new = zb[r] + gb[r] * upd
            if u == 0:
                zb[r] = new
            else:
                zi[r] = new.T.reshape(chunks, n, jrows, chan).swapaxes(0, 1).reshape(cols, chan)

    def ocopy(p):
        at = pl.ds(p * jrows, jrows)
        return pltpu.make_async_copy(zi.at[at], o_hbm.at[at], osem.at[p])

    project(0)
    send_own(0)
    project(1)
    forward_far(0)
    send_own(1)
    prepare()
    forward_near(0)
    forward_opp(0)
    partner_all(0)
    outer(0, 0, blocks // 2)
    forward_far(1)
    outer(0, blocks // 2, blocks)
    zcopy.wait()
    mix(0)
    forward_near(1)
    piece_rows(0, ((0, 0), (jrows, 0)))
    turn(0)
    for t in (1, 0):
        for s in range(2):
            ab_send(0, t, 0, s)
    forward_opp(1)
    partner_all(1)
    outer(1, 0, blocks)
    mix(1)
    piece_rows(0, ((0, 1), (jrows, 1)))
    turn(1)
    for t in (1, 0):
        for s in range(2):
            ab_send(0, t, 1, s)
    for p in range(2):
        for s in range(2):
            ab_wait(0, 1, p, s)
    for p in range(2):
        ab_wait(0, 0, 0, p)
        ab_wait(0, 0, 1, p)
        x_out(p)
        x_send(0, p)
    sent(0)
    for p in range(2):
        x_wait(0, p)
        finish(0, p)
        piece_rows(1, ((p * jrows, 0), (p * jrows, 1)))
        turn(p)
        for t in range(2):
            for s in range(2):
                ab_send(1, t, p, s)
    x_sent(0)
    for t in range(2):
        for p in range(2):
            for s in range(2):
                ab_wait(1, t, p, s)
    x_in()
    for p in range(2):
        x_send(1, p)
    for p in range(2):
        x_wait(1, p)
        finish(1, p)
        ocopy(p).start()
    for p in range(2):
        ocopy(p).wait()
    sent(1)
    x_sent(1)
    for c in range(chunks):
        for h in (0, 1):
            for k, src in ((0, me), (1, me), (2, me), (3, left if h == 0 else right), (4, left if h == 0 else right),
                           (5, right if h == 0 else left), (6, opp)):
                send(c, h, src, k, part).wait_send()


def solution(mesh):
    row_spec = P(("data", "dap"), None, None)
    mask_spec = P(("data", "dap"), None)
    msa_spec = P(None, ("data", "dap"), None)
    replicated = P()

    def local_program(pair_loc, mask_loc, msa_loc, opm_norm, opm_proj, opm_out, opm_bias, tri_norm, tri_proj, tri_gate, tri_xnorm, tri_out):
        n = lax.axis_size("dap")
        rows, cols, chan = pair_loc.shape
        depth, _, mdim = msa_loc.shape
        odim = opm_proj.shape[1] // 2
        grp, chunks = 8, 2
        lanes = cols // chunks
        jrows = rows // chunks
        cown = chan // n
        vm = pl.BlockSpec(memory_space=pltpu.VMEM)
        hbm = pl.BlockSpec(memory_space=pl.ANY)
        f32, bf16 = jnp.float32, jnp.bfloat16
        dma = pltpu.SemaphoreType.DMA
        staged = max(4 * jrows * (chan + 8), depth // LANES * jrows * (odim + 8))
        return pl.pallas_call(
            functools.partial(_kernel, n),
            out_shape=jax.ShapeDtypeStruct(pair_loc.shape, f32),
            in_specs=[hbm, vm, hbm] + [vm] * 9,
            out_specs=hbm,
            scratch_shapes=[
                pltpu.VMEM((2, depth, grp, mdim), bf16),
                pltpu.VMEM((max(depth * grp, 2 * chan * (jrows + 8)), LANES), f32),
                pltpu.VMEM((rows * odim, depth), bf16),
                pltpu.VMEM((chunks, odim, lanes, depth), bf16),
                pltpu.VMEM((odim // 2, 2 * rows * odim // TILE, TILE, lanes), bf16),
                pltpu.VMEM((rows, cols, chan), f32),
                pltpu.VMEM((rows, chan, cols), f32),
                pltpu.VMEM((rows, chan, cols), f32),
                pltpu.VMEM((staged, LANES), f32),
                pltpu.VMEM((2, 2, 2, chan, jrows, lanes), bf16),
                pltpu.VMEM((2, 2, n, cown, jrows, lanes), bf16),
                pltpu.VMEM((2, 2, n, cown, jrows, lanes), bf16),
                pltpu.VMEM((2, n, cown, jrows, cols), bf16),
                pltpu.VMEM((2, chan, jrows, cols), bf16),
                pltpu.VMEM((rows, cols), f32),
                pltpu.VMEM((chan, odim * odim), bf16),
                pltpu.VMEM((2, 5 * chan, chan), bf16),
                pltpu.VMEM((2, chan, chan), bf16),
                pltpu.VMEM((2, 4, chan, lanes), f32),
                pltpu.VMEM((chan, lanes), f32),
                dma((2,)), dma((1,)), dma((2,)),
                dma((chunks, 2, 7)), dma((chunks, 2, n)),
                dma((2, 2, 2, 2, n)), dma((2, 2, 2, 2, n)),
                dma((2, 2, n)), dma((2, 2, n)),
            ],
            compiler_params=pltpu.CompilerParams(collective_id=0, has_side_effects=True, vmem_limit_bytes=63 * 1024 * 1024),
            name="pair_stack",
        )(pair_loc, mask_loc, msa_loc, opm_norm, opm_proj, opm_out, opm_bias.reshape(1, chan), tri_norm, tri_proj, tri_gate, tri_xnorm, tri_out)

    return jax.shard_map(local_program, mesh=mesh, in_specs=(row_spec, mask_spec, msa_spec) + (replicated,) * 9, out_specs=row_spec, check_vma=False)
```

```python
import functools

import jax
import jax.numpy as jnp
from jax import lax
from jax.experimental import pallas as pl
from jax.experimental.pallas import tpu as pltpu
from jax.sharding import PartitionSpec as P

LN_EPS = 1e-5
LANES = 128
TILE = 16
MESH = pl.DeviceIdType.MESH


def _norm_rows(v, scale, shift):
    mean = jnp.mean(v, axis=0, keepdims=True)
    cen = v - mean
    var = jnp.mean(cen * cen, axis=0, keepdims=True)
    return (cen * lax.rsqrt(var + LN_EPS) * scale + shift).astype(jnp.bfloat16)


def _column(row, n):
    return jnp.broadcast_to(row, (n, row.shape[1])).T


def _kernel(n, z_hbm, mask_ref, msa_hbm, onrm_ref, oproj_ref, oout_ref, obias_ref, nrm_ref, proj_ref, gate_ref, xnrm_ref, out_ref, o_hbm,
            mb, fb, at_b, ball, obuf, zi, zb, gb, st, snd, ra, rb, xs, xr, mk, wt, wa, wo, nc, bc,
            msem, zsem, osem, ss, rs, ss_o, rs_o, ss_xo, rs_xo, ss_ab, rs_ab, ss_x, rs_x):
    me = lax.axis_index("dap")
    depth, grp, mdim = mb.shape[1:]
    rows, cols, chan = zi.shape
    chunks, odim, lanes = ball.shape[:3]
    jrows = lanes // n
    groups = rows // grp
    per = jrows // grp
    qh = odim // 2
    cown = chan // n
    blocks = odim // 2
    tiles = depth // LANES
    bst, pst, pxt = odim + 8, chan + 8, jrows + 8
    part = me + 1 - 2 * lax.rem(me, 2)
    right, left, opp = lax.rem(me + 2, n), lax.rem(me + n - 2, n), lax.rem(me + 4, n)

    def mcopy(g):
        return pltpu.make_async_copy(msa_hbm.at[:, pl.ds(g * grp, grp)], mb.at[g % 2], msem.at[g % 2])

    mcopy(0).start()
    mcopy(1).start()
    zcopy = pltpu.make_async_copy(z_hbm, zi, zsem.at[0])
    zcopy.start()
    barrier = pltpu.get_barrier_semaphore()
    for s in range(1, n):
        pl.semaphore_signal(barrier, inc=1, device_id={"dap": lax.rem(me + s, n)}, device_id_type=MESH)
    pl.semaphore_wait(barrier, n - 1)

    def slot(c, dev):
        return lax.rem(dev + c * (n // 2), n)

    def turned(v, c):
        return v if c == 0 else jnp.concatenate([v[n // 2:], v[:n // 2]], axis=0)

    def block(c, h, src):
        return ball.at[c, h * qh:(h + 1) * qh, pl.ds(pl.multiple_of(slot(c, src) * jrows, jrows), jrows)]

    def send(c, h, src, k, dst):
        return pltpu.make_async_remote_copy(
            src_ref=block(c, h, src), dst_ref=block(c, h, src), send_sem=ss.at[c, h, k], recv_sem=rs.at[c, h, src],
            device_id={"dap": dst}, device_id_type=MESH)

    def arrived(c, h, src):
        send(c, h, src, 0, part).wait_recv()

    oscale, oshift = onrm_ref[0:1, :], onrm_ref[1:2, :]
    sb = 64

    def project(c):
        for k in range(per):
            g = c * per + k
            mcopy(g).wait()

            @pl.loop(0, depth // sb)
            def _(b, g=g):
                x = mb[g % 2, pl.ds(b * sb, sb)].reshape(sb * grp, mdim)
                mean = jnp.dot(x, jnp.ones((mdim, LANES), jnp.bfloat16), preferred_element_type=jnp.float32) * (1.0 / mdim)
                cen = x.astype(jnp.float32) - jnp.concatenate([mean] * (mdim // LANES), axis=1)
                var = jnp.mean(cen * cen, axis=1, keepdims=True)
                y = (cen * lax.rsqrt(var + LN_EPS) * oscale + oshift).astype(jnp.bfloat16)
                at = pl.ds(pl.multiple_of(b * (sb * grp), sb * grp), sb * grp)
                fb[at, :2 * odim] = jnp.dot(y, oproj_ref[...], preferred_element_type=jnp.float32)
            if g + 2 < groups:
                mcopy(g + 2).start()

            @pl.loop(0, grp)
            def _(i, g=g, k=k):
                v = fb[pl.ds(i, depth, stride=grp), :].T
                r = g * grp + i
                at_b[pl.ds(pl.multiple_of(r * odim, odim), odim), :] = v[:odim].astype(jnp.bfloat16)
                for t in range(tiles):
                    row = pl.multiple_of(t * (jrows * bst) + (k * grp + i) * bst, 8)
                    st[pl.ds(row, odim), :] = v[odim:2 * odim, t * LANES:(t + 1) * LANES]

        @pl.loop(0, odim, unroll=4)
        def _(q):
            for t in range(tiles):
                ball[c, q, pl.ds(pl.multiple_of(slot(c, me) * jrows, jrows), jrows), t * LANES:(t + 1) * LANES] = (
                    st[pl.ds(t * (jrows * bst) + q, jrows, stride=bst), :].astype(jnp.bfloat16))

    def send_own(c):
        for h in (0, 1):
            send(c, h, me, 0, right).start()
            send(c, 1 - h, me, 1, left).start()
        for h in (0, 1):
            send(c, h, me, 2, part).start()

    def forward_far(c):
        arrived(c, 0, left)
        send(c, 0, left, 3, right).start()
        send(c, 0, left, 4, part).start()
        arrived(c, 1, right)
        send(c, 1, right, 3, left).start()
        send(c, 1, right, 4, part).start()

    def forward_near(c):
        arrived(c, 1, left)
        send(c, 1, left, 5, part).start()
        arrived(c, 0, right)
        send(c, 0, right, 5, part).start()

    def forward_opp(c):
        for h in (0, 1):
            arrived(c, h, opp)
            send(c, h, opp, 6, part).start()

    def partner_all(c):
        for d in (0, 2, 4, 6):
            for h in (0, 1):
                arrived(c, h, lax.rem(part + d, n))

    def outer(c, lo, hi):
        @pl.loop(lo, hi)
        def _(b):
            rhs = ball[c, pl.ds(b * 2, 2)].reshape(2 * lanes, depth)
            o = lax.dot_general(at_b[...], rhs, (((1,), (1,)), ((), ())), preferred_element_type=jnp.float32)
            o = (o * (1.0 / depth)).astype(jnp.bfloat16)
            nt = rows * odim // TILE
            for t in range(2):
                obuf[b, t * nt:(t + 1) * nt] = o[:, t * lanes:(t + 1) * lanes].reshape(nt, TILE, lanes)

    def mix(c):
        @pl.loop(0, rows)
        def _(i):
            nt, w = rows * odim // TILE, odim // TILE
            rhs = jnp.stack([obuf[:, pl.ds(t * nt + i * w, w)] for t in range(2)], axis=1).reshape(odim * odim, lanes)
            upd = jnp.dot(wt[...], rhs, preferred_element_type=jnp.float32)
            zt = turned(zi[i].reshape(n, chunks, jrows, chan)[:, c], c).reshape(lanes, chan).T
            zb[i, :, c * lanes:(c + 1) * lanes] = zt + (upd + bc[...])

    def prepare():
        rid = lax.broadcasted_iota(jnp.int32, (cols, cols), 0)
        cid = lax.broadcasted_iota(jnp.int32, (cols, cols), 1)
        two = chunks * jrows
        piece = (rid // jrows) % chunks
        place = piece * lanes + ((rid // two + piece * (n // 2)) % n) * jrows + rid % jrows
        perm = (cid == place).astype(jnp.float32).astype(jnp.bfloat16)
        mk[...] = jnp.dot(mask_ref[...].astype(jnp.float32).astype(jnp.bfloat16), perm, preferred_element_type=jnp.float32)
        bc[...] = _column(obias_ref[...], lanes)
        for t in range(2):
            for k in range(2):
                nc[t, k] = _column(nrm_ref[t, k:k + 1, :], lanes)
                nc[t, 2 + k] = _column(xnrm_ref[t, k:k + 1, :], lanes)
            for k in range(4):
                wa[t, k * chan:(k + 1) * chan] = proj_ref[t, :, k * chan:(k + 1) * chan].astype(jnp.float32).T.astype(jnp.bfloat16)
            wa[t, 4 * chan:] = gate_ref[t].astype(jnp.float32).T.astype(jnp.bfloat16)
            wo[t] = out_ref[t].astype(jnp.float32).T.astype(jnp.bfloat16)
        fb[:odim * odim, :] = oout_ref[...].astype(jnp.float32)

        @pl.loop(0, odim * odim // LANES)
        def _(b):
            m = LANES // odim
            v = jnp.concatenate([fb[pl.ds(b * m + k, odim, stride=odim), :] for k in range(m)], axis=0)
            wt[:, pl.ds(pl.multiple_of(b * LANES, LANES), LANES)] = v.T.astype(jnp.bfloat16)

    def piece_rows(u, pieces):
        @pl.loop(0, jrows)
        def _(i):
            at = [(r0 + i, h * lanes) for r0, h in pieces]
            z = jnp.concatenate([zb[r, :, h:h + lanes] for r, h in at], axis=1)
            m = jnp.concatenate([mk[pl.ds(r, 1), :][:, h:h + lanes] for r, h in at], axis=1)
            scale = jnp.concatenate([nc[u, 0]] * 2, axis=1)
            shift = jnp.concatenate([nc[u, 1]] * 2, axis=1)
            q = jnp.dot(wa[u], _norm_rows(z, scale, shift), preferred_element_type=jnp.float32)
            ab = (m * jax.nn.sigmoid(q[chan:2 * chan]) * q[:chan], m * jax.nn.sigmoid(q[3 * chan:4 * chan]) * q[2 * chan:3 * chan])
            g = jax.nn.sigmoid(q[4 * chan:])
            for s, (r, h) in enumerate(at):
                gb[r, :, h:h + lanes] = g[:, s * lanes:(s + 1) * lanes]
                for t in range(2):
                    st[pl.ds(pl.multiple_of((t * 2 + s) * (jrows * pst) + i * pst, 8), chan), :] = ab[t][:, s * lanes:(s + 1) * lanes]

    def turn(p):
        @pl.loop(0, chan, unroll=8)
        def _(c):
            for t in range(2):
                for s in range(2):
                    snd[t, p, s, c] = st[pl.ds((t * 2 + s) * (jrows * pst) + c, jrows, stride=pst), :].astype(jnp.bfloat16)

    own = pl.ds(pl.multiple_of(me * cown, cown), cown)

    chip, core = me // 2, lax.rem(me, 2)
    first, second = chip + 1 - 2 * lax.rem(chip, 2), n // 2 - 1 - chip
    gchan, cslice = chan // 2, chan // 4
    sides = (lax.rem((chip + 1) // 2, 2), chip // 2)

    def mate(t, g):
        return first if t == g else second

    def o_copy(t, p, s, g, far, src_core, dst_core, sending):
        other = 2 * (mate(t, g) if far else chip) + (dst_core if sending else src_core)
        src = me if sending else other
        buf = rb if t else ra
        k = (2 if far else 0)
        return pltpu.make_async_remote_copy(
            src_ref=snd.at[t, p, s, pl.ds(pl.multiple_of(g * gchan + (dst_core if sending else core) * cslice, cslice), cslice)],
            dst_ref=buf.at[g, p, slot(s, src)],
            send_sem=ss_o.at[t, p, s, g, k + (dst_core if sending else 0)], recv_sem=rs_o.at[t, p, s, g, k + (core if sending else src_core)],
            device_id={"dap": other}, device_id_type=MESH)

    def o_send(t, p, s):
        for g in range(2):
            for c in range(2):
                o_copy(t, p, s, g, True, core, c, True).start()
            o_copy(t, p, s, g, False, core, 1 - core, True).start()
            buf = rb if t else ra
            buf[g, p, slot(s, me)] = snd[t, p, s, pl.ds(pl.multiple_of(g * gchan + core * cslice, cslice), cslice)]

    def o_wait(t, p, s):
        for g in range(2):
            o_copy(t, p, s, g, False, 1 - core, core, False).wait_recv()
            for c in range(2):
                o_copy(t, p, s, g, True, c, core, False).wait_recv()

    def o_sent():
        for t in range(2):
            for p in range(2):
                for s in range(2):
                    for g in range(2):
                        for c in range(2):
                            o_copy(t, p, s, g, True, core, c, True).wait_send()
                        o_copy(t, p, s, g, False, core, 1 - core, True).wait_send()

    def xo_copy(p, g, far, src_core, dst_core, sending):
        other = 2 * (mate(0, g) if far else chip) + (dst_core if sending else src_core)
        dst = other if sending else me
        k = 2 if far else 0
        return pltpu.make_async_remote_copy(
            src_ref=xs.at[g, :, slot(p, dst)],
            dst_ref=xr.at[p, sides[g], pl.ds((g * 2 + (core if sending else src_core)) * 2, 2)],
            send_sem=ss_xo.at[p, g, k + (dst_core if sending else 0)], recv_sem=rs_xo.at[p, g, k + (core if sending else src_core)],
            device_id={"dap": other}, device_id_type=MESH)

    def xo_send(p):
        for g in range(2):
            for c in range(2):
                xo_copy(p, g, True, core, c, True).start()
            xo_copy(p, g, False, core, 1 - core, True).start()
            xr[p, sides[g], pl.ds((g * 2 + core) * 2, 2)] = xs[g, :, slot(p, me)]

    def xo_wait(p):
        for g in range(2):
            xo_copy(p, g, False, 1 - core, core, False).wait_recv()
            for c in range(2):
                xo_copy(p, g, True, c, core, False).wait_recv()

    def xo_sent():
        for p in range(2):
            for g in range(2):
                for c in range(2):
                    xo_copy(p, g, True, core, c, True).wait_send()
                xo_copy(p, g, False, core, 1 - core, True).wait_send()

    def x_out(p):
        for g in range(2):
            at = [slot(p, 2 * w + c) for w in (chip, mate(0, g)) for c in range(2)]
            for e in range(cslice // cown):
                @pl.loop(0, cown, unroll=2)
                def _(c, g=g, e=e, at=at):
                    k = e * cown + c
                    a = jnp.concatenate([jnp.concatenate([ra[g, h, d, k] for d in at], axis=0) for h in range(2)], axis=1)
                    b = jnp.concatenate([rb[g, h, :, k].reshape(lanes, lanes) for h in range(2)], axis=1)
                    x = lax.dot_general(a, b, (((1,), (1,)), ((), ())), preferred_element_type=jnp.float32).astype(jnp.bfloat16)
                    for m, d in enumerate(at):
                        xs[g, e, d, c] = x[m * jrows:(m + 1) * jrows]

    def parts(p):
        return ((0, cown),) if p == 0 else ((0, cown // 2), (cown // 2, cown // 2))

    def landing(t, p, s, src, e):
        lo, m = parts(p)[e]
        return obuf.at[t * 4 + p * 2 + s, pl.ds(pl.multiple_of(src * cown, cown) + lo, m)]

    def ab_copy(t, p, s, e, src, dst):
        lo, m = parts(p)[e]
        return pltpu.make_async_remote_copy(
            src_ref=snd.at[t, p, s, pl.ds(pl.multiple_of(dst * cown, cown) + lo, m)], dst_ref=landing(t, p, s, src, e),
            send_sem=ss_ab.at[t, p, s, e, dst], recv_sem=rs_ab.at[t, p, s, e, src],
            device_id={"dap": dst}, device_id_type=MESH)

    def ab_send(p, e):
        lo, m = parts(p)[e]
        for t in range(2):
            for s in range(2):
                for d in range(1, n):
                    ab_copy(t, p, s, e, me, lax.rem(me + d, n)).start()
                obuf[t * 4 + p * 2 + s, pl.ds(pl.multiple_of(me * cown, cown) + lo, m)] = snd[t, p, s, pl.ds(pl.multiple_of(me * cown, cown) + lo, m)]

    def ab_wait(p, e):
        for t in range(2):
            for s in range(2):
                for d in range(1, n):
                    ab_copy(t, p, s, e, lax.rem(me + d, n), me).wait_recv()

    def ab_sent():
        for p in range(2):
            for e in range(len(parts(p))):
                for t in range(2):
                    for s in range(2):
                        for d in range(1, n):
                            ab_copy(t, p, s, e, me, lax.rem(me + d, n)).wait_send()

    hown = cown // 2

    def x_copy(p, e, src, dst):
        at = pl.ds(e * hown, hown)
        return pltpu.make_async_remote_copy(
            src_ref=xs.at[p, :, dst, at], dst_ref=xr.at[p, :, src, at],
            send_sem=ss_x.at[p, e, dst], recv_sem=rs_x.at[p, e, src],
            device_id={"dap": dst}, device_id_type=MESH)

    def x_send(p, e):
        for d in range(1, n):
            x_copy(p, e, me, lax.rem(me + d, n)).start()
        at = slice(e * hown, (e + 1) * hown)
        xr[p, :, me, at] = xs[p, :, me, at]

    def x_wait(p):
        for e in range(2):
            for d in range(1, n):
                x_copy(p, e, lax.rem(me + d, n), me).wait_recv()

    def x_sent():
        for p in range(2):
            for e in range(2):
                for d in range(1, n):
                    x_copy(p, e, me, lax.rem(me + d, n)).wait_send()

    def x_in(e):
        @pl.loop(e * hown, (e + 1) * hown)
        def _(c):
            a, b = (jnp.concatenate([
                jnp.concatenate([obuf[t * 4 + p * 2 + s, src * cown + c] for p in range(2) for src in range(n)], axis=0)
                for s in range(2)], axis=1) for t in range(2))
            x = lax.dot_general(a, b, (((0,), (0,)), ((), ())), preferred_element_type=jnp.float32)
            x = x.astype(jnp.bfloat16).reshape(2, n, jrows, cols)
            for p in range(2):
                v = turned(x[p], p)
                for h in range(2):
                    xs[p, h, :, c] = v[:, :, h * lanes:(h + 1) * lanes]

    def finish(u, p):
        half = chan * pxt

        lane = lax.broadcasted_iota(jnp.int32, (jrows, lanes), 1) // (lanes // 4)
        for k in range(n):
            take = ((lane == 0) | (lane == 3)) if k < n // 2 else (lane < 2)

            @pl.loop(0, cown, unroll=8)
            def _(c, k=k, take=take):
                x0, x1 = (xr[p, h, k, c].astype(jnp.float32) for h in range(2))
                if u == 0:
                    x0, x1 = jnp.where(take, x0, x1), jnp.where(take, x1, x0)
                for h, x in enumerate((x0, x1)):
                    fb[pl.ds(pl.multiple_of(h * half + (k * cown + c) * pxt, 8), jrows), :] = x

        @pl.loop(0, jrows)
        def _(i):
            r = p * jrows + i
            x = jnp.concatenate([fb[pl.ds(h * half + i, chan, stride=pxt), :] for h in range(2)], axis=1)
            xscale = jnp.concatenate([nc[u, 2]] * 2, axis=1)
            xshift = jnp.concatenate([nc[u, 3]] * 2, axis=1)
            upd = jnp.dot(wo[u], _norm_rows(x, xscale, xshift), preferred_element_type=jnp.float32)
            new = zb[r] + gb[r] * upd
            if u == 0:
                zb[r] = new
            else:
                new = new.T.reshape(chunks, n, jrows, chan)
                zi[r] = jnp.stack([turned(new[c], c) for c in range(chunks)], axis=1).reshape(cols, chan)

    def ocopy(p):
        at = pl.ds(p * jrows, jrows)
        return pltpu.make_async_copy(zi.at[at], o_hbm.at[at], osem.at[p])

    project(0)
    send_own(0)
    project(1)
    forward_far(0)
    send_own(1)
    prepare()
    forward_near(0)
    forward_opp(0)
    partner_all(0)
    outer(0, 0, blocks // 2)
    forward_far(1)
    outer(0, blocks // 2, blocks)
    zcopy.wait()
    mix(0)
    forward_near(1)
    piece_rows(0, ((0, 0), (jrows, 0)))
    turn(0)
    for t in (1, 0):
        for s in range(2):
            o_send(t, 0, s)
    forward_opp(1)
    partner_all(1)
    outer(1, 0, blocks)
    mix(1)
    piece_rows(0, ((0, 1), (jrows, 1)))
    turn(1)
    for t in (1, 0):
        for s in range(2):
            o_send(t, 1, s)
    for p in range(2):
        for s in range(2):
            o_wait(1, p, s)
    for p in range(2):
        o_wait(0, 0, p)
        o_wait(0, 1, p)
        x_out(p)
        xo_send(p)
    o_sent()
    for p in range(2):
        xo_wait(p)
        finish(0, p)
        piece_rows(1, ((p * jrows, 0), (p * jrows, 1)))
        turn(p)
        for e in range(len(parts(p))):
            ab_send(p, e)
    xo_sent()
    ab_wait(0, 0)
    for e in range(2):
        ab_wait(1, e)
        x_in(e)
        for p in range(2):
            x_send(p, e)
    for p in range(2):
        x_wait(p)
        finish(1, p)
        ocopy(p).start()
    for p in range(2):
        ocopy(p).wait()
    ab_sent()
    x_sent()
    for c in range(chunks):
        for h in (0, 1):
            for k, src in ((0, me), (1, me), (2, me), (3, left if h == 0 else right), (4, left if h == 0 else right),
                           (5, right if h == 0 else left), (6, opp)):
                send(c, h, src, k, part).wait_send()


def solution(mesh):
    row_spec = P(("data", "dap"), None, None)
    mask_spec = P(("data", "dap"), None)
    msa_spec = P(None, ("data", "dap"), None)
    replicated = P()

    def local_program(pair_loc, mask_loc, msa_loc, opm_norm, opm_proj, opm_out, opm_bias, tri_norm, tri_proj, tri_gate, tri_xnorm, tri_out):
        n = lax.axis_size("dap")
        rows, cols, chan = pair_loc.shape
        depth, _, mdim = msa_loc.shape
        odim = opm_proj.shape[1] // 2
        grp, chunks = 8, 2
        lanes = cols // chunks
        jrows = rows // chunks
        cown = chan // n
        vm = pl.BlockSpec(memory_space=pltpu.VMEM)
        hbm = pl.BlockSpec(memory_space=pl.ANY)
        f32, bf16 = jnp.float32, jnp.bfloat16
        dma = pltpu.SemaphoreType.DMA
        staged = max(4 * jrows * (chan + 8), depth // LANES * jrows * (odim + 8))
        return pl.pallas_call(
            functools.partial(_kernel, n),
            out_shape=jax.ShapeDtypeStruct(pair_loc.shape, f32),
            in_specs=[hbm, vm, hbm] + [vm] * 9,
            out_specs=hbm,
            scratch_shapes=[
                pltpu.VMEM((2, depth, grp, mdim), bf16),
                pltpu.VMEM((max(depth * grp, 2 * chan * (jrows + 8)), LANES), f32),
                pltpu.VMEM((rows * odim, depth), bf16),
                pltpu.VMEM((chunks, odim, lanes, depth), bf16),
                pltpu.VMEM((odim // 2, 2 * rows * odim // TILE, TILE, lanes), bf16),
                pltpu.VMEM((rows, cols, chan), f32),
                pltpu.VMEM((rows, chan, cols), f32),
                pltpu.VMEM((rows, chan, cols), f32),
                pltpu.VMEM((staged, LANES), f32),
                pltpu.VMEM((2, 2, 2, chan, jrows, lanes), bf16),
                pltpu.VMEM((2, 2, n, chan // 4, jrows, lanes), bf16),
                pltpu.VMEM((2, 2, n, chan // 4, jrows, lanes), bf16),
                pltpu.VMEM((2, 2, n, cown, jrows, lanes), bf16),
                pltpu.VMEM((2, 2, n, cown, jrows, lanes), bf16),
                pltpu.VMEM((rows, cols), f32),
                pltpu.VMEM((chan, odim * odim), bf16),
                pltpu.VMEM((2, 5 * chan, chan), bf16),
                pltpu.VMEM((2, chan, chan), bf16),
                pltpu.VMEM((2, 4, chan, lanes), f32),
                pltpu.VMEM((chan, lanes), f32),
                dma((2,)), dma((1,)), dma((2,)),
                dma((chunks, 2, 7)), dma((chunks, 2, n)),
                dma((2, 2, 2, 2, 4)), dma((2, 2, 2, 2, 4)), dma((2, 2, 4)), dma((2, 2, 4)),
                dma((2, 2, 2, 2, n)), dma((2, 2, 2, 2, n)), dma((2, 2, n)), dma((2, 2, n)),
            ],
            compiler_params=pltpu.CompilerParams(collective_id=0, has_side_effects=True, vmem_limit_bytes=63 * 1024 * 1024),
            name="pair_stack",
        )(pair_loc, mask_loc, msa_loc, opm_norm, opm_proj, opm_out, opm_bias.reshape(1, chan), tri_norm, tri_proj, tri_gate, tri_xnorm, tri_out)

    return jax.shard_map(local_program, mesh=mesh, in_specs=(row_spec, mask_spec, msa_spec) + (replicated,) * 9, out_specs=row_spec, check_vma=False)
```

```python
import functools

import jax
import jax.numpy as jnp
from jax import lax
from jax.experimental import pallas as pl
from jax.experimental.pallas import tpu as pltpu
from jax.sharding import PartitionSpec as P

LN_EPS = 1e-5
LANES = 128
TILE = 16
MESH = pl.DeviceIdType.MESH


def _norm_rows(v, scale, shift):
    mean = jnp.mean(v, axis=0, keepdims=True)
    cen = v - mean
    var = jnp.mean(cen * cen, axis=0, keepdims=True)
    return (cen * lax.rsqrt(var + LN_EPS) * scale + shift).astype(jnp.bfloat16)


def _column(row, n):
    return jnp.broadcast_to(row, (n, row.shape[1])).T


def _kernel(n, z_hbm, mask_ref, msa_hbm, onrm_ref, oproj_ref, oout_ref, obias_ref, nrm_ref, proj_ref, gate_ref, xnrm_ref, out_ref, o_hbm,
            mb, fb, at_b, ball, obuf, zi, zb, gb, st, snd, ra, rb, xs, xr, mk, wt, wa, wo, nc, bc,
            msem, zsem, osem, ss, rs, rf, ss_o, rs_o, ss_xo, rs_xo, ss_ab, rs_ab, ss_x, rs_x):
    me = lax.axis_index("dap")
    depth, grp, mdim = mb.shape[1:]
    rows, cols, chan = zi.shape
    chunks, lanes, jrows, odim = 2, cols // 2, rows // 2, ball.shape[3]
    groups = rows // grp
    per = jrows // grp
    qh = odim // 2
    cown = chan // n
    blocks = odim // 2
    bst, pst, pxt = odim + 8, chan + 8, jrows + 8
    part = me + 1 - 2 * lax.rem(me, 2)
    right, left, opp = lax.rem(me + 2, n), lax.rem(me + n - 2, n), lax.rem(me + 4, n)

    def mcopy(g):
        return pltpu.make_async_copy(msa_hbm.at[:, pl.ds(g * grp, grp)], mb.at[g % 2], msem.at[g % 2])

    mcopy(0).start()
    mcopy(1).start()
    zcopy = pltpu.make_async_copy(z_hbm, zi, zsem.at[0])
    zcopy.start()
    barrier = pltpu.get_barrier_semaphore()
    for s in range(1, n):
        pl.semaphore_signal(barrier, inc=1, device_id={"dap": lax.rem(me + s, n)}, device_id_type=MESH)
    pl.semaphore_wait(barrier, n - 1)

    def slot(c, dev):
        return lax.rem(dev + c * (n // 2), n)

    def turned(v, c):
        return v if c == 0 else jnp.concatenate([v[n // 2:], v[:n // 2]], axis=0)

    def block(c, h, src):
        return ball.at[c, h, slot(c, src)]

    def send(c, h, src, k, dst):
        return pltpu.make_async_remote_copy(
            src_ref=block(c, h, src), dst_ref=block(c, h, src), send_sem=ss.at[c, h, k], recv_sem=rs.at[c, h, src],
            device_id={"dap": dst}, device_id_type=MESH)

    def arrived(c, h, src):
        send(c, h, src, 0, part).wait_recv()

    def far(c, h, src, k, dst):
        at = ball.at[c, h, slot(c, src), k * qh:(k + 1) * qh]
        return pltpu.make_async_remote_copy(
            src_ref=at, dst_ref=at, send_sem=ss.at[c, h, 6 + k], recv_sem=rf.at[c, h, k],
            device_id={"dap": dst}, device_id_type=MESH)

    oscale, oshift = onrm_ref[0:1, :], onrm_ref[1:2, :]
    sb = 64
    hdep = depth // 2
    tiles = hdep // LANES

    def project(c, h):
        for k in range(per):
            g = c * per + k
            if h == 0:
                mcopy(g).wait()

            @pl.loop(0, hdep // sb)
            def _(b, g=g):
                x = mb[g % 2, pl.ds(h * hdep + b * sb, sb)].astype(jnp.float32).reshape(sb * grp, mdim)
                mean = jnp.mean(x, axis=1, keepdims=True)
                cen = x - mean
                var = jnp.mean(cen * cen, axis=1, keepdims=True)
                y = (cen * lax.rsqrt(var + LN_EPS) * oscale + oshift).astype(jnp.bfloat16)
                at = pl.ds(pl.multiple_of(b * (sb * grp), sb * grp), sb * grp)
                fb[at, :2 * odim] = lax.dot_general(y, oproj_ref[...], (((1,), (1,)), ((), ())), preferred_element_type=jnp.float32)
            if h == 1 and g + 2 < groups:
                mcopy(g + 2).start()

            @pl.loop(0, grp)
            def _(i, g=g, k=k):
                v = fb[pl.ds(i, hdep, stride=grp), :].T
                r = g * grp + i
                at_b[pl.ds(pl.multiple_of(r * odim, odim), odim), h * hdep:(h + 1) * hdep] = v[:odim].astype(jnp.bfloat16)
                for t in range(tiles):
                    row = pl.multiple_of(t * (jrows * bst) + (k * grp + i) * bst, 8)
                    st[pl.ds(row, odim), :] = v[odim:2 * odim, t * LANES:(t + 1) * LANES]

        @pl.loop(0, odim, unroll=4)
        def _(q):
            for t in range(tiles):
                ball[c, h, slot(c, me), q, :, t * LANES:(t + 1) * LANES] = (
                    st[pl.ds(t * (jrows * bst) + q, jrows, stride=bst), :].astype(jnp.bfloat16))

    def send_own(c, h):
        for k, dst in enumerate((right, left, part)):
            send(c, h, me, k, dst).start()

    def forward_far(c, h):
        for k, (src, dst) in enumerate(((left, right), (right, left))):
            arrived(c, h, src)
            far(c, h, src, k, dst).start()
            send(c, h, src, 3 + k, part).start()

    def forward_opp(c):
        for h in (0, 1):
            for k in (0, 1):
                far(c, h, opp, k, part).wait_recv()
            send(c, h, opp, 5, part).start()

    def partner_all(c):
        for d in (0, 2, 4, 6):
            for h in (0, 1):
                arrived(c, h, lax.rem(part + d, n))

    def outer(c, lo, hi):
        @pl.loop(lo, hi)
        def _(b):
            rhs = jnp.concatenate([jnp.concatenate([ball[c, h, :, b * 2 + t].reshape(lanes, hdep) for h in range(2)], axis=1) for t in range(2)], axis=0)
            o = lax.dot_general(at_b[...], rhs, (((1,), (1,)), ((), ())), preferred_element_type=jnp.float32)
            o = (o * (1.0 / depth)).astype(jnp.bfloat16)
            nt = rows * odim // TILE
            for t in range(2):
                obuf[b, t * nt:(t + 1) * nt] = o[:, t * lanes:(t + 1) * lanes].reshape(nt, TILE, lanes)

    def mix(c):
        @pl.loop(0, rows)
        def _(i):
            nt, w = rows * odim // TILE, odim // TILE
            rhs = jnp.stack([obuf[:, pl.ds(t * nt + i * w, w)] for t in range(2)], axis=1).reshape(odim * odim, lanes)
            upd = jnp.dot(wt[...], rhs, preferred_element_type=jnp.float32)
            zt = turned(zi[i].reshape(n, chunks, jrows, chan)[:, c], c).reshape(lanes, chan).T
            zb[i, :, c * lanes:(c + 1) * lanes] = zt + (upd + bc[...])

    def prepare():
        rid = lax.broadcasted_iota(jnp.int32, (cols, cols), 0)
        cid = lax.broadcasted_iota(jnp.int32, (cols, cols), 1)
        two = chunks * jrows
        piece = (rid // jrows) % chunks
        place = piece * lanes + ((rid // two + piece * (n // 2)) % n) * jrows + rid % jrows
        perm = (cid == place).astype(jnp.float32).astype(jnp.bfloat16)
        mk[...] = jnp.dot(mask_ref[...].astype(jnp.float32).astype(jnp.bfloat16), perm, preferred_element_type=jnp.float32)
        bc[...] = _column(obias_ref[...], lanes)
        for t in range(2):
            for k in range(2):
                nc[t, k] = _column(nrm_ref[t, k:k + 1, :], lanes)
                nc[t, 2 + k] = _column(xnrm_ref[t, k:k + 1, :], lanes)
            for k in range(4):
                wa[t, k * chan:(k + 1) * chan] = proj_ref[t, :, k * chan:(k + 1) * chan].astype(jnp.float32).T.astype(jnp.bfloat16)
            wa[t, 4 * chan:] = gate_ref[t].astype(jnp.float32).T.astype(jnp.bfloat16)
            wo[t] = out_ref[t].astype(jnp.float32).T.astype(jnp.bfloat16)
        fb[:odim * odim, :] = oout_ref[...].astype(jnp.float32)

        @pl.loop(0, odim * odim // LANES)
        def _(b):
            m = LANES // odim
            v = jnp.concatenate([fb[pl.ds(b * m + k, odim, stride=odim), :] for k in range(m)], axis=0)
            wt[:, pl.ds(pl.multiple_of(b * LANES, LANES), LANES)] = v.T.astype(jnp.bfloat16)

    def piece_rows(u, steps, pieces):
        @pl.loop(0, steps)
        def _(i):
            at = [(r0 + i, h * lanes) for r0, h, _, _ in pieces]
            z = jnp.concatenate([zb[r, :, h:h + lanes] for r, h in at], axis=1)
            m = jnp.concatenate([mk[pl.ds(r, 1), :][:, h:h + lanes] for r, h in at], axis=1)
            scale = jnp.concatenate([nc[u, 0]] * 2, axis=1)
            shift = jnp.concatenate([nc[u, 1]] * 2, axis=1)
            q = jnp.dot(wa[u], _norm_rows(z, scale, shift), preferred_element_type=jnp.float32)
            ab = (m * jax.nn.sigmoid(q[chan:2 * chan]) * q[:chan], m * jax.nn.sigmoid(q[3 * chan:4 * chan]) * q[2 * chan:3 * chan])
            g = jax.nn.sigmoid(q[4 * chan:])
            for s, (r, h) in enumerate(at):
                gb[r, :, h:h + lanes] = g[:, s * lanes:(s + 1) * lanes]
                for t in range(2):
                    row = pl.multiple_of((t * 2 + pieces[s][2]) * (jrows * pst) + (i + pieces[s][3]) * pst, 8)
                    st[pl.ds(row, chan), :] = ab[t][:, s * lanes:(s + 1) * lanes]

    def turn(p, which=(0, 1)):
        @pl.loop(0, chan, unroll=8)
        def _(c):
            for t in range(2):
                for s in which:
                    snd[t, p, s, c] = st[pl.ds((t * 2 + s) * (jrows * pst) + c, jrows, stride=pst), :].astype(jnp.bfloat16)

    own = pl.ds(pl.multiple_of(me * cown, cown), cown)

    chip, core = me // 2, lax.rem(me, 2)
    first, second = chip + 1 - 2 * lax.rem(chip, 2), n // 2 - 1 - chip
    gchan, cslice = chan // 2, chan // 4
    sides = (lax.rem((chip + 1) // 2, 2), chip // 2)

    def mate(t, g):
        return first if t == g else second

    def o_copy(t, p, s, g, far, src_core, dst_core, sending):
        other = 2 * (mate(t, g) if far else chip) + (dst_core if sending else src_core)
        src = me if sending else other
        buf = rb if t else ra
        k = (2 if far else 0)
        return pltpu.make_async_remote_copy(
            src_ref=snd.at[t, p, s, pl.ds(pl.multiple_of(g * gchan + (dst_core if sending else core) * cslice, cslice), cslice)],
            dst_ref=buf.at[g, p, slot(s, src)],
            send_sem=ss_o.at[t, p, s, g, k + (dst_core if sending else 0)], recv_sem=rs_o.at[t, p, s, g, k + (core if sending else src_core)],
            device_id={"dap": other}, device_id_type=MESH)

    def o_send(t, p, s):
        for g in range(2):
            for c in range(2):
                o_copy(t, p, s, g, True, core, c, True).start()
            o_copy(t, p, s, g, False, core, 1 - core, True).start()
            buf = rb if t else ra
            buf[g, p, slot(s, me)] = snd[t, p, s, pl.ds(pl.multiple_of(g * gchan + core * cslice, cslice), cslice)]

    def o_wait(t, p, s):
        for g in range(2):
            o_copy(t, p, s, g, False, 1 - core, core, False).wait_recv()
            for c in range(2):
                o_copy(t, p, s, g, True, c, core, False).wait_recv()

    def o_sent():
        for t in range(2):
            for p in range(2):
                for s in range(2):
                    for g in range(2):
                        for c in range(2):
                            o_copy(t, p, s, g, True, core, c, True).wait_send()
                        o_copy(t, p, s, g, False, core, 1 - core, True).wait_send()

    def xo_copy(p, g, far, src_core, dst_core, sending):
        other = 2 * (mate(0, g) if far else chip) + (dst_core if sending else src_core)
        dst = other if sending else me
        k = 2 if far else 0
        return pltpu.make_async_remote_copy(
            src_ref=xs.at[g, :, slot(p, dst)],
            dst_ref=xr.at[p, sides[g], pl.ds((g * 2 + (core if sending else src_core)) * 2, 2)],
            send_sem=ss_xo.at[p, g, k + (dst_core if sending else 0)], recv_sem=rs_xo.at[p, g, k + (core if sending else src_core)],
            device_id={"dap": other}, device_id_type=MESH)

    def xo_send(p):
        for g in range(2):
            for c in range(2):
                xo_copy(p, g, True, core, c, True).start()
            xo_copy(p, g, False, core, 1 - core, True).start()
            xr[p, sides[g], pl.ds((g * 2 + core) * 2, 2)] = xs[g, :, slot(p, me)]

    def xo_wait(p):
        for g in range(2):
            xo_copy(p, g, False, 1 - core, core, False).wait_recv()
            for c in range(2):
                xo_copy(p, g, True, c, core, False).wait_recv()

    def xo_sent():
        for p in range(2):
            for g in range(2):
                for c in range(2):
                    xo_copy(p, g, True, core, c, True).wait_send()
                xo_copy(p, g, False, core, 1 - core, True).wait_send()

    def x_out(p):
        for g in range(2):
            at = [slot(p, 2 * w + c) for w in (chip, mate(0, g)) for c in range(2)]
            for e in range(cslice // cown):
                @pl.loop(0, cown, unroll=2)
                def _(c, g=g, e=e, at=at):
                    k = e * cown + c
                    a = jnp.concatenate([jnp.concatenate([ra[g, h, d, k] for d in at], axis=0) for h in range(2)], axis=1)
                    b = jnp.concatenate([rb[g, h, :, k].reshape(lanes, lanes) for h in range(2)], axis=1)
                    x = lax.dot_general(a, b, (((1,), (1,)), ((), ())), preferred_element_type=jnp.float32).astype(jnp.bfloat16)
                    for m, d in enumerate(at):
                        xs[g, e, d, c] = x[m * jrows:(m + 1) * jrows]

    def parts(p):
        return ((0, cown),) if p == 0 else ((0, cown // 2), (cown // 2, cown // 2))

    def landing(t, p, s, src, e):
        lo, m = parts(p)[e]
        return obuf.at[t * 4 + p * 2 + s, pl.ds(pl.multiple_of(src * cown, cown) + lo, m)]

    def ab_copy(t, p, s, e, src, dst):
        lo, m = parts(p)[e]
        return pltpu.make_async_remote_copy(
            src_ref=snd.at[t, p, s, pl.ds(pl.multiple_of(dst * cown, cown) + lo, m)], dst_ref=landing(t, p, s, src, e),
            send_sem=ss_ab.at[t, p, s, e, dst], recv_sem=rs_ab.at[t, p, s, e, src],
            device_id={"dap": dst}, device_id_type=MESH)

    def ab_send(p, e, which=(0, 1)):
        lo, m = parts(p)[e]
        for s in which:
            for t in range(2):
                for d in range(1, n):
                    ab_copy(t, p, s, e, me, lax.rem(me + d, n)).start()
                obuf[t * 4 + p * 2 + s, pl.ds(pl.multiple_of(me * cown, cown) + lo, m)] = snd[t, p, s, pl.ds(pl.multiple_of(me * cown, cown) + lo, m)]

    def ab_wait(p, e):
        for t in range(2):
            for s in range(2):
                for d in range(1, n):
                    ab_copy(t, p, s, e, lax.rem(me + d, n), me).wait_recv()

    def ab_sent():
        for p in range(2):
            for e in range(len(parts(p))):
                for t in range(2):
                    for s in range(2):
                        for d in range(1, n):
                            ab_copy(t, p, s, e, me, lax.rem(me + d, n)).wait_send()

    hown = cown // 2

    def x_copy(p, e, src, dst):
        at = pl.ds(e * hown, hown)
        return pltpu.make_async_remote_copy(
            src_ref=xs.at[p, :, dst, at], dst_ref=xr.at[p, :, src, at],
            send_sem=ss_x.at[p, e, dst], recv_sem=rs_x.at[p, e, src],
            device_id={"dap": dst}, device_id_type=MESH)

    def x_send(p, e):
        for d in range(1, n):
            x_copy(p, e, me, lax.rem(me + d, n)).start()
        at = slice(e * hown, (e + 1) * hown)
        xr[p, :, me, at] = xs[p, :, me, at]

    def x_wait(p):
        for e in range(2):
            for d in range(1, n):
                x_copy(p, e, lax.rem(me + d, n), me).wait_recv()

    def x_sent():
        for p in range(2):
            for e in range(2):
                for d in range(1, n):
                    x_copy(p, e, me, lax.rem(me + d, n)).wait_send()

    def x_in(e):
        @pl.loop(e * hown, (e + 1) * hown)
        def _(c):
            a, b = (jnp.concatenate([
                jnp.concatenate([obuf[t * 4 + p * 2 + s, src * cown + c] for p in range(2) for src in range(n)], axis=0)
                for s in range(2)], axis=1) for t in range(2))
            x = lax.dot_general(a, b, (((0,), (0,)), ((), ())), preferred_element_type=jnp.float32)
            x = x.astype(jnp.bfloat16).reshape(2, n, jrows, cols)
            for p in range(2):
                v = turned(x[p], p)
                for h in range(2):
                    xs[p, h, :, c] = v[:, :, h * lanes:(h + 1) * lanes]

    half = chan * pxt

    def stage(u, p):
        lane = lax.broadcasted_iota(jnp.int32, (jrows, lanes), 1) // (lanes // 4)
        for k in range(n):
            take = ((lane == 0) | (lane == 3)) if k < n // 2 else (lane < 2)

            @pl.loop(0, cown, unroll=8)
            def _(c, k=k, take=take):
                x0, x1 = (xr[p, h, k, c].astype(jnp.float32) for h in range(2))
                if u == 0:
                    x0, x1 = jnp.where(take, x0, x1), jnp.where(take, x1, x0)
                for h, x in enumerate((x0, x1)):
                    fb[pl.ds(pl.multiple_of(h * half + (k * cown + c) * pxt, 8), jrows), :] = x

    def finish(u, p, steps, pieces):
        @pl.loop(0, steps)
        def _(i):
            at = [(p * jrows + r0 + i, h * lanes) for r0, h in pieces]
            x = jnp.concatenate([fb[pl.ds(h * half + r0 + i, chan, stride=pxt), :] for r0, h in pieces], axis=1)
            xscale = jnp.concatenate([nc[u, 2]] * 2, axis=1)
            xshift = jnp.concatenate([nc[u, 3]] * 2, axis=1)
            upd = jnp.dot(wo[u], _norm_rows(x, xscale, xshift), preferred_element_type=jnp.float32)
            new = [zb[r, :, h:h + lanes] + gb[r, :, h:h + lanes] * upd[:, k * lanes:(k + 1) * lanes] for k, (r, h) in enumerate(at)]
            if u == 0:
                for (r, h), v in zip(at, new):
                    zb[r, :, h:h + lanes] = v
            else:
                zi[at[0][0]] = jnp.stack([turned(v.T.reshape(n, jrows, chan), c) for c, v in enumerate(new)], axis=1).reshape(cols, chan)

    def ocopy(p):
        at = pl.ds(p * jrows, jrows)
        return pltpu.make_async_copy(zi.at[at], o_hbm.at[at], osem.at[p])

    project(0, 0)
    send_own(0, 0)
    project(0, 1)
    send_own(0, 1)
    project(1, 0)
    forward_far(0, 0)
    project(1, 1)
    prepare()
    forward_far(0, 1)
    send_own(1, 0)
    send_own(1, 1)
    forward_opp(0)
    partner_all(0)
    outer(0, 0, blocks)
    forward_far(1, 0)
    zcopy.wait()
    mix(0)
    forward_far(1, 1)
    piece_rows(0, jrows, ((0, 0, 0, 0), (jrows, 0, 1, 0)))
    turn(0)
    for t in (1, 0):
        for s in range(2):
            o_send(t, 0, s)
    forward_opp(1)
    partner_all(1)
    outer(1, 0, blocks)
    mix(1)
    piece_rows(0, jrows, ((0, 1, 0, 0), (jrows, 1, 1, 0)))
    turn(1)
    for t in (1, 0):
        for s in range(2):
            o_send(t, 1, s)
    for p in range(2):
        for s in range(2):
            o_wait(1, p, s)
    for p in range(2):
        o_wait(0, 0, p)
        o_wait(0, 1, p)
        x_out(p)
        xo_send(p)
    o_sent()
    hr = jrows // 2
    for p in range(2):
        xo_wait(p)
        stage(0, p)
        for h in range(2):
            finish(0, p, hr, ((0, h), (hr, h)))
            piece_rows(1, hr, ((p * jrows, h, h, 0), (p * jrows + hr, h, h, hr)))
            turn(p, (h,))
            if p == 0:
                ab_send(0, 0, (h,))
    for e in range(2):
        ab_send(1, e)
    xo_sent()
    ab_wait(0, 0)
    for e in range(2):
        ab_wait(1, e)
        x_in(e)
        for p in range(2):
            x_send(p, e)
    for p in range(2):
        x_wait(p)
        stage(1, p)
        finish(1, p, jrows, ((0, 0), (0, 1)))
        ocopy(p).start()
    for p in range(2):
        ocopy(p).wait()
    ab_sent()
    x_sent()
    for c in range(chunks):
        for h in (0, 1):
            for k, src in enumerate((me, me, me, left, right, opp)):
                send(c, h, src, k, part).wait_send()
            far(c, h, left, 0, right).wait_send()
            far(c, h, right, 1, left).wait_send()


def solution(mesh):
    row_spec = P(("data", "dap"), None, None)
    mask_spec = P(("data", "dap"), None)
    msa_spec = P(None, ("data", "dap"), None)
    replicated = P()

    def local_program(pair_loc, mask_loc, msa_loc, opm_norm, opm_proj, opm_out, opm_bias, tri_norm, tri_proj, tri_gate, tri_xnorm, tri_out):
        n = lax.axis_size("dap")
        rows, cols, chan = pair_loc.shape
        depth, _, mdim = msa_loc.shape
        odim = opm_proj.shape[1] // 2
        grp, chunks = 8, 2
        lanes = cols // chunks
        jrows = rows // chunks
        cown = chan // n
        vm = pl.BlockSpec(memory_space=pltpu.VMEM)
        hbm = pl.BlockSpec(memory_space=pl.ANY)
        f32, bf16 = jnp.float32, jnp.bfloat16
        dma = pltpu.SemaphoreType.DMA
        staged = max(4 * jrows * (chan + 8), depth // LANES * jrows * (odim + 8))
        return pl.pallas_call(
            functools.partial(_kernel, n),
            out_shape=jax.ShapeDtypeStruct(pair_loc.shape, f32),
            in_specs=[hbm, vm, hbm] + [vm] * 9,
            out_specs=hbm,
            scratch_shapes=[
                pltpu.VMEM((2, depth, grp, mdim), bf16),
                pltpu.VMEM((max(depth * grp, 2 * chan * (jrows + 8)), LANES), f32),
                pltpu.VMEM((rows * odim, depth), bf16),
                pltpu.VMEM((chunks, 2, n, odim, jrows, depth // 2), bf16),
                pltpu.VMEM((odim // 2, 2 * rows * odim // TILE, TILE, lanes), bf16),
                pltpu.VMEM((rows, cols, chan), f32),
                pltpu.VMEM((rows, chan, cols), f32),
                pltpu.VMEM((rows, chan, cols), f32),
                pltpu.VMEM((staged, LANES), f32),
                pltpu.VMEM((2, 2, 2, chan, jrows, lanes), bf16),
                pltpu.VMEM((2, 2, n, chan // 4, jrows, lanes), bf16),
                pltpu.VMEM((2, 2, n, chan // 4, jrows, lanes), bf16),
                pltpu.VMEM((2, 2, n, cown, jrows, lanes), bf16),
                pltpu.VMEM((2, 2, n, cown, jrows, lanes), bf16),
                pltpu.VMEM((rows, cols), f32),
                pltpu.VMEM((chan, odim * odim), bf16),
                pltpu.VMEM((2, 5 * chan, chan), bf16),
                pltpu.VMEM((2, chan, chan), bf16),
                pltpu.VMEM((2, 4, chan, lanes), f32),
                pltpu.VMEM((chan, lanes), f32),
                dma((2,)), dma((1,)), dma((2,)),
                dma((chunks, 2, 8)), dma((chunks, 2, n)), dma((chunks, 2, 2)),
                dma((2, 2, 2, 2, 4)), dma((2, 2, 2, 2, 4)), dma((2, 2, 4)), dma((2, 2, 4)),
                dma((2, 2, 2, 2, n)), dma((2, 2, 2, 2, n)), dma((2, 2, n)), dma((2, 2, n)),
            ],
            compiler_params=pltpu.CompilerParams(collective_id=0, has_side_effects=True, vmem_limit_bytes=63 * 1024 * 1024),
            name="pair_stack",
        )(pair_loc, mask_loc, msa_loc, opm_norm, opm_proj.T, opm_out, opm_bias.reshape(1, chan), tri_norm, tri_proj, tri_gate, tri_xnorm, tri_out)

    return jax.shard_map(local_program, mesh=mesh, in_specs=(row_spec, mask_spec, msa_spec) + (replicated,) * 9, out_specs=row_spec, check_vma=False)
```

```python
import functools

import jax
import jax.numpy as jnp
from jax import lax
from jax.experimental import pallas as pl
from jax.experimental.pallas import tpu as pltpu
from jax.sharding import PartitionSpec as P

LN_EPS = 1e-5
LANES = 128
TILE = 16
MESH = pl.DeviceIdType.MESH


def _norm_rows(v, scale, shift):
    mean = jnp.mean(v, axis=0, keepdims=True)
    cen = v - mean
    var = jnp.mean(cen * cen, axis=0, keepdims=True)
    return (cen * lax.rsqrt(var + LN_EPS) * scale + shift).astype(jnp.bfloat16)


def _column(row, n):
    return jnp.broadcast_to(row, (n, row.shape[1])).T


def _kernel(n, z_hbm, mask_ref, msa_hbm, onrm_ref, oproj_ref, oout_ref, obias_ref, nrm_ref, proj_ref, gate_ref, xnrm_ref, out_ref, o_hbm,
            mb, fb, at_b, ball, obuf, zi, zb, gb, st, snd, ra, rb, xs, xr, mk, wt, wa, wo, nc, bc,
            msem, zsem, osem, ss, rs, rf, ss_o, rs_o, ss_xo, rs_xo, ss_ab, rs_ab, ss_x, rs_x):
    me = lax.axis_index("dap")
    depth, _, mdim = mb.shape
    rows, cols, chan = zi.shape
    chunks, lanes, jrows, odim = 2, cols // 2, rows // 2, ball.shape[3]
    grp = 8
    per = jrows // grp
    mblocks = msem.shape[0]
    qh = odim // 2
    cown = chan // n
    blocks = odim // 2
    bst, pst, pxt = odim + 8, chan + 8, jrows + 8
    part = me + 1 - 2 * lax.rem(me, 2)
    right, left, opp = lax.rem(me + 2, n), lax.rem(me + n - 2, n), lax.rem(me + 4, n)

    def mcopy(g):
        at = pl.ds(g * (depth // mblocks), depth // mblocks)
        return pltpu.make_async_copy(msa_hbm.at[at], mb.at[at], msem.at[g])

    for g in range(mblocks):
        mcopy(g).start()
    zcopy = pltpu.make_async_copy(z_hbm, zi, zsem.at[0])
    barrier = pltpu.get_barrier_semaphore()
    for s in range(1, n):
        pl.semaphore_signal(barrier, inc=1, device_id={"dap": lax.rem(me + s, n)}, device_id_type=MESH)
    pl.semaphore_wait(barrier, n - 1)

    def slot(c, dev):
        return lax.rem(dev + c * (n // 2), n)

    def turned(v, c):
        return v if c == 0 else jnp.concatenate([v[n // 2:], v[:n // 2]], axis=0)

    def block(c, h, src):
        return ball.at[c, h, slot(c, src)]

    def send(c, h, src, k, dst):
        return pltpu.make_async_remote_copy(
            src_ref=block(c, h, src), dst_ref=block(c, h, src), send_sem=ss.at[c, h, k], recv_sem=rs.at[c, h, src],
            device_id={"dap": dst}, device_id_type=MESH)

    def arrived(c, h, src):
        send(c, h, src, 0, part).wait_recv()

    def far(c, h, src, k, dst):
        at = ball.at[c, h, slot(c, src), k * qh:(k + 1) * qh]
        return pltpu.make_async_remote_copy(
            src_ref=at, dst_ref=at, send_sem=ss.at[c, h, 6 + k], recv_sem=rf.at[c, h, k],
            device_id={"dap": dst}, device_id_type=MESH)

    oscale, oshift = onrm_ref[0:1, :], onrm_ref[1:2, :]
    sb = 32
    hdep = depth // 2
    tiles = hdep // LANES

    def project(c, h):
        section = hdep * grp
        if c == 0:
            for g in range(h * mblocks // 2, (h + 1) * mblocks // 2):
                mcopy(g).wait()

        @pl.loop(0, hdep // sb)
        def _(b):
            x = mb[pl.ds(h * hdep + b * sb, sb), c * jrows:(c + 1) * jrows].astype(jnp.float32).reshape(sb * jrows, mdim)
            mean = jnp.mean(x, axis=1, keepdims=True)
            cen = x - mean
            var = jnp.mean(cen * cen, axis=1, keepdims=True)
            y = (cen * lax.rsqrt(var + LN_EPS) * oscale + oshift).astype(jnp.bfloat16)
            v = lax.dot_general(y, oproj_ref[...], (((1,), (1,)), ((), ())), preferred_element_type=jnp.float32)
            v = v.reshape(sb, per, grp, 2 * odim)
            for k in range(per):
                at = pl.ds(pl.multiple_of(k * section + b * (sb * grp), sb * grp), sb * grp)
                fb[at, :2 * odim] = v[:, k].reshape(sb * grp, 2 * odim)

        for k in range(per):
            @pl.loop(0, grp)
            def _(i, k=k):
                v = fb[pl.ds(k * section + i, hdep, stride=grp), :].T
                r = (c * per + k) * grp + i
                at_b[pl.ds(pl.multiple_of(r * odim, odim), odim), h * hdep:(h + 1) * hdep] = v[:odim].astype(jnp.bfloat16)
                for t in range(tiles):
                    row = pl.multiple_of(t * (jrows * bst) + (k * grp + i) * bst, 8)
                    st[pl.ds(row, odim), :] = v[odim:2 * odim, t * LANES:(t + 1) * LANES]

        @pl.loop(0, odim, unroll=4)
        def _(q):
            for t in range(tiles):
                ball[c, h, slot(c, me), q, :, t * LANES:(t + 1) * LANES] = (
                    st[pl.ds(t * (jrows * bst) + q, jrows, stride=bst), :].astype(jnp.bfloat16))

    def send_own(c, h):
        for k, dst in enumerate((right, left, part)):
            send(c, h, me, k, dst).start()

    def forward_far(c, h):
        for k, (src, dst) in enumerate(((left, right), (right, left))):
            arrived(c, h, src)
            far(c, h, src, k, dst).start()
            send(c, h, src, 3 + k, part).start()

    def forward_opp(c):
        for h in (0, 1):
            for k in (0, 1):
                far(c, h, opp, k, part).wait_recv()
            send(c, h, opp, 5, part).start()

    def partner_all(c):
        for d in (0, 2, 4, 6):
            for h in (0, 1):
                arrived(c, h, lax.rem(part + d, n))

    def outer(c, lo, hi):
        @pl.loop(lo, hi)
        def _(b):
            rhs = jnp.concatenate([jnp.concatenate([ball[c, h, :, b * 2 + t].reshape(lanes, hdep) for h in range(2)], axis=1) for t in range(2)], axis=0)
            o = lax.dot_general(at_b[...], rhs, (((1,), (1,)), ((), ())), preferred_element_type=jnp.float32)
            o = (o * (1.0 / depth)).astype(jnp.bfloat16)
            nt = rows * odim // TILE
            for t in range(2):
                obuf[b, t * nt:(t + 1) * nt] = o[:, t * lanes:(t + 1) * lanes].reshape(nt, TILE, lanes)

    def mix(c, lo, hi):
        @pl.loop(lo, hi, unroll=2)
        def _(i):
            nt, w = rows * odim // TILE, odim // TILE
            rhs = jnp.stack([obuf[:, pl.ds(t * nt + i * w, w)] for t in range(2)], axis=1).reshape(odim * odim, lanes)
            upd = jnp.dot(wt[...], rhs, preferred_element_type=jnp.float32)
            zt = turned(zi[i].reshape(n, chunks, jrows, chan)[:, c], c).reshape(lanes, chan).T
            zb[i, :, c * lanes:(c + 1) * lanes] = zt + (upd + bc[...])

    def prepare():
        rid = lax.broadcasted_iota(jnp.int32, (cols, cols), 0)
        cid = lax.broadcasted_iota(jnp.int32, (cols, cols), 1)
        two = chunks * jrows
        piece = (rid // jrows) % chunks
        place = piece * lanes + ((rid // two + piece * (n // 2)) % n) * jrows + rid % jrows
        perm = (cid == place).astype(jnp.float32).astype(jnp.bfloat16)
        mk[...] = jnp.dot(mask_ref[...].astype(jnp.float32).astype(jnp.bfloat16), perm, preferred_element_type=jnp.float32)
        bc[...] = _column(obias_ref[...], lanes)
        for t in range(2):
            for k in range(2):
                nc[t, k] = _column(nrm_ref[t, k:k + 1, :], lanes)
                nc[t, 2 + k] = _column(xnrm_ref[t, k:k + 1, :], lanes)
            for k in range(4):
                wa[t, k * chan:(k + 1) * chan] = proj_ref[t, :, k * chan:(k + 1) * chan].astype(jnp.float32).T.astype(jnp.bfloat16)
            wa[t, 4 * chan:] = gate_ref[t].astype(jnp.float32).T.astype(jnp.bfloat16)
            wo[t] = out_ref[t].astype(jnp.float32).T.astype(jnp.bfloat16)
        fb[:odim * odim, :] = oout_ref[...].astype(jnp.float32)

        @pl.loop(0, odim * odim // LANES)
        def _(b):
            m = LANES // odim
            v = jnp.concatenate([fb[pl.ds(b * m + k, odim, stride=odim), :] for k in range(m)], axis=0)
            wt[:, pl.ds(pl.multiple_of(b * LANES, LANES), LANES)] = v.T.astype(jnp.bfloat16)

    def piece_rows(u, steps, pieces):
        @pl.loop(0, steps)
        def _(i):
            at = [(r0 + i, h * lanes) for r0, h, _, _ in pieces]
            z = jnp.concatenate([zb[r, :, h:h + lanes] for r, h in at], axis=1)
            m = jnp.concatenate([mk[pl.ds(r, 1), :][:, h:h + lanes] for r, h in at], axis=1)
            scale = jnp.concatenate([nc[u, 0]] * 2, axis=1)
            shift = jnp.concatenate([nc[u, 1]] * 2, axis=1)
            q = jnp.dot(wa[u], _norm_rows(z, scale, shift), preferred_element_type=jnp.float32)
            ab = (m * jax.nn.sigmoid(q[chan:2 * chan]) * q[:chan], m * jax.nn.sigmoid(q[3 * chan:4 * chan]) * q[2 * chan:3 * chan])
            g = jax.nn.sigmoid(q[4 * chan:])
            for s, (r, h) in enumerate(at):
                gb[r, :, h:h + lanes] = g[:, s * lanes:(s + 1) * lanes]
                for t in range(2):
                    row = pl.multiple_of((t * 2 + pieces[s][2]) * (jrows * pst) + (i + pieces[s][3]) * pst, 8)
                    st[pl.ds(row, chan), :] = ab[t][:, s * lanes:(s + 1) * lanes]

    def turn(p, which=(0, 1)):
        @pl.loop(0, chan, unroll=8)
        def _(c):
            for t in range(2):
                for s in which:
                    snd[t, p, s, c] = st[pl.ds((t * 2 + s) * (jrows * pst) + c, jrows, stride=pst), :].astype(jnp.bfloat16)

    own = pl.ds(pl.multiple_of(me * cown, cown), cown)

    chip, core = me // 2, lax.rem(me, 2)
    first, second = chip + 1 - 2 * lax.rem(chip, 2), n // 2 - 1 - chip
    gchan, cslice = chan // 2, chan // 4
    sides = (lax.rem((chip + 1) // 2, 2), chip // 2)

    def mate(t, g):
        return first if t == g else second

    def o_copy(t, p, s, g, far, src_core, dst_core, sending):
        other = 2 * (mate(t, g) if far else chip) + (dst_core if sending else src_core)
        src = me if sending else other
        buf = rb if t else ra
        k = (2 if far else 0)
        return pltpu.make_async_remote_copy(
            src_ref=snd.at[t, p, s, pl.ds(pl.multiple_of(g * gchan + (dst_core if sending else core) * cslice, cslice), cslice)],
            dst_ref=buf.at[g, p, slot(s, src)],
            send_sem=ss_o.at[t, p, s, g, k + (dst_core if sending else 0)], recv_sem=rs_o.at[t, p, s, g, k + (core if sending else src_core)],
            device_id={"dap": other}, device_id_type=MESH)

    def o_send(t, p, s):
        for g in range(2):
            for c in range(2):
                o_copy(t, p, s, g, True, core, c, True).start()
            o_copy(t, p, s, g, False, core, 1 - core, True).start()
            buf = rb if t else ra
            buf[g, p, slot(s, me)] = snd[t, p, s, pl.ds(pl.multiple_of(g * gchan + core * cslice, cslice), cslice)]

    def o_wait(t, p, s):
        for g in range(2):
            o_copy(t, p, s, g, False, 1 - core, core, False).wait_recv()
            for c in range(2):
                o_copy(t, p, s, g, True, c, core, False).wait_recv()

    def o_sent():
        for t in range(2):
            for p in range(2):
                for s in range(2):
                    for g in range(2):
                        for c in range(2):
                            o_copy(t, p, s, g, True, core, c, True).wait_send()
                        o_copy(t, p, s, g, False, core, 1 - core, True).wait_send()

    def xo_copy(p, g, far, src_core, dst_core, sending):
        other = 2 * (mate(0, g) if far else chip) + (dst_core if sending else src_core)
        dst = other if sending else me
        k = 2 if far else 0
        return pltpu.make_async_remote_copy(
            src_ref=xs.at[g, :, slot(p, dst)],
            dst_ref=xr.at[p, sides[g], pl.ds((g * 2 + (core if sending else src_core)) * 2, 2)],
            send_sem=ss_xo.at[p, g, k + (dst_core if sending else 0)], recv_sem=rs_xo.at[p, g, k + (core if sending else src_core)],
            device_id={"dap": other}, device_id_type=MESH)

    def xo_send(p):
        for g in range(2):
            for c in range(2):
                xo_copy(p, g, True, core, c, True).start()
            xo_copy(p, g, False, core, 1 - core, True).start()
            xr[p, sides[g], pl.ds((g * 2 + core) * 2, 2)] = xs[g, :, slot(p, me)]

    def xo_wait(p):
        for g in range(2):
            xo_copy(p, g, False, 1 - core, core, False).wait_recv()
            for c in range(2):
                xo_copy(p, g, True, c, core, False).wait_recv()

    def xo_sent():
        for p in range(2):
            for g in range(2):
                for c in range(2):
                    xo_copy(p, g, True, core, c, True).wait_send()
                xo_copy(p, g, False, core, 1 - core, True).wait_send()

    def x_out(p):
        for g in range(2):
            at = [slot(p, 2 * w + c) for w in (chip, mate(0, g)) for c in range(2)]
            for e in range(cslice // cown):
                @pl.loop(0, cown, unroll=2)
                def _(c, g=g, e=e, at=at):
                    k = e * cown + c
                    a = jnp.concatenate([jnp.concatenate([ra[g, h, d, k] for d in at], axis=0) for h in range(2)], axis=1)
                    b = jnp.concatenate([rb[g, h, :, k].reshape(lanes, lanes) for h in range(2)], axis=1)
                    x = lax.dot_general(a, b, (((1,), (1,)), ((), ())), preferred_element_type=jnp.float32).astype(jnp.bfloat16)
                    for m, d in enumerate(at):
                        xs[g, e, d, c] = x[m * jrows:(m + 1) * jrows]

    def parts(p):
        return ((0, cown),) if p == 0 else ((0, cown // 2), (cown // 2, cown // 2))

    def landing(t, p, s, src, e):
        lo, m = parts(p)[e]
        return obuf.at[t * 4 + p * 2 + s, pl.ds(pl.multiple_of(src * cown, cown) + lo, m)]

    def ab_copy(t, p, s, e, src, dst):
        lo, m = parts(p)[e]
        return pltpu.make_async_remote_copy(
            src_ref=snd.at[t, p, s, pl.ds(pl.multiple_of(dst * cown, cown) + lo, m)], dst_ref=landing(t, p, s, src, e),
            send_sem=ss_ab.at[t, p, s, e, dst], recv_sem=rs_ab.at[t, p, s, e, src],
            device_id={"dap": dst}, device_id_type=MESH)

    def ab_send(p, e, which=(0, 1)):
        lo, m = parts(p)[e]
        for s in which:
            for t in range(2):
                for d in range(1, n):
                    ab_copy(t, p, s, e, me, lax.rem(me + d, n)).start()
                obuf[t * 4 + p * 2 + s, pl.ds(pl.multiple_of(me * cown, cown) + lo, m)] = snd[t, p, s, pl.ds(pl.multiple_of(me * cown, cown) + lo, m)]

    def ab_wait(p, e):
        for t in range(2):
            for s in range(2):
                for d in range(1, n):
                    ab_copy(t, p, s, e, lax.rem(me + d, n), me).wait_recv()

    def ab_sent():
        for p in range(2):
            for e in range(len(parts(p))):
                for t in range(2):
                    for s in range(2):
                        for d in range(1, n):
                            ab_copy(t, p, s, e, me, lax.rem(me + d, n)).wait_send()

    hown = cown // 2

    def x_copy(p, e, src, dst):
        at = pl.ds(e * hown, hown)
        return pltpu.make_async_remote_copy(
            src_ref=xs.at[p, :, dst, at], dst_ref=xr.at[p, :, src, at],
            send_sem=ss_x.at[p, e, dst], recv_sem=rs_x.at[p, e, src],
            device_id={"dap": dst}, device_id_type=MESH)

    def x_send(p, e):
        for d in range(1, n):
            x_copy(p, e, me, lax.rem(me + d, n)).start()
        at = slice(e * hown, (e + 1) * hown)
        xr[p, :, me, at] = xs[p, :, me, at]

    def x_wait(p):
        for e in range(2):
            for d in range(1, n):
                x_copy(p, e, lax.rem(me + d, n), me).wait_recv()

    def x_sent():
        for p in range(2):
            for e in range(2):
                for d in range(1, n):
                    x_copy(p, e, me, lax.rem(me + d, n)).wait_send()

    def x_in(e):
        @pl.loop(e * hown, (e + 1) * hown)
        def _(c):
            a, b = (jnp.concatenate([
                jnp.concatenate([obuf[t * 4 + p * 2 + s, src * cown + c] for p in range(2) for src in range(n)], axis=0)
                for s in range(2)], axis=1) for t in range(2))
            x = lax.dot_general(a, b, (((0,), (0,)), ((), ())), preferred_element_type=jnp.float32)
            x = x.astype(jnp.bfloat16).reshape(2, n, jrows, cols)
            for p in range(2):
                v = turned(x[p], p)
                for h in range(2):
                    xs[p, h, :, c] = v[:, :, h * lanes:(h + 1) * lanes]

    half = chan * pxt

    def stage(u, p):
        lane = lax.broadcasted_iota(jnp.int32, (jrows, lanes), 1) // (lanes // 4)
        for k in range(n):
            take = ((lane == 0) | (lane == 3)) if k < n // 2 else (lane < 2)

            @pl.loop(0, cown, unroll=8)
            def _(c, k=k, take=take):
                x0, x1 = (xr[p, h, k, c].astype(jnp.float32) for h in range(2))
                if u == 0:
                    x0, x1 = jnp.where(take, x0, x1), jnp.where(take, x1, x0)
                for h, x in enumerate((x0, x1)):
                    fb[pl.ds(pl.multiple_of(h * half + (k * cown + c) * pxt, 8), jrows), :] = x

    def finish(u, p, steps, pieces):
        @pl.loop(0, steps)
        def _(i):
            at = [(p * jrows + r0 + i, h * lanes) for r0, h in pieces]
            x = jnp.concatenate([fb[pl.ds(h * half + r0 + i, chan, stride=pxt), :] for r0, h in pieces], axis=1)
            xscale = jnp.concatenate([nc[u, 2]] * 2, axis=1)
            xshift = jnp.concatenate([nc[u, 3]] * 2, axis=1)
            upd = jnp.dot(wo[u], _norm_rows(x, xscale, xshift), preferred_element_type=jnp.float32)
            new = [zb[r, :, h:h + lanes] + gb[r, :, h:h + lanes] * upd[:, k * lanes:(k + 1) * lanes] for k, (r, h) in enumerate(at)]
            if u == 0:
                for (r, h), v in zip(at, new):
                    zb[r, :, h:h + lanes] = v
            else:
                zi[at[0][0]] = jnp.stack([turned(v.T.reshape(n, jrows, chan), c) for c, v in enumerate(new)], axis=1).reshape(cols, chan)

    def ocopy(p):
        at = pl.ds(p * jrows, jrows)
        return pltpu.make_async_copy(zi.at[at], o_hbm.at[at], osem.at[p])

    project(0, 0)
    send_own(0, 0)
    project(0, 1)
    send_own(0, 1)
    zcopy.start()
    project(1, 0)
    forward_far(0, 0)
    project(1, 1)
    prepare()
    forward_far(0, 1)
    send_own(1, 0)
    send_own(1, 1)
    forward_opp(0)
    partner_all(0)
    outer(0, 0, blocks * 3 // 8)
    forward_far(1, 0)
    outer(0, blocks * 3 // 8, blocks)
    zcopy.wait()
    mix(0, 0, rows // 2)
    forward_far(1, 1)
    mix(0, rows // 2, rows)
    piece_rows(0, jrows, ((0, 0, 0, 0), (jrows, 0, 1, 0)))
    turn(0)
    for t in (1, 0):
        for s in range(2):
            o_send(t, 0, s)
    forward_opp(1)
    partner_all(1)
    outer(1, 0, blocks)
    mix(1, 0, rows)
    piece_rows(0, jrows, ((0, 1, 0, 0), (jrows, 1, 1, 0)))
    turn(1)
    for t in (1, 0):
        for s in range(2):
            o_send(t, 1, s)
    for p in range(2):
        for s in range(2):
            o_wait(1, p, s)
    for p in range(2):
        o_wait(0, 0, p)
        o_wait(0, 1, p)
        x_out(p)
        xo_send(p)
    o_sent()
    hr = jrows // 2
    for p in range(2):
        xo_wait(p)
        stage(0, p)
        for h in range(2):
            finish(0, p, hr, ((0, h), (hr, h)))
            piece_rows(1, hr, ((p * jrows, h, h, 0), (p * jrows + hr, h, h, hr)))
            turn(p, (h,))
            if p == 0:
                ab_send(0, 0, (h,))
    for e in range(2):
        ab_send(1, e)
    xo_sent()
    ab_wait(0, 0)
    for e in range(2):
        ab_wait(1, e)
        x_in(e)
        for p in range(2):
            x_send(p, e)
    for p in range(2):
        x_wait(p)
        stage(1, p)
        finish(1, p, jrows, ((0, 0), (0, 1)))
        ocopy(p).start()
    for p in range(2):
        ocopy(p).wait()
    ab_sent()
    x_sent()
    for c in range(chunks):
        for h in (0, 1):
            for k, src in enumerate((me, me, me, left, right, opp)):
                send(c, h, src, k, part).wait_send()
            far(c, h, left, 0, right).wait_send()
            far(c, h, right, 1, left).wait_send()


def solution(mesh):
    row_spec = P(("data", "dap"), None, None)
    mask_spec = P(("data", "dap"), None)
    msa_spec = P(None, ("data", "dap"), None)
    replicated = P()

    def local_program(pair_loc, mask_loc, msa_loc, opm_norm, opm_proj, opm_out, opm_bias, tri_norm, tri_proj, tri_gate, tri_xnorm, tri_out):
        n = lax.axis_size("dap")
        rows, cols, chan = pair_loc.shape
        depth, _, mdim = msa_loc.shape
        odim = opm_proj.shape[1] // 2
        chunks = 2
        lanes = cols // chunks
        jrows = rows // chunks
        cown = chan // n
        vm = pl.BlockSpec(memory_space=pltpu.VMEM)
        hbm = pl.BlockSpec(memory_space=pl.ANY)
        f32, bf16 = jnp.float32, jnp.bfloat16
        dma = pltpu.SemaphoreType.DMA
        staged = max(4 * jrows * (chan + 8), depth // LANES * jrows * (odim + 8))
        return pl.pallas_call(
            functools.partial(_kernel, n),
            out_shape=jax.ShapeDtypeStruct(pair_loc.shape, f32),
            in_specs=[hbm, vm, hbm] + [vm] * 9,
            out_specs=hbm,
            scratch_shapes=[
                pltpu.VMEM((depth, rows, mdim), bf16),
                pltpu.VMEM((max(depth // 2 * jrows, 2 * chan * (jrows + 8)), LANES), f32),
                pltpu.VMEM((rows * odim, depth), bf16),
                pltpu.VMEM((chunks, 2, n, odim, jrows, depth // 2), bf16),
                pltpu.VMEM((odim // 2, 2 * rows * odim // TILE, TILE, lanes), bf16),
                pltpu.VMEM((rows, cols, chan), f32),
                pltpu.VMEM((rows, chan, cols), f32),
                pltpu.VMEM((rows, chan, cols), f32),
                pltpu.VMEM((staged, LANES), f32),
                pltpu.VMEM((2, 2, 2, chan, jrows, lanes), bf16),
                pltpu.VMEM((2, 2, n, chan // 4, jrows, lanes), bf16),
                pltpu.VMEM((2, 2, n, chan // 4, jrows, lanes), bf16),
                pltpu.VMEM((2, 2, n, cown, jrows, lanes), bf16),
                pltpu.VMEM((2, 2, n, cown, jrows, lanes), bf16),
                pltpu.VMEM((rows, cols), f32),
                pltpu.VMEM((chan, odim * odim), bf16),
                pltpu.VMEM((2, 5 * chan, chan), bf16),
                pltpu.VMEM((2, chan, chan), bf16),
                pltpu.VMEM((2, 4, chan, lanes), f32),
                pltpu.VMEM((chan, lanes), f32),
                dma((8,)), dma((1,)), dma((2,)),
                dma((chunks, 2, 8)), dma((chunks, 2, n)), dma((chunks, 2, 2)),
                dma((2, 2, 2, 2, 4)), dma((2, 2, 2, 2, 4)), dma((2, 2, 4)), dma((2, 2, 4)),
                dma((2, 2, 2, 2, n)), dma((2, 2, 2, 2, n)), dma((2, 2, n)), dma((2, 2, n)),
            ],
            compiler_params=pltpu.CompilerParams(collective_id=0, has_side_effects=True, vmem_limit_bytes=67043328),
            name="pair_stack",
        )(pair_loc, mask_loc, msa_loc, opm_norm, opm_proj.T, opm_out, opm_bias.reshape(1, chan), tri_norm, tri_proj, tri_gate, tri_xnorm, tri_out)

    return jax.shard_map(local_program, mesh=mesh, in_specs=(row_spec, mask_spec, msa_spec) + (replicated,) * 9, out_specs=row_spec, check_vma=False)
```

```python
import functools

import jax
import jax.numpy as jnp
from jax import lax
from jax.experimental import pallas as pl
from jax.experimental.pallas import tpu as pltpu
from jax.sharding import PartitionSpec as P

LN_EPS = 1e-5
LANES = 128
TILE = 16
MESH = pl.DeviceIdType.MESH


def _norm_rows(v, scale, shift):
    mean = jnp.mean(v, axis=0, keepdims=True)
    cen = v - mean
    var = jnp.mean(cen * cen, axis=0, keepdims=True)
    return (cen * lax.rsqrt(var + LN_EPS) * scale + shift).astype(jnp.bfloat16)


def _column(row, n):
    return jnp.broadcast_to(row, (n, row.shape[1])).T


def _kernel(n, z_hbm, mask_hbm, msa_hbm, onrm_hbm, oproj_hbm, oout_hbm, obias_hbm, nrm_hbm, proj_hbm, gate_hbm, xnrm_hbm, out_hbm, o_hbm,
            mask_ref, onrm_ref, oproj_ref, oout_ref, obias_ref, nrm_ref, proj_ref, gate_ref, xnrm_ref, out_ref,
            mb, fb, at_b, ball, obuf, zi, zb, gb, st, snd, ra, rb, xs, xr, mk, wt, wa, wo, nc, bc,
            wsem, msem, zsem, osem, ss, rs, rf, ss_o, rs_o, ss_xo, rs_xo, ss_ab, rs_ab, ss_x, rs_x):
    me = lax.axis_index("dap")
    depth, _, mdim = mb.shape
    rows, chan, cols = zb.shape
    chunks, lanes, jrows, odim = 2, cols // 2, rows // 2, ball.shape[3]
    grp = 8
    per = jrows // grp
    mblocks = msem.shape[0]
    qh = odim // 2
    cown = chan // n
    blocks = odim // 2
    bst, pst, pxt = odim + 8, chan + 8, jrows + 8
    part = me + 1 - 2 * lax.rem(me, 2)
    right, left, opp = lax.rem(me + 2, n), lax.rem(me + n - 2, n), lax.rem(me + 4, n)

    def mcopy(g):
        at = pl.ds(g * (depth // mblocks), depth // mblocks)
        return pltpu.make_async_copy(msa_hbm.at[at], mb.at[at], msem.at[g])

    smalls = [pltpu.make_async_copy(a, b, wsem.at[k]) for k, (a, b) in enumerate((
        (onrm_hbm, onrm_ref), (oproj_hbm, oproj_ref), (mask_hbm, mask_ref), (oout_hbm, oout_ref), (obias_hbm, obias_ref),
        (nrm_hbm, nrm_ref), (proj_hbm, proj_ref), (gate_hbm, gate_ref), (xnrm_hbm, xnrm_ref), (out_hbm, out_ref)))]
    for copy in smalls[:2]:
        copy.start()
    for g in range(mblocks):
        mcopy(g).start()
    for copy in smalls[2:]:
        copy.start()
    zcopy = pltpu.make_async_copy(z_hbm, zi, zsem.at[0])
    barrier = pltpu.get_barrier_semaphore()
    for s in range(1, n):
        pl.semaphore_signal(barrier, inc=1, device_id={"dap": lax.rem(me + s, n)}, device_id_type=MESH)
    for copy in smalls[:2]:
        copy.wait()

    def slot(c, dev):
        return lax.rem(dev + c * (n // 2), n)

    def turned(v, c):
        return v if c == 0 else jnp.concatenate([v[n // 2:], v[:n // 2]], axis=0)

    def block(c, h, src):
        return ball.at[c, h, slot(c, src)]

    def send(c, h, src, k, dst):
        return pltpu.make_async_remote_copy(
            src_ref=block(c, h, src), dst_ref=block(c, h, src), send_sem=ss.at[c, h, k], recv_sem=rs.at[c, h, src],
            device_id={"dap": dst}, device_id_type=MESH)

    def arrived(c, h, src):
        send(c, h, src, 0, part).wait_recv()

    def far(c, h, src, k, dst):
        at = ball.at[c, h, slot(c, src), k * qh:(k + 1) * qh]
        return pltpu.make_async_remote_copy(
            src_ref=at, dst_ref=at, send_sem=ss.at[c, h, 6 + k], recv_sem=rf.at[c, h, k],
            device_id={"dap": dst}, device_id_type=MESH)

    oscale, oshift = onrm_ref[0:1, :], onrm_ref[1:2, :]
    sb = 32
    hdep = depth // 2
    tiles = hdep // LANES

    def project(c, h):
        section = hdep * grp
        @pl.loop(0, hdep // sb)
        def _(b):
            if c == 0:
                mcopy(h * (hdep // sb) + b).wait()
            x = mb[pl.ds(h * hdep + b * sb, sb), c * jrows:(c + 1) * jrows].astype(jnp.float32).reshape(sb * jrows, mdim)
            mean = jnp.mean(x, axis=1, keepdims=True)
            cen = x - mean
            var = jnp.mean(cen * cen, axis=1, keepdims=True)
            y = (cen * lax.rsqrt(var + LN_EPS) * oscale + oshift).astype(jnp.bfloat16)
            v = lax.dot_general(y, oproj_ref[...], (((1,), (1,)), ((), ())), preferred_element_type=jnp.float32)
            v = v.reshape(sb, per, grp, 2 * odim)
            for k in range(per):
                at = pl.ds(pl.multiple_of(k * section + b * (sb * grp), sb * grp), sb * grp)
                fb[at, :2 * odim] = v[:, k].reshape(sb * grp, 2 * odim)

        for k in range(per):
            @pl.loop(0, grp)
            def _(i, k=k):
                v = fb[pl.ds(k * section + i, hdep, stride=grp), :].T
                r = (c * per + k) * grp + i
                at_b[pl.ds(pl.multiple_of(r * odim, odim), odim), h * hdep:(h + 1) * hdep] = v[:odim].astype(jnp.bfloat16)
                for t in range(tiles):
                    row = pl.multiple_of(t * (jrows * bst) + (k * grp + i) * bst, 8)
                    st[pl.ds(row, odim), :] = v[odim:2 * odim, t * LANES:(t + 1) * LANES]

        @pl.loop(0, odim, unroll=4)
        def _(q):
            for t in range(tiles):
                ball[c, h, slot(c, me), q, :, t * LANES:(t + 1) * LANES] = (
                    st[pl.ds(t * (jrows * bst) + q, jrows, stride=bst), :].astype(jnp.bfloat16))

    def send_own(c, h):
        for k, dst in enumerate((right, left, part)):
            send(c, h, me, k, dst).start()

    def forward_far(c, h):
        for k, (src, dst) in enumerate(((left, right), (right, left))):
            arrived(c, h, src)
            far(c, h, src, k, dst).start()
            send(c, h, src, 3 + k, part).start()

    def forward_opp(c):
        for h in (0, 1):
            for k in (0, 1):
                far(c, h, opp, k, part).wait_recv()
            send(c, h, opp, 5, part).start()

    def partner_all(c):
        for d in (0, 2, 4, 6):
            for h in (0, 1):
                arrived(c, h, lax.rem(part + d, n))

    def outer(c, lo, hi):
        @pl.loop(lo, hi)
        def _(b):
            rhs = jnp.concatenate([jnp.concatenate([ball[c, h, :, b * 2 + t].reshape(lanes, hdep) for h in range(2)], axis=1) for t in range(2)], axis=0)
            o = lax.dot_general(at_b[...], rhs, (((1,), (1,)), ((), ())), preferred_element_type=jnp.float32)
            o = (o * (1.0 / depth)).astype(jnp.bfloat16)
            nt = rows * odim // TILE
            for t in range(2):
                obuf[b, t * nt:(t + 1) * nt] = o[:, t * lanes:(t + 1) * lanes].reshape(nt, TILE, lanes)

    def mix(c, lo, hi):
        @pl.loop(lo, hi, unroll=2)
        def _(i):
            nt, w = rows * odim // TILE, odim // TILE
            rhs = jnp.stack([obuf[:, pl.ds(t * nt + i * w, w)] for t in range(2)], axis=1).reshape(odim * odim, lanes)
            upd = jnp.dot(wt[...], rhs, preferred_element_type=jnp.float32)
            zt = turned(zi[i, :, c], c).reshape(lanes, chan).T
            zb[i, :, c * lanes:(c + 1) * lanes] = zt + (upd + bc[...])

    def prepare():
        for copy in smalls[2:]:
            copy.wait()
        rid = lax.broadcasted_iota(jnp.int32, (cols, cols), 0)
        cid = lax.broadcasted_iota(jnp.int32, (cols, cols), 1)
        two = chunks * jrows
        piece = (rid // jrows) % chunks
        place = piece * lanes + ((rid // two + piece * (n // 2)) % n) * jrows + rid % jrows
        perm = (cid == place).astype(jnp.float32).astype(jnp.bfloat16)
        mk[...] = jnp.dot(mask_ref[...].astype(jnp.float32).astype(jnp.bfloat16), perm, preferred_element_type=jnp.float32)
        bc[...] = _column(obias_ref[...], lanes)
        for t in range(2):
            for k in range(2):
                nc[t, k] = _column(nrm_ref[t, k:k + 1, :], lanes)
                nc[t, 2 + k] = _column(xnrm_ref[t, k:k + 1, :], lanes)
            for k in range(4):
                wa[t, k * chan:(k + 1) * chan] = proj_ref[t, :, k * chan:(k + 1) * chan].astype(jnp.float32).T.astype(jnp.bfloat16)
            wa[t, 4 * chan:] = gate_ref[t].astype(jnp.float32).T.astype(jnp.bfloat16)
            wo[t] = out_ref[t].astype(jnp.float32).T.astype(jnp.bfloat16)
        fb[:odim * odim, :] = oout_ref[...].astype(jnp.float32)

        @pl.loop(0, odim * odim // LANES)
        def _(b):
            m = LANES // odim
            v = jnp.concatenate([fb[pl.ds(b * m + k, odim, stride=odim), :] for k in range(m)], axis=0)
            wt[:, pl.ds(pl.multiple_of(b * LANES, LANES), LANES)] = v.T.astype(jnp.bfloat16)

    def piece_rows(u, steps, pieces):
        @pl.loop(0, steps)
        def _(i):
            at = [(r0 + i, h * lanes) for r0, h, _, _ in pieces]
            z = jnp.concatenate([zb[r, :, h:h + lanes] for r, h in at], axis=1)
            m = jnp.concatenate([mk[pl.ds(r, 1), :][:, h:h + lanes] for r, h in at], axis=1)
            scale = jnp.concatenate([nc[u, 0]] * 2, axis=1)
            shift = jnp.concatenate([nc[u, 1]] * 2, axis=1)
            q = jnp.dot(wa[u], _norm_rows(z, scale, shift), preferred_element_type=jnp.float32)
            ab = (m * jax.nn.sigmoid(q[chan:2 * chan]) * q[:chan], m * jax.nn.sigmoid(q[3 * chan:4 * chan]) * q[2 * chan:3 * chan])
            g = jax.nn.sigmoid(q[4 * chan:])
            for s, (r, h) in enumerate(at):
                gb[r, :, h:h + lanes] = g[:, s * lanes:(s + 1) * lanes]
                for t in range(2):
                    row = pl.multiple_of((t * 2 + pieces[s][2]) * (jrows * pst) + (i + pieces[s][3]) * pst, 8)
                    st[pl.ds(row, chan), :] = ab[t][:, s * lanes:(s + 1) * lanes]

    def turn(p, which=(0, 1)):
        @pl.loop(0, chan, unroll=8)
        def _(c):
            for t in range(2):
                for s in which:
                    snd[t, p, s, c] = st[pl.ds((t * 2 + s) * (jrows * pst) + c, jrows, stride=pst), :].astype(jnp.bfloat16)

    own = pl.ds(pl.multiple_of(me * cown, cown), cown)

    chip, core = me // 2, lax.rem(me, 2)
    first, second = chip + 1 - 2 * lax.rem(chip, 2), n // 2 - 1 - chip
    gchan, cslice = chan // 2, chan // 4
    sides = (lax.rem((chip + 1) // 2, 2), chip // 2)

    def mate(t, g):
        return first if t == g else second

    def o_copy(t, p, s, g, far, src_core, dst_core, sending):
        other = 2 * (mate(t, g) if far else chip) + (dst_core if sending else src_core)
        src = me if sending else other
        buf = rb if t else ra
        k = (2 if far else 0)
        return pltpu.make_async_remote_copy(
            src_ref=snd.at[t, p, s, pl.ds(pl.multiple_of(g * gchan + (dst_core if sending else core) * cslice, cslice), cslice)],
            dst_ref=buf.at[g, p, slot(s, src)],
            send_sem=ss_o.at[t, p, s, g, k + (dst_core if sending else 0)], recv_sem=rs_o.at[t, p, s, g, k + (core if sending else src_core)],
            device_id={"dap": other}, device_id_type=MESH)

    def o_send(t, p, s):
        for g in range(2):
            for c in range(2):
                o_copy(t, p, s, g, True, core, c, True).start()
            o_copy(t, p, s, g, False, core, 1 - core, True).start()
            buf = rb if t else ra
            buf[g, p, slot(s, me)] = snd[t, p, s, pl.ds(pl.multiple_of(g * gchan + core * cslice, cslice), cslice)]

    def o_wait(t, p, s):
        for g in range(2):
            o_copy(t, p, s, g, False, 1 - core, core, False).wait_recv()
            for c in range(2):
                o_copy(t, p, s, g, True, c, core, False).wait_recv()

    def o_sent():
        for t in range(2):
            for p in range(2):
                for s in range(2):
                    for g in range(2):
                        for c in range(2):
                            o_copy(t, p, s, g, True, core, c, True).wait_send()
                        o_copy(t, p, s, g, False, core, 1 - core, True).wait_send()

    def xo_copy(p, g, far, src_core, dst_core, sending):
        other = 2 * (mate(0, g) if far else chip) + (dst_core if sending else src_core)
        dst = other if sending else me
        k = 2 if far else 0
        return pltpu.make_async_remote_copy(
            src_ref=xs.at[g, :, slot(p, dst)],
            dst_ref=xr.at[p, sides[g], pl.ds((g * 2 + (core if sending else src_core)) * 2, 2)],
            send_sem=ss_xo.at[p, g, k + (dst_core if sending else 0)], recv_sem=rs_xo.at[p, g, k + (core if sending else src_core)],
            device_id={"dap": other}, device_id_type=MESH)

    def xo_send(p):
        for g in range(2):
            for c in range(2):
                xo_copy(p, g, True, core, c, True).start()
            xo_copy(p, g, False, core, 1 - core, True).start()
            xr[p, sides[g], pl.ds((g * 2 + core) * 2, 2)] = xs[g, :, slot(p, me)]

    def xo_wait(p):
        for g in range(2):
            xo_copy(p, g, False, 1 - core, core, False).wait_recv()
            for c in range(2):
                xo_copy(p, g, True, c, core, False).wait_recv()

    def xo_sent():
        for p in range(2):
            for g in range(2):
                for c in range(2):
                    xo_copy(p, g, True, core, c, True).wait_send()
                xo_copy(p, g, False, core, 1 - core, True).wait_send()

    def x_out(p):
        for g in range(2):
            at = [slot(p, 2 * w + c) for w in (chip, mate(0, g)) for c in range(2)]
            for e in range(cslice // cown):
                @pl.loop(0, cown, unroll=2)
                def _(c, g=g, e=e, at=at):
                    k = e * cown + c
                    a = jnp.concatenate([jnp.concatenate([ra[g, h, d, k] for d in at], axis=0) for h in range(2)], axis=1)
                    b = jnp.concatenate([rb[g, h, :, k].reshape(lanes, lanes) for h in range(2)], axis=1)
                    x = lax.dot_general(a, b, (((1,), (1,)), ((), ())), preferred_element_type=jnp.float32).astype(jnp.bfloat16)
                    for m, d in enumerate(at):
                        xs[g, e, d, c] = x[m * jrows:(m + 1) * jrows]

    def parts(p):
        return ((0, cown),) if p == 0 else ((0, cown // 2), (cown // 2, cown // 2))

    def landing(t, p, s, src, e):
        lo, m = parts(p)[e]
        return obuf.at[t * 4 + p * 2 + s, pl.ds(pl.multiple_of(src * cown, cown) + lo, m)]

    def ab_copy(t, p, s, e, src, dst):
        lo, m = parts(p)[e]
        return pltpu.make_async_remote_copy(
            src_ref=snd.at[t, p, s, pl.ds(pl.multiple_of(dst * cown, cown) + lo, m)], dst_ref=landing(t, p, s, src, e),
            send_sem=ss_ab.at[t, p, s, e, dst], recv_sem=rs_ab.at[t, p, s, e, src],
            device_id={"dap": dst}, device_id_type=MESH)

    def ab_send(p, e, which=(0, 1)):
        lo, m = parts(p)[e]
        for s in which:
            for t in range(2):
                for d in range(1, n):
                    ab_copy(t, p, s, e, me, lax.rem(me + d, n)).start()
                obuf[t * 4 + p * 2 + s, pl.ds(pl.multiple_of(me * cown, cown) + lo, m)] = snd[t, p, s, pl.ds(pl.multiple_of(me * cown, cown) + lo, m)]

    def ab_wait(p, e):
        for t in range(2):
            for s in range(2):
                for d in range(1, n):
                    ab_copy(t, p, s, e, lax.rem(me + d, n), me).wait_recv()

    def ab_sent():
        for p in range(2):
            for e in range(len(parts(p))):
                for t in range(2):
                    for s in range(2):
                        for d in range(1, n):
                            ab_copy(t, p, s, e, me, lax.rem(me + d, n)).wait_send()

    hown = cown // 2

    def x_copy(p, e, h, src, dst):
        at = pl.ds(e * hown, hown)
        return pltpu.make_async_remote_copy(
            src_ref=xs.at[p, h, dst, at], dst_ref=xr.at[p, h, src, at],
            send_sem=ss_x.at[p, e, h, dst], recv_sem=rs_x.at[p, e, h, src],
            device_id={"dap": dst}, device_id_type=MESH)

    def x_send(p, e):
        for h in range(2):
            for d in range(1, n):
                x_copy(p, e, h, me, lax.rem(me + d, n)).start()
        at = slice(e * hown, (e + 1) * hown)
        xr[p, :, me, at] = xs[p, :, me, at]

    def x_wait(p, h):
        for e in range(2):
            for d in range(1, n):
                x_copy(p, e, h, lax.rem(me + d, n), me).wait_recv()

    def x_sent():
        for p in range(2):
            for e in range(2):
                for h in range(2):
                    for d in range(1, n):
                        x_copy(p, e, h, me, lax.rem(me + d, n)).wait_send()

    def x_in(e):
        @pl.loop(e * hown, (e + 1) * hown)
        def _(c):
            a, b = (jnp.concatenate([
                jnp.concatenate([obuf[t * 4 + p * 2 + s, src * cown + c] for p in range(2) for src in range(n)], axis=0)
                for s in range(2)], axis=1) for t in range(2))
            x = lax.dot_general(a, b, (((0,), (0,)), ((), ())), preferred_element_type=jnp.float32)
            x = x.astype(jnp.bfloat16).reshape(2, n, jrows, cols)
            for p in range(2):
                v = turned(x[p], p)
                for h in range(2):
                    xs[p, h, :, c] = v[:, :, h * lanes:(h + 1) * lanes]

    half = chan * pxt

    def stage(u, p, which=(0, 1)):
        lane = lax.broadcasted_iota(jnp.int32, (jrows, lanes), 1) // (lanes // 4)
        for k in range(n):
            take = ((lane == 0) | (lane == 3)) if k < n // 2 else (lane < 2)

            @pl.loop(0, cown, unroll=8)
            def _(c, k=k, take=take):
                x = [xr[p, h, k, c].astype(jnp.float32) for h in which]
                if u == 0:
                    x = [jnp.where(take, x[0], x[1]), jnp.where(take, x[1], x[0])]
                for h, x in zip(which, x):
                    fb[pl.ds(pl.multiple_of(h * half + (k * cown + c) * pxt, 8), jrows), :] = x

    def finish(u, p, steps, pieces):
        @pl.loop(0, steps)
        def _(i):
            at = [(p * jrows + r0 + i, h * lanes) for r0, h in pieces]
            x = jnp.concatenate([fb[pl.ds(h * half + r0 + i, chan, stride=pxt), :] for r0, h in pieces], axis=1)
            xscale = jnp.concatenate([nc[u, 2]] * 2, axis=1)
            xshift = jnp.concatenate([nc[u, 3]] * 2, axis=1)
            upd = jnp.dot(wo[u], _norm_rows(x, xscale, xshift), preferred_element_type=jnp.float32)
            new = [zb[r, :, h:h + lanes] + gb[r, :, h:h + lanes] * upd[:, k * lanes:(k + 1) * lanes] for k, (r, h) in enumerate(at)]
            if u == 0:
                for (r, h), v in zip(at, new):
                    zb[r, :, h:h + lanes] = v
            else:
                for (r, h), v in zip(at, new):
                    c = h // lanes
                    zi[r, :, c] = turned(v.T.reshape(n, jrows, chan), c)

    def ocopy(p, h):
        at = pl.ds(p * jrows, jrows)
        return pltpu.make_async_copy(zi.at[at, :, h], o_hbm.at[at, :, h], osem.at[p * 2 + h])

    project(0, 0)
    pl.semaphore_wait(barrier, n - 1)
    send_own(0, 0)
    project(0, 1)
    send_own(0, 1)
    zcopy.start()
    project(1, 0)
    forward_far(0, 0)
    project(1, 1)
    prepare()
    forward_far(0, 1)
    send_own(1, 0)
    send_own(1, 1)
    forward_opp(0)
    partner_all(0)
    outer(0, 0, blocks * 3 // 8)
    forward_far(1, 0)
    outer(0, blocks * 3 // 8, blocks)
    zcopy.wait()
    hr = jrows // 2
    for s in range(2):
        mix(0, s * jrows, (s + 1) * jrows)
        if s == 0:
            forward_far(1, 1)
        piece_rows(0, hr, ((s * jrows, 0, s, 0), (s * jrows + hr, 0, s, hr)))
        turn(0, (s,))
        for t in (1, 0):
            o_send(t, 0, s)
    forward_opp(1)
    partner_all(1)
    outer(1, 0, blocks)
    mix(1, 0, rows)
    piece_rows(0, jrows, ((0, 1, 0, 0), (jrows, 1, 1, 0)))
    turn(1)
    for t in (1, 0):
        for s in range(2):
            o_send(t, 1, s)
    for p in range(2):
        for s in range(2):
            o_wait(1, p, s)
    for p in range(2):
        o_wait(0, 0, p)
        o_wait(0, 1, p)
        x_out(p)
        xo_send(p)
    o_sent()
    for p in range(2):
        xo_wait(p)
        stage(0, p)
        for h in range(2):
            finish(0, p, hr, ((0, h), (hr, h)))
            piece_rows(1, hr, ((p * jrows, h, h, 0), (p * jrows + hr, h, h, hr)))
            turn(p, (h,))
            if p == 0:
                ab_send(0, 0, (h,))
    for e in range(2):
        ab_send(1, e)
    xo_sent()
    ab_wait(0, 0)
    for e in range(2):
        ab_wait(1, e)
        x_in(e)
        for p in range(2):
            x_send(p, e)
    for p in range(2):
        for h in range(2):
            x_wait(p, h)
            stage(1, p, (h,))
            finish(1, p, hr, ((0, h), (hr, h)))
            ocopy(p, h).start()
    for p in range(2):
        for h in range(2):
            ocopy(p, h).wait()
    ab_sent()
    x_sent()
    for c in range(chunks):
        for h in (0, 1):
            for k, src in enumerate((me, me, me, left, right, opp)):
                send(c, h, src, k, part).wait_send()
            far(c, h, left, 0, right).wait_send()
            far(c, h, right, 1, left).wait_send()


def solution(mesh):
    row_spec = P(("data", "dap"), None, None)
    mask_spec = P(("data", "dap"), None)
    msa_spec = P(None, ("data", "dap"), None)
    replicated = P()

    def local_program(pair_loc, mask_loc, msa_loc, opm_norm, opm_proj, opm_out, opm_bias, tri_norm, tri_proj, tri_gate, tri_xnorm, tri_out):
        n = lax.axis_size("dap")
        rows, cols, chan = pair_loc.shape
        depth, _, mdim = msa_loc.shape
        odim = opm_proj.shape[1] // 2
        chunks = 2
        lanes = cols // chunks
        jrows = rows // chunks
        cown = chan // n
        hbm = pl.BlockSpec(memory_space=pl.ANY)
        f32, bf16 = jnp.float32, jnp.bfloat16
        dma = pltpu.SemaphoreType.DMA
        staged = max(4 * jrows * (chan + 8), depth // LANES * jrows * (odim + 8))
        block = (rows, n, chunks, jrows, chan)
        smalls = (mask_loc, opm_norm, opm_proj.T, opm_out, opm_bias.reshape(1, chan), tri_norm, tri_proj, tri_gate, tri_xnorm, tri_out)
        return pl.pallas_call(
            functools.partial(_kernel, n),
            out_shape=jax.ShapeDtypeStruct(block, f32),
            in_specs=[hbm] * 12,
            out_specs=hbm,
            scratch_shapes=[pltpu.VMEM(a.shape, a.dtype) for a in smalls] + [
                pltpu.VMEM((depth, rows, mdim), bf16),
                pltpu.VMEM((max(depth // 2 * jrows, 2 * chan * (jrows + 8)), LANES), f32),
                pltpu.VMEM((rows * odim, depth), bf16),
                pltpu.VMEM((chunks, 2, n, odim, jrows, depth // 2), bf16),
                pltpu.VMEM((odim // 2, 2 * rows * odim // TILE, TILE, lanes), bf16),
                pltpu.VMEM(block, f32),
                pltpu.VMEM((rows, chan, cols), f32),
                pltpu.VMEM((rows, chan, cols), f32),
                pltpu.VMEM((staged, LANES), f32),
                pltpu.VMEM((2, 2, 2, chan, jrows, lanes), bf16),
                pltpu.VMEM((2, 2, n, chan // 4, jrows, lanes), bf16),
                pltpu.VMEM((2, 2, n, chan // 4, jrows, lanes), bf16),
                pltpu.VMEM((2, 2, n, cown, jrows, lanes), bf16),
                pltpu.VMEM((2, 2, n, cown, jrows, lanes), bf16),
                pltpu.VMEM((rows, cols), f32),
                pltpu.VMEM((chan, odim * odim), bf16),
                pltpu.VMEM((2, 5 * chan, chan), bf16),
                pltpu.VMEM((2, chan, chan), bf16),
                pltpu.VMEM((2, 4, chan, lanes), f32),
                pltpu.VMEM((chan, lanes), f32),
                dma((10,)), dma((depth // 32,)), dma((1,)), dma((4,)),
                dma((chunks, 2, 8)), dma((chunks, 2, n)), dma((chunks, 2, 2)),
                dma((2, 2, 2, 2, 4)), dma((2, 2, 2, 2, 4)), dma((2, 2, 4)), dma((2, 2, 4)),
                dma((2, 2, 2, 2, n)), dma((2, 2, 2, 2, n)), dma((2, 2, 2, n)), dma((2, 2, 2, n)),
            ],
            compiler_params=pltpu.CompilerParams(collective_id=0, has_side_effects=True, vmem_limit_bytes=67043328),
            name="pair_stack",
        )(pair_loc.reshape(block), mask_loc, msa_loc, *smalls[1:]).reshape(pair_loc.shape)

    return jax.shard_map(local_program, mesh=mesh, in_specs=(row_spec, mask_spec, msa_spec) + (replicated,) * 9, out_specs=row_spec, check_vma=False)
```

```python
import functools

import jax
import jax.numpy as jnp
from jax import lax
from jax.experimental import pallas as pl
from jax.experimental.pallas import tpu as pltpu
from jax.sharding import PartitionSpec as P

LN_EPS = 1e-5
LANES = 128
TILE = 16
MESH = pl.DeviceIdType.MESH


def _norm_rows(v, scale, shift):
    mean = jnp.mean(v, axis=0, keepdims=True)
    cen = v - mean
    var = jnp.mean(cen * cen, axis=0, keepdims=True)
    return (cen * lax.rsqrt(var + LN_EPS) * scale + shift).astype(jnp.bfloat16)


def _column(row, n):
    return jnp.broadcast_to(row, (n, row.shape[1])).T


def _kernel(n, z_hbm, mask_hbm, msa_hbm, onrm_hbm, oproj_hbm, oout_hbm, obias_hbm, nrm_hbm, proj_hbm, gate_hbm, xnrm_hbm, out_hbm, o_hbm,
            mask_ref, onrm_ref, oproj_ref, oout_ref, obias_ref, nrm_ref, proj_ref, gate_ref, xnrm_ref, out_ref,
            mb, fb, at_b, ball, obuf, zi, zb, gb, st, snd, ra, rb, xs, xr, mk, wt, wa, wo, nc, bc,
            wsem, msem, zsem, osem, ss, rs, rf, ss_o, rs_o, ss_xo, rs_xo, ss_ab, rs_ab, ss_x, rs_x):
    me = lax.axis_index("dap")
    depth, _, mdim = mb.shape
    rows, chan, cols = zb.shape
    chunks, lanes, jrows, odim = 2, cols // 2, rows // 2, ball.shape[3]
    grp = 8
    per = jrows // grp
    mblocks = msem.shape[0]
    qh = odim // 2
    cown = chan // n
    blocks = odim // 2
    bst, pst, pxt = odim + 8, chan + 8, jrows + 8
    part = me + 1 - 2 * lax.rem(me, 2)
    right, left, opp = lax.rem(me + 2, n), lax.rem(me + n - 2, n), lax.rem(me + 4, n)

    def mcopy(g):
        at = pl.ds(g * (depth // mblocks), depth // mblocks)
        return pltpu.make_async_copy(msa_hbm.at[at], mb.at[at], msem.at[g])

    smalls = [pltpu.make_async_copy(a, b, wsem.at[k]) for k, (a, b) in enumerate((
        (onrm_hbm, onrm_ref), (oproj_hbm, oproj_ref), (mask_hbm, mask_ref), (oout_hbm, oout_ref), (obias_hbm, obias_ref),
        (nrm_hbm, nrm_ref), (proj_hbm, proj_ref), (gate_hbm, gate_ref), (xnrm_hbm, xnrm_ref), (out_hbm, out_ref)))]
    for copy in smalls[:2]:
        copy.start()
    for g in range(mblocks):
        mcopy(g).start()
    for copy in smalls[2:]:
        copy.start()
    zcopy = pltpu.make_async_copy(z_hbm, zi, zsem.at[0])
    barrier = pltpu.get_barrier_semaphore()
    for s in range(1, n):
        pl.semaphore_signal(barrier, inc=1, device_id={"dap": lax.rem(me + s, n)}, device_id_type=MESH)
    for copy in smalls[:2]:
        copy.wait()

    def slot(c, dev):
        return lax.rem(dev + c * (n // 2), n)

    def turned(v, c):
        return v if c == 0 else jnp.concatenate([v[n // 2:], v[:n // 2]], axis=0)

    def block(c, h, src):
        return ball.at[c, h, slot(c, src)]

    def send(c, h, src, k, dst):
        return pltpu.make_async_remote_copy(
            src_ref=block(c, h, src), dst_ref=block(c, h, src), send_sem=ss.at[c, h, k], recv_sem=rs.at[c, h, src],
            device_id={"dap": dst}, device_id_type=MESH)

    def arrived(c, h, src):
        send(c, h, src, 0, part).wait_recv()

    def far(c, h, src, k, dst):
        at = ball.at[c, h, slot(c, src), k * qh:(k + 1) * qh]
        return pltpu.make_async_remote_copy(
            src_ref=at, dst_ref=at, send_sem=ss.at[c, h, 6 + k], recv_sem=rf.at[c, h, k],
            device_id={"dap": dst}, device_id_type=MESH)

    oscale, oshift = onrm_ref[0:1, :], onrm_ref[1:2, :]
    sb = 32
    pieces_d = ball.shape[1]
    hdep = depth // pieces_d
    tiles = hdep // LANES

    def project(c, h):
        section = hdep * grp
        @pl.loop(0, hdep // sb)
        def _(b):
            if c == 0:
                mcopy(h * (hdep // sb) + b).wait()
            x = mb[pl.ds(h * hdep + b * sb, sb), c * jrows:(c + 1) * jrows].astype(jnp.float32).reshape(sb * jrows, mdim)
            mean = jnp.mean(x, axis=1, keepdims=True)
            cen = x - mean
            var = jnp.mean(cen * cen, axis=1, keepdims=True)
            y = (cen * lax.rsqrt(var + LN_EPS) * oscale + oshift).astype(jnp.bfloat16)
            v = lax.dot_general(y, oproj_ref[...], (((1,), (1,)), ((), ())), preferred_element_type=jnp.float32)
            v = v.reshape(sb, per, grp, 2 * odim)
            for k in range(per):
                at = pl.ds(pl.multiple_of(k * section + b * (sb * grp), sb * grp), sb * grp)
                fb[at, :2 * odim] = v[:, k].reshape(sb * grp, 2 * odim)

        for k in range(per):
            @pl.loop(0, grp)
            def _(i, k=k):
                v = fb[pl.ds(k * section + i, hdep, stride=grp), :].T
                r = (c * per + k) * grp + i
                at_b[pl.ds(pl.multiple_of(r * odim, odim), odim), h * hdep:(h + 1) * hdep] = v[:odim].astype(jnp.bfloat16)
                for t in range(tiles):
                    row = pl.multiple_of(t * (jrows * bst) + (k * grp + i) * bst, 8)
                    st[pl.ds(row, odim), :] = v[odim:2 * odim, t * LANES:(t + 1) * LANES]

        @pl.loop(0, odim, unroll=4)
        def _(q):
            for t in range(tiles):
                ball[c, h, slot(c, me), q, :, t * LANES:(t + 1) * LANES] = (
                    st[pl.ds(t * (jrows * bst) + q, jrows, stride=bst), :].astype(jnp.bfloat16))

    def send_own(c, h):
        for k, dst in enumerate((right, left, part)):
            send(c, h, me, k, dst).start()

    def forward_far(c, h):
        for k, (src, dst) in enumerate(((left, right), (right, left))):
            arrived(c, h, src)
            far(c, h, src, k, dst).start()
            send(c, h, src, 3 + k, part).start()

    def forward_opp(c):
        for h in range(pieces_d):
            for k in (0, 1):
                far(c, h, opp, k, part).wait_recv()
            send(c, h, opp, 5, part).start()

    def partner_all(c):
        for d in (0, 2, 4, 6):
            for h in range(pieces_d):
                arrived(c, h, lax.rem(part + d, n))

    def outer(c, lo, hi):
        @pl.loop(lo, hi)
        def _(b):
            rhs = jnp.concatenate([jnp.concatenate([ball[c, h, :, b * 2 + t].reshape(lanes, hdep) for h in range(pieces_d)], axis=1) for t in range(2)], axis=0)
            o = lax.dot_general(at_b[...], rhs, (((1,), (1,)), ((), ())), preferred_element_type=jnp.float32)
            o = (o * (1.0 / depth)).astype(jnp.bfloat16)
            nt = rows * odim // TILE
            for t in range(2):
                obuf[b, t * nt:(t + 1) * nt] = o[:, t * lanes:(t + 1) * lanes].reshape(nt, TILE, lanes)

    def mix(c, lo, hi):
        @pl.loop(lo, hi, unroll=2)
        def _(i):
            nt, w = rows * odim // TILE, odim // TILE
            rhs = jnp.stack([obuf[:, pl.ds(t * nt + i * w, w)] for t in range(2)], axis=1).reshape(odim * odim, lanes)
            upd = jnp.dot(wt[...], rhs, preferred_element_type=jnp.float32)
            zt = turned(zi[i, :, c], c).reshape(lanes, chan).T
            zb[i, :, c * lanes:(c + 1) * lanes] = zt + (upd + bc[...])

    def prepare():
        for copy in smalls[2:]:
            copy.wait()
        rid = lax.broadcasted_iota(jnp.int32, (cols, cols), 0)
        cid = lax.broadcasted_iota(jnp.int32, (cols, cols), 1)
        two = chunks * jrows
        piece = (rid // jrows) % chunks
        place = piece * lanes + ((rid // two + piece * (n // 2)) % n) * jrows + rid % jrows
        perm = (cid == place).astype(jnp.float32).astype(jnp.bfloat16)
        mk[...] = jnp.dot(mask_ref[...].astype(jnp.float32).astype(jnp.bfloat16), perm, preferred_element_type=jnp.float32)
        bc[...] = _column(obias_ref[...], lanes)
        for t in range(2):
            for k in range(2):
                nc[t, k] = _column(nrm_ref[t, k:k + 1, :], lanes)
                nc[t, 2 + k] = _column(xnrm_ref[t, k:k + 1, :], lanes)
            for k in range(4):
                wa[t, k * chan:(k + 1) * chan] = proj_ref[t, :, k * chan:(k + 1) * chan].astype(jnp.float32).T.astype(jnp.bfloat16)
            wa[t, 4 * chan:] = gate_ref[t].astype(jnp.float32).T.astype(jnp.bfloat16)
            wo[t] = out_ref[t].astype(jnp.float32).T.astype(jnp.bfloat16)
        fb[:odim * odim, :] = oout_ref[...].astype(jnp.float32)

        @pl.loop(0, odim * odim // LANES)
        def _(b):
            m = LANES // odim
            v = jnp.concatenate([fb[pl.ds(b * m + k, odim, stride=odim), :] for k in range(m)], axis=0)
            wt[:, pl.ds(pl.multiple_of(b * LANES, LANES), LANES)] = v.T.astype(jnp.bfloat16)

    def piece_rows(u, steps, pieces):
        @pl.loop(0, steps)
        def _(i):
            at = [(r0 + i, h * lanes) for r0, h, _, _ in pieces]
            z = jnp.concatenate([zb[r, :, h:h + lanes] for r, h in at], axis=1)
            m = jnp.concatenate([mk[pl.ds(r, 1), :][:, h:h + lanes] for r, h in at], axis=1)
            scale = jnp.concatenate([nc[u, 0]] * 2, axis=1)
            shift = jnp.concatenate([nc[u, 1]] * 2, axis=1)
            q = jnp.dot(wa[u], _norm_rows(z, scale, shift), preferred_element_type=jnp.float32)
            ab = (m * jax.nn.sigmoid(q[chan:2 * chan]) * q[:chan], m * jax.nn.sigmoid(q[3 * chan:4 * chan]) * q[2 * chan:3 * chan])
            g = jax.nn.sigmoid(q[4 * chan:])
            for s, (r, h) in enumerate(at):
                gb[r, :, h:h + lanes] = g[:, s * lanes:(s + 1) * lanes]
                for t in range(2):
                    row = pl.multiple_of((t * 2 + pieces[s][2]) * (jrows * pst) + (i + pieces[s][3]) * pst, 8)
                    st[pl.ds(row, chan), :] = ab[t][:, s * lanes:(s + 1) * lanes]

    def turn(p, which=(0, 1)):
        @pl.loop(0, chan, unroll=8)
        def _(c):
            for t in range(2):
                for s in which:
                    snd[t, p, s, c] = st[pl.ds((t * 2 + s) * (jrows * pst) + c, jrows, stride=pst), :].astype(jnp.bfloat16)

    own = pl.ds(pl.multiple_of(me * cown, cown), cown)

    chip, core = me // 2, lax.rem(me, 2)
    first, second = chip + 1 - 2 * lax.rem(chip, 2), n // 2 - 1 - chip
    gchan, cslice = chan // 2, chan // 4
    sides = (lax.rem((chip + 1) // 2, 2), chip // 2)

    def mate(t, g):
        return first if t == g else second

    def o_copy(t, p, s, g, far, src_core, dst_core, sending):
        other = 2 * (mate(t, g) if far else chip) + (dst_core if sending else src_core)
        src = me if sending else other
        buf = rb if t else ra
        k = (2 if far else 0)
        return pltpu.make_async_remote_copy(
            src_ref=snd.at[t, p, s, pl.ds(pl.multiple_of(g * gchan + (dst_core if sending else core) * cslice, cslice), cslice)],
            dst_ref=buf.at[g, p, slot(s, src)],
            send_sem=ss_o.at[t, p, s, g, k + (dst_core if sending else 0)], recv_sem=rs_o.at[t, p, s, g, k + (core if sending else src_core)],
            device_id={"dap": other}, device_id_type=MESH)

    def o_send(t, p, s):
        for g in range(2):
            for c in range(2):
                o_copy(t, p, s, g, True, core, c, True).start()
            o_copy(t, p, s, g, False, core, 1 - core, True).start()
            buf = rb if t else ra
            buf[g, p, slot(s, me)] = snd[t, p, s, pl.ds(pl.multiple_of(g * gchan + core * cslice, cslice), cslice)]

    def o_wait(t, p, s):
        for g in range(2):
            o_copy(t, p, s, g, False, 1 - core, core, False).wait_recv()
            for c in range(2):
                o_copy(t, p, s, g, True, c, core, False).wait_recv()

    def o_sent():
        for t in range(2):
            for p in range(2):
                for s in range(2):
                    for g in range(2):
                        for c in range(2):
                            o_copy(t, p, s, g, True, core, c, True).wait_send()
                        o_copy(t, p, s, g, False, core, 1 - core, True).wait_send()

    def xo_copy(p, g, far, src_core, dst_core, sending):
        other = 2 * (mate(0, g) if far else chip) + (dst_core if sending else src_core)
        dst = other if sending else me
        k = 2 if far else 0
        return pltpu.make_async_remote_copy(
            src_ref=xs.at[g, :, slot(p, dst)],
            dst_ref=xr.at[p, sides[g], pl.ds((g * 2 + (core if sending else src_core)) * 2, 2)],
            send_sem=ss_xo.at[p, g, k + (dst_core if sending else 0)], recv_sem=rs_xo.at[p, g, k + (core if sending else src_core)],
            device_id={"dap": other}, device_id_type=MESH)

    def xo_send(p):
        for g in range(2):
            for c in range(2):
                xo_copy(p, g, True, core, c, True).start()
            xo_copy(p, g, False, core, 1 - core, True).start()
            xr[p, sides[g], pl.ds((g * 2 + core) * 2, 2)] = xs[g, :, slot(p, me)]

    def xo_wait(p):
        for g in range(2):
            xo_copy(p, g, False, 1 - core, core, False).wait_recv()
            for c in range(2):
                xo_copy(p, g, True, c, core, False).wait_recv()

    def xo_sent():
        for p in range(2):
            for g in range(2):
                for c in range(2):
                    xo_copy(p, g, True, core, c, True).wait_send()
                xo_copy(p, g, False, core, 1 - core, True).wait_send()

    def x_out(p):
        for g in range(2):
            at = [slot(p, 2 * w + c) for w in (chip, mate(0, g)) for c in range(2)]
            for e in range(cslice // cown):
                @pl.loop(0, cown, unroll=2)
                def _(c, g=g, e=e, at=at):
                    k = e * cown + c
                    a = jnp.concatenate([jnp.concatenate([ra[g, h, d, k] for d in at], axis=0) for h in range(2)], axis=1)
                    b = jnp.concatenate([rb[g, h, :, k].reshape(lanes, lanes) for h in range(2)], axis=1)
                    x = lax.dot_general(a, b, (((1,), (1,)), ((), ())), preferred_element_type=jnp.float32).astype(jnp.bfloat16)
                    for m, d in enumerate(at):
                        xs[g, e, d, c] = x[m * jrows:(m + 1) * jrows]

    def parts(p):
        return ((0, cown),) if p == 0 else ((0, cown // 2), (cown // 2, cown // 2))

    def landing(t, p, s, src, e):
        lo, m = parts(p)[e]
        return obuf.at[t * 4 + p * 2 + s, pl.ds(pl.multiple_of(src * cown, cown) + lo, m)]

    def ab_copy(t, p, s, e, src, dst):
        lo, m = parts(p)[e]
        return pltpu.make_async_remote_copy(
            src_ref=snd.at[t, p, s, pl.ds(pl.multiple_of(dst * cown, cown) + lo, m)], dst_ref=landing(t, p, s, src, e),
            send_sem=ss_ab.at[t, p, s, e, dst], recv_sem=rs_ab.at[t, p, s, e, src],
            device_id={"dap": dst}, device_id_type=MESH)

    def ab_send(p, e, which=(0, 1)):
        lo, m = parts(p)[e]
        for s in which:
            for t in range(2):
                for d in range(1, n):
                    ab_copy(t, p, s, e, me, lax.rem(me + d, n)).start()
                obuf[t * 4 + p * 2 + s, pl.ds(pl.multiple_of(me * cown, cown) + lo, m)] = snd[t, p, s, pl.ds(pl.multiple_of(me * cown, cown) + lo, m)]

    def ab_wait(p, e):
        for t in range(2):
            for s in range(2):
                for d in range(1, n):
                    ab_copy(t, p, s, e, lax.rem(me + d, n), me).wait_recv()

    def ab_sent():
        for p in range(2):
            for e in range(len(parts(p))):
                for t in range(2):
                    for s in range(2):
                        for d in range(1, n):
                            ab_copy(t, p, s, e, me, lax.rem(me + d, n)).wait_send()

    hown = cown // 2

    def x_copy(p, e, h, src, dst):
        at = pl.ds(e * hown, hown)
        return pltpu.make_async_remote_copy(
            src_ref=xs.at[p, h, dst, at], dst_ref=xr.at[p, h, src, at],
            send_sem=ss_x.at[p, e, h, dst], recv_sem=rs_x.at[p, e, h, src],
            device_id={"dap": dst}, device_id_type=MESH)

    def x_send(p, e):
        for h in range(2):
            for d in range(1, n):
                x_copy(p, e, h, me, lax.rem(me + d, n)).start()
        at = slice(e * hown, (e + 1) * hown)
        xr[p, :, me, at] = xs[p, :, me, at]

    def x_wait(p, h):
        for e in range(2):
            for d in range(1, n):
                x_copy(p, e, h, lax.rem(me + d, n), me).wait_recv()

    def x_sent():
        for p in range(2):
            for e in range(2):
                for h in range(2):
                    for d in range(1, n):
                        x_copy(p, e, h, me, lax.rem(me + d, n)).wait_send()

    def x_in(e):
        @pl.loop(e * hown, (e + 1) * hown)
        def _(c):
            a, b = (jnp.concatenate([
                jnp.concatenate([obuf[t * 4 + p * 2 + s, src * cown + c] for p in range(2) for src in range(n)], axis=0)
                for s in range(2)], axis=1) for t in range(2))
            x = lax.dot_general(a, b, (((0,), (0,)), ((), ())), preferred_element_type=jnp.float32)
            x = x.astype(jnp.bfloat16).reshape(2, n, jrows, cols)
            for p in range(2):
                v = turned(x[p], p)
                for h in range(2):
                    xs[p, h, :, c] = v[:, :, h * lanes:(h + 1) * lanes]

    half = chan * pxt

    def stage(u, p, which=(0, 1)):
        lane = lax.broadcasted_iota(jnp.int32, (jrows, lanes), 1) // (lanes // 4)
        for k in range(n):
            take = ((lane == 0) | (lane == 3)) if k < n // 2 else (lane < 2)

            @pl.loop(0, cown, unroll=8)
            def _(c, k=k, take=take):
                x = [xr[p, h, k, c].astype(jnp.float32) for h in which]
                if u == 0:
                    x = [jnp.where(take, x[0], x[1]), jnp.where(take, x[1], x[0])]
                for h, x in zip(which, x):
                    fb[pl.ds(pl.multiple_of(h * half + (k * cown + c) * pxt, 8), jrows), :] = x

    def finish(u, p, steps, pieces):
        @pl.loop(0, steps)
        def _(i):
            at = [(p * jrows + r0 + i, h * lanes) for r0, h in pieces]
            x = jnp.concatenate([fb[pl.ds(h * half + r0 + i, chan, stride=pxt), :] for r0, h in pieces], axis=1)
            xscale = jnp.concatenate([nc[u, 2]] * 2, axis=1)
            xshift = jnp.concatenate([nc[u, 3]] * 2, axis=1)
            upd = jnp.dot(wo[u], _norm_rows(x, xscale, xshift), preferred_element_type=jnp.float32)
            new = [zb[r, :, h:h + lanes] + gb[r, :, h:h + lanes] * upd[:, k * lanes:(k + 1) * lanes] for k, (r, h) in enumerate(at)]
            if u == 0:
                for (r, h), v in zip(at, new):
                    zb[r, :, h:h + lanes] = v
            else:
                for (r, h), v in zip(at, new):
                    c = h // lanes
                    zi[r, :, c] = turned(v.T.reshape(n, jrows, chan), c)

    def ocopy(p, h):
        at = pl.ds(p * jrows, jrows)
        return pltpu.make_async_copy(zi.at[at, :, h], o_hbm.at[at, :, h], osem.at[p * 2 + h])

    project(0, 0)
    pl.semaphore_wait(barrier, n - 1)
    send_own(0, 0)
    for h in range(1, pieces_d):
        project(0, h)
        send_own(0, h)
    zcopy.start()
    for h in range(pieces_d):
        project(1, h)
        if h == pieces_d - 1:
            prepare()
        forward_far(0, h)
    for h in range(pieces_d):
        send_own(1, h)
    forward_opp(0)
    partner_all(0)
    outer(0, 0, blocks * 3 // 8)
    for h in range(pieces_d // 2):
        forward_far(1, h)
    outer(0, blocks * 3 // 8, blocks)
    zcopy.wait()
    hr = jrows // 2
    for s in range(2):
        mix(0, s * jrows, (s + 1) * jrows)
        if s == 0:
            for h in range(pieces_d // 2, pieces_d):
                forward_far(1, h)
        piece_rows(0, hr, ((s * jrows, 0, s, 0), (s * jrows + hr, 0, s, hr)))
        turn(0, (s,))
        for t in (1, 0):
            o_send(t, 0, s)
        if s == 0:
            forward_opp(1)
    partner_all(1)
    outer(1, 0, blocks)
    for s in range(2):
        mix(1, s * jrows, (s + 1) * jrows)
        piece_rows(0, hr, ((s * jrows, 1, s, 0), (s * jrows + hr, 1, s, hr)))
        turn(1, (s,))
        o_send(1, 1, s)
    for s in range(2):
        o_send(0, 1, s)
    for p in range(2):
        for s in range(2):
            o_wait(1, p, s)
    for p in range(2):
        o_wait(0, 0, p)
        o_wait(0, 1, p)
        x_out(p)
        xo_send(p)
    o_sent()
    for p in range(2):
        xo_wait(p)
        stage(0, p)
        for h in range(2):
            finish(0, p, hr, ((0, h), (hr, h)))
            piece_rows(1, hr, ((p * jrows, h, h, 0), (p * jrows + hr, h, h, hr)))
            turn(p, (h,))
            if p == 0:
                ab_send(0, 0, (h,))
    for e in range(2):
        ab_send(1, e)
    xo_sent()
    ab_wait(0, 0)
    for e in range(2):
        ab_wait(1, e)
        x_in(e)
        for p in range(2):
            x_send(p, e)
    for p in range(2):
        for h in range(2):
            x_wait(p, h)
            stage(1, p, (h,))
            finish(1, p, hr, ((0, h), (hr, h)))
            ocopy(p, h).start()
    for p in range(2):
        for h in range(2):
            ocopy(p, h).wait()
    ab_sent()
    x_sent()
    for c in range(chunks):
        for h in range(pieces_d):
            for k, src in enumerate((me, me, me, left, right, opp)):
                send(c, h, src, k, part).wait_send()
            far(c, h, left, 0, right).wait_send()
            far(c, h, right, 1, left).wait_send()


def solution(mesh):
    row_spec = P(("data", "dap"), None, None)
    mask_spec = P(("data", "dap"), None)
    msa_spec = P(None, ("data", "dap"), None)
    replicated = P()

    def local_program(pair_loc, mask_loc, msa_loc, opm_norm, opm_proj, opm_out, opm_bias, tri_norm, tri_proj, tri_gate, tri_xnorm, tri_out):
        n = lax.axis_size("dap")
        rows, cols, chan = pair_loc.shape
        depth, _, mdim = msa_loc.shape
        odim = opm_proj.shape[1] // 2
        chunks = 2
        lanes = cols // chunks
        jrows = rows // chunks
        cown = chan // n
        hbm = pl.BlockSpec(memory_space=pl.ANY)
        f32, bf16 = jnp.float32, jnp.bfloat16
        dma = pltpu.SemaphoreType.DMA
        staged = max(4 * jrows * (chan + 8), depth // LANES * jrows * (odim + 8))
        block = (rows, n, chunks, jrows, chan)
        smalls = (mask_loc, opm_norm, opm_proj.T, opm_out, opm_bias.reshape(1, chan), tri_norm, tri_proj, tri_gate, tri_xnorm, tri_out)
        return pl.pallas_call(
            functools.partial(_kernel, n),
            out_shape=jax.ShapeDtypeStruct(block, f32),
            in_specs=[hbm] * 12,
            out_specs=hbm,
            scratch_shapes=[pltpu.VMEM(a.shape, a.dtype) for a in smalls] + [
                pltpu.VMEM((depth, rows, mdim), bf16),
                pltpu.VMEM((max(depth // 4 * jrows, 2 * chan * (jrows + 8)), LANES), f32),
                pltpu.VMEM((rows * odim, depth), bf16),
                pltpu.VMEM((chunks, 4, n, odim, jrows, depth // 4), bf16),
                pltpu.VMEM((odim // 2, 2 * rows * odim // TILE, TILE, lanes), bf16),
                pltpu.VMEM(block, f32),
                pltpu.VMEM((rows, chan, cols), f32),
                pltpu.VMEM((rows, chan, cols), f32),
                pltpu.VMEM((staged, LANES), f32),
                pltpu.VMEM((2, 2, 2, chan, jrows, lanes), bf16),
                pltpu.VMEM((2, 2, n, chan // 4, jrows, lanes), bf16),
                pltpu.VMEM((2, 2, n, chan // 4, jrows, lanes), bf16),
                pltpu.VMEM((2, 2, n, cown, jrows, lanes), bf16),
                pltpu.VMEM((2, 2, n, cown, jrows, lanes), bf16),
                pltpu.VMEM((rows, cols), f32),
                pltpu.VMEM((chan, odim * odim), bf16),
                pltpu.VMEM((2, 5 * chan, chan), bf16),
                pltpu.VMEM((2, chan, chan), bf16),
                pltpu.VMEM((2, 4, chan, lanes), f32),
                pltpu.VMEM((chan, lanes), f32),
                dma((10,)), dma((depth // 32,)), dma((1,)), dma((4,)),
                dma((chunks, 4, 8)), dma((chunks, 4, n)), dma((chunks, 4, 2)),
                dma((2, 2, 2, 2, 4)), dma((2, 2, 2, 2, 4)), dma((2, 2, 4)), dma((2, 2, 4)),
                dma((2, 2, 2, 2, n)), dma((2, 2, 2, 2, n)), dma((2, 2, 2, n)), dma((2, 2, 2, n)),
            ],
            compiler_params=pltpu.CompilerParams(collective_id=0, has_side_effects=True, vmem_limit_bytes=67043328),
            name="pair_stack",
        )(pair_loc.reshape(block), mask_loc, msa_loc, *smalls[1:]).reshape(pair_loc.shape)

    return jax.shard_map(local_program, mesh=mesh, in_specs=(row_spec, mask_spec, msa_spec) + (replicated,) * 9, out_specs=row_spec, check_vma=False)
```

```python
import functools

import jax
import jax.numpy as jnp
from jax import lax
from jax.experimental import pallas as pl
from jax.experimental.pallas import tpu as pltpu
from jax.sharding import PartitionSpec as P

LN_EPS = 1e-5
LANES = 128
TILE = 16
MESH = pl.DeviceIdType.MESH


def _norm_rows(v, scale, shift):
    mean = jnp.mean(v, axis=0, keepdims=True)
    cen = v - mean
    var = jnp.mean(cen * cen, axis=0, keepdims=True)
    return (cen * lax.rsqrt(var + LN_EPS) * scale + shift).astype(jnp.bfloat16)


def _column(row, n):
    return jnp.broadcast_to(row, (n, row.shape[1])).T


def _kernel(n, z_hbm, mask_hbm, msa_hbm, onrm_hbm, oproj_hbm, oout_hbm, obias_hbm, nrm_hbm, proj_hbm, gate_hbm, xnrm_hbm, out_hbm, o_hbm,
            mask_ref, onrm_ref, oproj_ref, oout_ref, obias_ref, nrm_ref, proj_ref, gate_ref, xnrm_ref, out_ref,
            mb, fb, at_b, ball, obuf, zi, zb, gb, st, snd, ra, rb, xs, xr, mk, wt, wa, wo, nc, bc,
            wsem, msem, zsem, osem, ss, rs, rf, ss_o, rs_o, ss_xo, rs_xo, ss_ab, rs_ab, ss_x, rs_x):
    me = lax.axis_index("dap")
    depth, _, mdim = mb.shape
    rows, chan, cols = zb.shape
    chunks, lanes, jrows, odim = 2, cols // 2, rows // 2, ball.shape[3]
    grp = 8
    per = jrows // grp
    mblocks = msem.shape[0]
    qh = odim // 2
    cown = chan // n
    blocks = odim // 2
    bst, pst, pxt = odim + 8, chan + 8, jrows + 8
    part = me + 1 - 2 * lax.rem(me, 2)
    right, left, opp = lax.rem(me + 2, n), lax.rem(me + n - 2, n), lax.rem(me + 4, n)

    def mcopy(g):
        at = pl.ds(g * (depth // mblocks), depth // mblocks)
        return pltpu.make_async_copy(msa_hbm.at[at], mb.at[at], msem.at[g])

    smalls = [pltpu.make_async_copy(a, b, wsem.at[k]) for k, (a, b) in enumerate((
        (onrm_hbm, onrm_ref), (oproj_hbm, oproj_ref), (mask_hbm, mask_ref), (oout_hbm, oout_ref), (obias_hbm, obias_ref),
        (nrm_hbm, nrm_ref), (proj_hbm, proj_ref), (gate_hbm, gate_ref), (xnrm_hbm, xnrm_ref), (out_hbm, out_ref)))]
    for copy in smalls[:2]:
        copy.start()
    for g in range(mblocks):
        mcopy(g).start()
    for copy in smalls[2:]:
        copy.start()
    zcopy = pltpu.make_async_copy(z_hbm, zi, zsem.at[0])
    barrier = pltpu.get_barrier_semaphore()
    for s in range(1, n):
        pl.semaphore_signal(barrier, inc=1, device_id={"dap": lax.rem(me + s, n)}, device_id_type=MESH)
    for copy in smalls[:2]:
        copy.wait()

    def slot(c, dev):
        return lax.rem(dev + c * (n // 2), n)

    def turned(v, c):
        return v if c == 0 else jnp.concatenate([v[n // 2:], v[:n // 2]], axis=0)

    def block(c, h, src):
        return ball.at[c, h, slot(c, src)]

    def send(c, h, src, k, dst):
        return pltpu.make_async_remote_copy(
            src_ref=block(c, h, src), dst_ref=block(c, h, src), send_sem=ss.at[c, h, k], recv_sem=rs.at[c, h, src],
            device_id={"dap": dst}, device_id_type=MESH)

    def arrived(c, h, src):
        send(c, h, src, 0, part).wait_recv()

    def far(c, h, src, k, dst):
        at = ball.at[c, h, slot(c, src), k * qh:(k + 1) * qh]
        return pltpu.make_async_remote_copy(
            src_ref=at, dst_ref=at, send_sem=ss.at[c, h, 6 + k], recv_sem=rf.at[c, h, k],
            device_id={"dap": dst}, device_id_type=MESH)

    oscale, oshift = onrm_ref[0:1, :], onrm_ref[1:2, :]
    sb = 32
    pieces_d = ball.shape[1]
    hdep = depth // pieces_d
    tiles = hdep // LANES

    def project(c, h):
        section = hdep * grp
        @pl.loop(0, hdep // sb)
        def _(b):
            if c == 0:
                mcopy(h * (hdep // sb) + b).wait()
            x = mb[pl.ds(h * hdep + b * sb, sb), c * jrows:(c + 1) * jrows].astype(jnp.float32).reshape(sb * jrows, mdim)
            mean = jnp.mean(x, axis=1, keepdims=True)
            cen = x - mean
            var = jnp.mean(cen * cen, axis=1, keepdims=True)
            y = (cen * lax.rsqrt(var + LN_EPS) * oscale + oshift).astype(jnp.bfloat16)
            v = lax.dot_general(y, oproj_ref[...], (((1,), (1,)), ((), ())), preferred_element_type=jnp.float32)
            v = v.reshape(sb, per, grp, 2 * odim)
            for k in range(per):
                at = pl.ds(pl.multiple_of(k * section + b * (sb * grp), sb * grp), sb * grp)
                fb[at, :2 * odim] = v[:, k].reshape(sb * grp, 2 * odim)

        for k in range(per):
            @pl.loop(0, grp)
            def _(i, k=k):
                v = fb[pl.ds(k * section + i, hdep, stride=grp), :].T
                r = (c * per + k) * grp + i
                at_b[pl.ds(pl.multiple_of(r * odim, odim), odim), h * hdep:(h + 1) * hdep] = v[:odim].astype(jnp.bfloat16)
                for t in range(tiles):
                    row = pl.multiple_of(t * (jrows * bst) + (k * grp + i) * bst, 8)
                    st[pl.ds(row, odim), :] = v[odim:2 * odim, t * LANES:(t + 1) * LANES]

        @pl.loop(0, odim, unroll=4)
        def _(q):
            for t in range(tiles):
                ball[c, h, slot(c, me), q, :, t * LANES:(t + 1) * LANES] = (
                    st[pl.ds(t * (jrows * bst) + q, jrows, stride=bst), :].astype(jnp.bfloat16))

    def send_own(c, h):
        for k, dst in enumerate((right, left, part)):
            send(c, h, me, k, dst).start()

    def forward_far(c, h):
        for k, (src, dst) in enumerate(((left, right), (right, left))):
            arrived(c, h, src)
            far(c, h, src, k, dst).start()
            send(c, h, src, 3 + k, part).start()

    def forward_opp(c):
        for h in range(pieces_d):
            for k in (0, 1):
                far(c, h, opp, k, part).wait_recv()
            send(c, h, opp, 5, part).start()

    def partner_all(c):
        for d in (0, 2, 4, 6):
            for h in range(pieces_d):
                arrived(c, h, lax.rem(part + d, n))

    def outer(c, lo, hi):
        @pl.loop(lo, hi)
        def _(b):
            rhs = jnp.concatenate([jnp.concatenate([ball[c, h, :, b * 2 + t].reshape(lanes, hdep) for h in range(pieces_d)], axis=1) for t in range(2)], axis=0)
            o = lax.dot_general(at_b[...], rhs, (((1,), (1,)), ((), ())), preferred_element_type=jnp.float32)
            o = (o * (1.0 / depth)).astype(jnp.bfloat16)
            nt = rows * odim // TILE
            for t in range(2):
                obuf[b, t * nt:(t + 1) * nt] = o[:, t * lanes:(t + 1) * lanes].reshape(nt, TILE, lanes)

    def mix(c, lo, hi):
        @pl.loop(lo, hi, unroll=2)
        def _(i):
            nt, w = rows * odim // TILE, odim // TILE
            rhs = jnp.stack([obuf[:, pl.ds(t * nt + i * w, w)] for t in range(2)], axis=1).reshape(odim * odim, lanes)
            upd = jnp.dot(wt[...], rhs, preferred_element_type=jnp.float32)
            zt = turned(zi[i, :, c], c).reshape(lanes, chan).T
            zb[i, :, c * lanes:(c + 1) * lanes] = zt + (upd + bc[...])

    def prepare():
        for copy in smalls[2:]:
            copy.wait()
        rid = lax.broadcasted_iota(jnp.int32, (cols, cols), 0)
        cid = lax.broadcasted_iota(jnp.int32, (cols, cols), 1)
        two = chunks * jrows
        piece = (rid // jrows) % chunks
        place = piece * lanes + ((rid // two + piece * (n // 2)) % n) * jrows + rid % jrows
        perm = (cid == place).astype(jnp.float32).astype(jnp.bfloat16)
        mk[...] = jnp.dot(mask_ref[...].astype(jnp.float32).astype(jnp.bfloat16), perm, preferred_element_type=jnp.float32)
        bc[...] = _column(obias_ref[...], lanes)
        for t in range(2):
            for k in range(2):
                nc[t, k] = _column(nrm_ref[t, k:k + 1, :], lanes)
                nc[t, 2 + k] = _column(xnrm_ref[t, k:k + 1, :], lanes)
            for k in range(4):
                wa[t, k * chan:(k + 1) * chan] = proj_ref[t, :, k * chan:(k + 1) * chan].astype(jnp.float32).T.astype(jnp.bfloat16)
            wa[t, 4 * chan:] = gate_ref[t].astype(jnp.float32).T.astype(jnp.bfloat16)
            wo[t] = out_ref[t].astype(jnp.float32).T.astype(jnp.bfloat16)
        fb[:odim * odim, :] = oout_ref[...].astype(jnp.float32)

        @pl.loop(0, odim * odim // LANES)
        def _(b):
            m = LANES // odim
            v = jnp.concatenate([fb[pl.ds(b * m + k, odim, stride=odim), :] for k in range(m)], axis=0)
            wt[:, pl.ds(pl.multiple_of(b * LANES, LANES), LANES)] = v.T.astype(jnp.bfloat16)

    def piece_rows(u, steps, pieces):
        @pl.loop(0, steps)
        def _(i):
            at = [(r0 + i, h * lanes) for r0, h, _, _ in pieces]
            z = jnp.concatenate([zb[r, :, h:h + lanes] for r, h in at], axis=1)
            m = jnp.concatenate([mk[pl.ds(r, 1), :][:, h:h + lanes] for r, h in at], axis=1)
            scale = jnp.concatenate([nc[u, 0]] * 2, axis=1)
            shift = jnp.concatenate([nc[u, 1]] * 2, axis=1)
            q = jnp.dot(wa[u], _norm_rows(z, scale, shift), preferred_element_type=jnp.float32)
            ab = (m * jax.nn.sigmoid(q[chan:2 * chan]) * q[:chan], m * jax.nn.sigmoid(q[3 * chan:4 * chan]) * q[2 * chan:3 * chan])
            g = jax.nn.sigmoid(q[4 * chan:])
            for s, (r, h) in enumerate(at):
                gb[r, :, h:h + lanes] = g[:, s * lanes:(s + 1) * lanes]
                for t in range(2):
                    row = pl.multiple_of((t * 2 + pieces[s][2]) * (jrows * pst) + (i + pieces[s][3]) * pst, 8)
                    st[pl.ds(row, chan), :] = ab[t][:, s * lanes:(s + 1) * lanes]

    def turn(p, which=(0, 1)):
        @pl.loop(0, chan, unroll=8)
        def _(c):
            for t in range(2):
                for s in which:
                    snd[t, p, s, c] = st[pl.ds((t * 2 + s) * (jrows * pst) + c, jrows, stride=pst), :].astype(jnp.bfloat16)

    own = pl.ds(pl.multiple_of(me * cown, cown), cown)

    chip, core = me // 2, lax.rem(me, 2)
    first, second = chip + 1 - 2 * lax.rem(chip, 2), n // 2 - 1 - chip
    gchan, cslice = chan // 2, chan // 4
    sides = (lax.rem((chip + 1) // 2, 2), chip // 2)

    def mate(t, g):
        return first if t == g else second

    def o_copy(t, p, s, g, far, src_core, dst_core, sending):
        other = 2 * (mate(t, g) if far else chip) + (dst_core if sending else src_core)
        src = me if sending else other
        buf = rb if t else ra
        k = (2 if far else 0)
        return pltpu.make_async_remote_copy(
            src_ref=snd.at[t, p, s, pl.ds(pl.multiple_of(g * gchan + (dst_core if sending else core) * cslice, cslice), cslice)],
            dst_ref=buf.at[g, p, slot(s, src)],
            send_sem=ss_o.at[t, p, s, g, k + (dst_core if sending else 0)], recv_sem=rs_o.at[t, p, s, g, k + (core if sending else src_core)],
            device_id={"dap": other}, device_id_type=MESH)

    def o_send(t, p, s):
        for g in range(2):
            for c in range(2):
                o_copy(t, p, s, g, True, core, c, True).start()
            o_copy(t, p, s, g, False, core, 1 - core, True).start()
            buf = rb if t else ra
            buf[g, p, slot(s, me)] = snd[t, p, s, pl.ds(pl.multiple_of(g * gchan + core * cslice, cslice), cslice)]

    def o_wait(t, p, s):
        for g in range(2):
            o_copy(t, p, s, g, False, 1 - core, core, False).wait_recv()
            for c in range(2):
                o_copy(t, p, s, g, True, c, core, False).wait_recv()

    def o_sent():
        for t in range(2):
            for p in range(2):
                for s in range(2):
                    for g in range(2):
                        for c in range(2):
                            o_copy(t, p, s, g, True, core, c, True).wait_send()
                        o_copy(t, p, s, g, False, core, 1 - core, True).wait_send()

    def xo_copy(p, g, far, src_core, dst_core, sending):
        other = 2 * (mate(0, g) if far else chip) + (dst_core if sending else src_core)
        dst = other if sending else me
        k = 2 if far else 0
        return pltpu.make_async_remote_copy(
            src_ref=xs.at[g, :, slot(p, dst)],
            dst_ref=xr.at[p, sides[g], pl.ds((g * 2 + (core if sending else src_core)) * 2, 2)],
            send_sem=ss_xo.at[p, g, k + (dst_core if sending else 0)], recv_sem=rs_xo.at[p, g, k + (core if sending else src_core)],
            device_id={"dap": other}, device_id_type=MESH)

    def xo_send(p):
        for g in range(2):
            for c in range(2):
                xo_copy(p, g, True, core, c, True).start()
            xo_copy(p, g, False, core, 1 - core, True).start()
            xr[p, sides[g], pl.ds((g * 2 + core) * 2, 2)] = xs[g, :, slot(p, me)]

    def xo_wait(p):
        for g in range(2):
            xo_copy(p, g, False, 1 - core, core, False).wait_recv()
            for c in range(2):
                xo_copy(p, g, True, c, core, False).wait_recv()

    def xo_sent():
        for p in range(2):
            for g in range(2):
                for c in range(2):
                    xo_copy(p, g, True, core, c, True).wait_send()
                xo_copy(p, g, False, core, 1 - core, True).wait_send()

    def x_out(p):
        for g in range(2):
            at = [slot(p, 2 * w + c) for w in (chip, mate(0, g)) for c in range(2)]
            for e in range(cslice // cown):
                @pl.loop(0, cown, unroll=2)
                def _(c, g=g, e=e, at=at):
                    k = e * cown + c
                    a = jnp.concatenate([jnp.concatenate([ra[g, h, d, k] for d in at], axis=0) for h in range(2)], axis=1)
                    b = jnp.concatenate([rb[g, h, :, k].reshape(lanes, lanes) for h in range(2)], axis=1)
                    x = lax.dot_general(a, b, (((1,), (1,)), ((), ())), preferred_element_type=jnp.float32).astype(jnp.bfloat16)
                    for m, d in enumerate(at):
                        xs[g, e, d, c] = x[m * jrows:(m + 1) * jrows]

    def parts(p):
        return ((0, cown),) if p == 0 else ((0, cown // 2), (cown // 2, cown // 2))

    def landing(t, p, s, src, e):
        lo, m = parts(p)[e]
        return obuf.at[t * 4 + p * 2 + s, pl.ds(pl.multiple_of(src * cown, cown) + lo, m)]

    def ab_copy(t, p, s, e, src, dst):
        lo, m = parts(p)[e]
        return pltpu.make_async_remote_copy(
            src_ref=snd.at[t, p, s, pl.ds(pl.multiple_of(dst * cown, cown) + lo, m)], dst_ref=landing(t, p, s, src, e),
            send_sem=ss_ab.at[t, p, s, e, dst], recv_sem=rs_ab.at[t, p, s, e, src],
            device_id={"dap": dst}, device_id_type=MESH)

    def ab_send(p, e, which=(0, 1)):
        lo, m = parts(p)[e]
        for s in which:
            for t in range(2):
                for d in range(1, n):
                    ab_copy(t, p, s, e, me, lax.rem(me + d, n)).start()
                obuf[t * 4 + p * 2 + s, pl.ds(pl.multiple_of(me * cown, cown) + lo, m)] = snd[t, p, s, pl.ds(pl.multiple_of(me * cown, cown) + lo, m)]

    def ab_wait(p, e):
        for t in range(2):
            for s in range(2):
                for d in range(1, n):
                    ab_copy(t, p, s, e, lax.rem(me + d, n), me).wait_recv()

    def ab_sent():
        for p in range(2):
            for e in range(len(parts(p))):
                for t in range(2):
                    for s in range(2):
                        for d in range(1, n):
                            ab_copy(t, p, s, e, me, lax.rem(me + d, n)).wait_send()

    hown = cown // 2

    def x_copy(p, e, h, src, dst):
        at = pl.ds(e * hown, hown)
        return pltpu.make_async_remote_copy(
            src_ref=xs.at[p, h, dst, at], dst_ref=xr.at[p, h, src, at],
            send_sem=ss_x.at[p, e, h, dst], recv_sem=rs_x.at[p, e, h, src],
            device_id={"dap": dst}, device_id_type=MESH)

    def x_send(p, e):
        for h in range(2):
            for d in range(1, n):
                x_copy(p, e, h, me, lax.rem(me + d, n)).start()
        at = slice(e * hown, (e + 1) * hown)
        xr[p, :, me, at] = xs[p, :, me, at]

    def x_wait(p, h):
        for e in range(2):
            for d in range(1, n):
                x_copy(p, e, h, lax.rem(me + d, n), me).wait_recv()

    def x_sent():
        for p in range(2):
            for e in range(2):
                for h in range(2):
                    for d in range(1, n):
                        x_copy(p, e, h, me, lax.rem(me + d, n)).wait_send()

    def x_in(e):
        @pl.loop(e * hown, (e + 1) * hown)
        def _(c):
            a, b = (jnp.concatenate([
                jnp.concatenate([obuf[t * 4 + p * 2 + s, src * cown + c] for p in range(2) for src in range(n)], axis=0)
                for s in range(2)], axis=1) for t in range(2))
            x = lax.dot_general(a, b, (((0,), (0,)), ((), ())), preferred_element_type=jnp.float32)
            x = x.astype(jnp.bfloat16).reshape(2, n, jrows, cols)
            for p in range(2):
                v = turned(x[p], p)
                for h in range(2):
                    xs[p, h, :, c] = v[:, :, h * lanes:(h + 1) * lanes]

    half = chan * pxt

    def stage(u, p, which=(0, 1)):
        lane = lax.broadcasted_iota(jnp.int32, (jrows, lanes), 1) // (lanes // 4)
        for k in range(n):
            take = ((lane == 0) | (lane == 3)) if k < n // 2 else (lane < 2)

            @pl.loop(0, cown, unroll=8)
            def _(c, k=k, take=take):
                x = [xr[p, h, k, c].astype(jnp.float32) for h in which]
                if u == 0:
                    x = [jnp.where(take, x[0], x[1]), jnp.where(take, x[1], x[0])]
                for h, x in zip(which, x):
                    fb[pl.ds(pl.multiple_of(h * half + (k * cown + c) * pxt, 8), jrows), :] = x

    def finish(u, p, steps, pieces):
        @pl.loop(0, steps)
        def _(i):
            at = [(p * jrows + r0 + i, h * lanes) for r0, h in pieces]
            x = jnp.concatenate([fb[pl.ds(h * half + r0 + i, chan, stride=pxt), :] for r0, h in pieces], axis=1)
            xscale = jnp.concatenate([nc[u, 2]] * 2, axis=1)
            xshift = jnp.concatenate([nc[u, 3]] * 2, axis=1)
            upd = jnp.dot(wo[u], _norm_rows(x, xscale, xshift), preferred_element_type=jnp.float32)
            new = [zb[r, :, h:h + lanes] + gb[r, :, h:h + lanes] * upd[:, k * lanes:(k + 1) * lanes] for k, (r, h) in enumerate(at)]
            if u == 0:
                for (r, h), v in zip(at, new):
                    zb[r, :, h:h + lanes] = v
            else:
                for (r, h), v in zip(at, new):
                    c = h // lanes
                    zi[r, :, c] = turned(v.T.reshape(n, jrows, chan), c)

    def ocopy(p, h):
        at = pl.ds(p * jrows, jrows)
        return pltpu.make_async_copy(zi.at[at, :, h], o_hbm.at[at, :, h], osem.at[p * 2 + h])

    project(0, 0)
    pl.semaphore_wait(barrier, n - 1)
    send_own(0, 0)
    for h in range(1, pieces_d):
        project(0, h)
        send_own(0, h)
    zcopy.start()
    for h in range(pieces_d):
        project(1, h)
        if h == pieces_d - 1:
            prepare()
        forward_far(0, h)
    for h in range(pieces_d):
        send_own(1, h)
    forward_opp(0)
    partner_all(0)
    cuts = (0, blocks * 3 // 8, blocks * 11 // 16, blocks)
    for h in range(pieces_d - 1):
        outer(0, cuts[h], cuts[h + 1])
        forward_far(1, h)
    zcopy.wait()
    hr = jrows // 2
    for s in range(2):
        mix(0, s * jrows, (s + 1) * jrows)
        if s == 0:
            forward_far(1, pieces_d - 1)
        piece_rows(0, hr, ((s * jrows, 0, s, 0), (s * jrows + hr, 0, s, hr)))
        turn(0, (s,))
        for t in (1, 0):
            o_send(t, 0, s)
    forward_opp(1)
    partner_all(1)
    outer(1, 0, blocks)
    for s in range(2):
        mix(1, s * jrows, (s + 1) * jrows)
        piece_rows(0, hr, ((s * jrows, 1, s, 0), (s * jrows + hr, 1, s, hr)))
        turn(1, (s,))
        o_send(1, 1, s)
    for s in range(2):
        o_send(0, 1, s)
    for p in range(2):
        for s in range(2):
            o_wait(1, p, s)
    for p in range(2):
        o_wait(0, 0, p)
        o_wait(0, 1, p)
        x_out(p)
        xo_send(p)
    o_sent()
    for p in range(2):
        xo_wait(p)
        stage(0, p)
        for h in range(2):
            finish(0, p, hr, ((0, h), (hr, h)))
            piece_rows(1, hr, ((p * jrows, h, h, 0), (p * jrows + hr, h, h, hr)))
            turn(p, (h,))
            if p == 0:
                ab_send(0, 0, (h,))
    for e in range(2):
        ab_send(1, e)
    xo_sent()
    ab_wait(0, 0)
    for e in range(2):
        ab_wait(1, e)
        x_in(e)
        for p in range(2):
            x_send(p, e)
    for p in range(2):
        for h in range(2):
            x_wait(p, h)
            stage(1, p, (h,))
            finish(1, p, hr, ((0, h), (hr, h)))
            ocopy(p, h).start()
    for p in range(2):
        for h in range(2):
            ocopy(p, h).wait()
    ab_sent()
    x_sent()
    for c in range(chunks):
        for h in range(pieces_d):
            for k, src in enumerate((me, me, me, left, right, opp)):
                send(c, h, src, k, part).wait_send()
            far(c, h, left, 0, right).wait_send()
            far(c, h, right, 1, left).wait_send()


def solution(mesh):
    row_spec = P(("data", "dap"), None, None)
    mask_spec = P(("data", "dap"), None)
    msa_spec = P(None, ("data", "dap"), None)
    replicated = P()

    def local_program(pair_loc, mask_loc, msa_loc, opm_norm, opm_proj, opm_out, opm_bias, tri_norm, tri_proj, tri_gate, tri_xnorm, tri_out):
        n = lax.axis_size("dap")
        rows, cols, chan = pair_loc.shape
        depth, _, mdim = msa_loc.shape
        odim = opm_proj.shape[1] // 2
        chunks = 2
        lanes = cols // chunks
        jrows = rows // chunks
        cown = chan // n
        hbm = pl.BlockSpec(memory_space=pl.ANY)
        f32, bf16 = jnp.float32, jnp.bfloat16
        dma = pltpu.SemaphoreType.DMA
        staged = max(4 * jrows * (chan + 8), depth // LANES * jrows * (odim + 8))
        block = (rows, n, chunks, jrows, chan)
        smalls = (mask_loc, opm_norm, opm_proj.T, opm_out, opm_bias.reshape(1, chan), tri_norm, tri_proj, tri_gate, tri_xnorm, tri_out)
        return pl.pallas_call(
            functools.partial(_kernel, n),
            out_shape=jax.ShapeDtypeStruct(block, f32),
            in_specs=[hbm] * 12,
            out_specs=hbm,
            scratch_shapes=[pltpu.VMEM(a.shape, a.dtype) for a in smalls] + [
                pltpu.VMEM((depth, rows, mdim), bf16),
                pltpu.VMEM((max(depth // 4 * jrows, 2 * chan * (jrows + 8)), LANES), f32),
                pltpu.VMEM((rows * odim, depth), bf16),
                pltpu.VMEM((chunks, 4, n, odim, jrows, depth // 4), bf16),
                pltpu.VMEM((odim // 2, 2 * rows * odim // TILE, TILE, lanes), bf16),
                pltpu.VMEM(block, f32),
                pltpu.VMEM((rows, chan, cols), f32),
                pltpu.VMEM((rows, chan, cols), f32),
                pltpu.VMEM((staged, LANES), f32),
                pltpu.VMEM((2, 2, 2, chan, jrows, lanes), bf16),
                pltpu.VMEM((2, 2, n, chan // 4, jrows, lanes), bf16),
                pltpu.VMEM((2, 2, n, chan // 4, jrows, lanes), bf16),
                pltpu.VMEM((2, 2, n, cown, jrows, lanes), bf16),
                pltpu.VMEM((2, 2, n, cown, jrows, lanes), bf16),
                pltpu.VMEM((rows, cols), f32),
                pltpu.VMEM((chan, odim * odim), bf16),
                pltpu.VMEM((2, 5 * chan, chan), bf16),
                pltpu.VMEM((2, chan, chan), bf16),
                pltpu.VMEM((2, 4, chan, lanes), f32),
                pltpu.VMEM((chan, lanes), f32),
                dma((10,)), dma((depth // 32,)), dma((1,)), dma((4,)),
                dma((chunks, 4, 8)), dma((chunks, 4, n)), dma((chunks, 4, 2)),
                dma((2, 2, 2, 2, 4)), dma((2, 2, 2, 2, 4)), dma((2, 2, 4)), dma((2, 2, 4)),
                dma((2, 2, 2, 2, n)), dma((2, 2, 2, 2, n)), dma((2, 2, 2, n)), dma((2, 2, 2, n)),
            ],
            compiler_params=pltpu.CompilerParams(collective_id=0, has_side_effects=True, vmem_limit_bytes=67043328),
            name="pair_stack",
        )(pair_loc.reshape(block), mask_loc, msa_loc, *smalls[1:]).reshape(pair_loc.shape)

    return jax.shard_map(local_program, mesh=mesh, in_specs=(row_spec, mask_spec, msa_spec) + (replicated,) * 9, out_specs=row_spec, check_vma=False)
```

```python
import functools

import jax
import jax.numpy as jnp
from jax import lax
from jax.experimental import pallas as pl
from jax.experimental.pallas import tpu as pltpu
from jax.sharding import PartitionSpec as P

LN_EPS = 1e-5
LANES = 128
TILE = 16
MESH = pl.DeviceIdType.MESH


def _norm_rows(v, scale, shift):
    mean = jnp.mean(v, axis=0, keepdims=True)
    cen = v - mean
    var = jnp.mean(cen * cen, axis=0, keepdims=True)
    return (cen * lax.rsqrt(var + LN_EPS) * scale + shift).astype(jnp.bfloat16)


def _column(row, n):
    return jnp.broadcast_to(row, (n, row.shape[1])).T


def _kernel(n, z_hbm, mask_hbm, msa_hbm, onrm_hbm, oproj_hbm, oout_hbm, obias_hbm, nrm_hbm, proj_hbm, gate_hbm, xnrm_hbm, out_hbm, o_hbm,
            mask_ref, onrm_ref, oproj_ref, oout_ref, obias_ref, nrm_ref, proj_ref, gate_ref, xnrm_ref, out_ref,
            mb, fb, at_b, ball, obuf, zi, zb, gb, st, snd, ra, rb, xs, xr, mk, wt, wa, wo, nc, bc,
            wsem, msem, zsem, osem, ss, rs, rf, ss_o, rs_o, ss_xo, rs_xo, ss_ab, rs_ab, ss_x, rs_x):
    me = lax.axis_index("dap")
    depth, _, mdim = mb.shape
    rows, chan, cols = zb.shape
    chunks, lanes, jrows, odim = 2, cols // 2, rows // 2, ball.shape[3]
    grp = 8
    per = jrows // grp
    mblocks = msem.shape[0]
    qh = odim // 2
    cown = chan // n
    blocks = odim // 2
    bst, pst, pxt = odim + 8, chan + 8, jrows + 8
    part = me + 1 - 2 * lax.rem(me, 2)
    right, left, opp = lax.rem(me + 2, n), lax.rem(me + n - 2, n), lax.rem(me + 4, n)

    def mcopy(g):
        at = pl.ds(g * (depth // mblocks), depth // mblocks)
        return pltpu.make_async_copy(msa_hbm.at[at], mb.at[at], msem.at[g])

    smalls = [pltpu.make_async_copy(a, b, wsem.at[k]) for k, (a, b) in enumerate((
        (onrm_hbm, onrm_ref), (oproj_hbm, oproj_ref), (mask_hbm, mask_ref), (oout_hbm, oout_ref), (obias_hbm, obias_ref),
        (nrm_hbm, nrm_ref), (proj_hbm, proj_ref), (gate_hbm, gate_ref), (xnrm_hbm, xnrm_ref), (out_hbm, out_ref)))]
    for copy in smalls[:2]:
        copy.start()
    for g in range(mblocks):
        mcopy(g).start()
    for copy in smalls[2:]:
        copy.start()
    zcopy = pltpu.make_async_copy(z_hbm, zi, zsem.at[0])
    barrier = pltpu.get_barrier_semaphore()
    for s in range(1, n):
        pl.semaphore_signal(barrier, inc=1, device_id={"dap": lax.rem(me + s, n)}, device_id_type=MESH)
    for copy in smalls[:2]:
        copy.wait()

    def slot(c, dev):
        return lax.rem(dev + c * (n // 2), n)

    def turned(v, c):
        return v if c == 0 else jnp.concatenate([v[n // 2:], v[:n // 2]], axis=0)

    def block(c, h, src):
        return ball.at[c, h, slot(c, src)]

    def send(c, h, src, k, dst):
        return pltpu.make_async_remote_copy(
            src_ref=block(c, h, src), dst_ref=block(c, h, src), send_sem=ss.at[c, h, k], recv_sem=rs.at[c, h, src],
            device_id={"dap": dst}, device_id_type=MESH)

    def arrived(c, h, src):
        send(c, h, src, 0, part).wait_recv()

    def far(c, h, src, k, dst):
        at = ball.at[c, h, slot(c, src), k * qh:(k + 1) * qh]
        return pltpu.make_async_remote_copy(
            src_ref=at, dst_ref=at, send_sem=ss.at[c, h, 6 + k], recv_sem=rf.at[c, h, k],
            device_id={"dap": dst}, device_id_type=MESH)

    oscale, oshift = onrm_ref[0:1, :], onrm_ref[1:2, :]
    sb = 32
    hdep = depth // 2
    tiles = hdep // LANES

    def project(c, h):
        section = hdep * grp
        @pl.loop(0, hdep // sb)
        def _(b):
            if c == 0:
                mcopy(h * (hdep // sb) + b).wait()
            x = mb[pl.ds(h * hdep + b * sb, sb), c * jrows:(c + 1) * jrows].astype(jnp.float32).reshape(sb * jrows, mdim)
            mean = jnp.mean(x, axis=1, keepdims=True)
            cen = x - mean
            var = jnp.mean(cen * cen, axis=1, keepdims=True)
            y = (cen * lax.rsqrt(var + LN_EPS) * oscale + oshift).astype(jnp.bfloat16)
            v = lax.dot_general(y, oproj_ref[...], (((1,), (1,)), ((), ())), preferred_element_type=jnp.float32)
            v = v.reshape(sb, per, grp, 2 * odim)
            for k in range(per):
                at = pl.ds(pl.multiple_of(k * section + b * (sb * grp), sb * grp), sb * grp)
                fb[at, :2 * odim] = v[:, k].reshape(sb * grp, 2 * odim)

        for k in range(per):
            @pl.loop(0, grp)
            def _(i, k=k):
                v = fb[pl.ds(k * section + i, hdep, stride=grp), :].T
                r = (c * per + k) * grp + i
                at_b[pl.ds(pl.multiple_of(r * odim, odim), odim), h * hdep:(h + 1) * hdep] = v[:odim].astype(jnp.bfloat16)
                for t in range(tiles):
                    row = pl.multiple_of(t * (jrows * bst) + (k * grp + i) * bst, 8)
                    st[pl.ds(row, odim), :] = v[odim:2 * odim, t * LANES:(t + 1) * LANES]

        @pl.loop(0, odim, unroll=4)
        def _(q):
            for t in range(tiles):
                ball[c, h, slot(c, me), q, :, t * LANES:(t + 1) * LANES] = (
                    st[pl.ds(t * (jrows * bst) + q, jrows, stride=bst), :].astype(jnp.bfloat16))

    def send_own(c, h):
        for k, dst in enumerate((right, left, part)):
            send(c, h, me, k, dst).start()

    def forward_far(c, h):
        for k, (src, dst) in enumerate(((left, right), (right, left))):
            arrived(c, h, src)
            far(c, h, src, k, dst).start()
            send(c, h, src, 3 + k, part).start()

    def forward_opp(c):
        for h in (0, 1):
            for k in (0, 1):
                far(c, h, opp, k, part).wait_recv()
            send(c, h, opp, 5, part).start()

    def partner_all(c):
        for d in (0, 2, 4, 6):
            for h in (0, 1):
                arrived(c, h, lax.rem(part + d, n))

    def outer(c, lo, hi):
        @pl.loop(lo, hi)
        def _(b):
            rhs = jnp.concatenate([jnp.concatenate([ball[c, h, :, b * 2 + t].reshape(lanes, hdep) for h in range(2)], axis=1) for t in range(2)], axis=0)
            o = lax.dot_general(at_b[...], rhs, (((1,), (1,)), ((), ())), preferred_element_type=jnp.float32)
            o = (o * (1.0 / depth)).astype(jnp.bfloat16)
            nt = rows * odim // TILE
            for t in range(2):
                obuf[b, t * nt:(t + 1) * nt] = o[:, t * lanes:(t + 1) * lanes].reshape(nt, TILE, lanes)

    def mix(c, lo, hi):
        @pl.loop(lo, hi, unroll=2)
        def _(i):
            nt, w = rows * odim // TILE, odim // TILE
            rhs = jnp.stack([obuf[:, pl.ds(t * nt + i * w, w)] for t in range(2)], axis=1).reshape(odim * odim, lanes)
            upd = jnp.dot(wt[...], rhs, preferred_element_type=jnp.float32)
            zt = turned(zi[i, :, c], c).reshape(lanes, chan).T
            zb[i, :, c * lanes:(c + 1) * lanes] = zt + (upd + bc[...])

    def prepare():
        for copy in smalls[2:]:
            copy.wait()
        rid = lax.broadcasted_iota(jnp.int32, (cols, cols), 0)
        cid = lax.broadcasted_iota(jnp.int32, (cols, cols), 1)
        two = chunks * jrows
        piece = (rid // jrows) % chunks
        place = piece * lanes + ((rid // two + piece * (n // 2)) % n) * jrows + rid % jrows
        perm = (cid == place).astype(jnp.float32).astype(jnp.bfloat16)
        mk[...] = jnp.dot(mask_ref[...].astype(jnp.float32).astype(jnp.bfloat16), perm, preferred_element_type=jnp.float32)
        bc[...] = _column(obias_ref[...], lanes)
        for t in range(2):
            for k in range(2):
                nc[t, k] = _column(nrm_ref[t, k:k + 1, :], lanes)
                nc[t, 2 + k] = _column(xnrm_ref[t, k:k + 1, :], lanes)
            for k in range(4):
                wa[t, k * chan:(k + 1) * chan] = proj_ref[t, :, k * chan:(k + 1) * chan].astype(jnp.float32).T.astype(jnp.bfloat16)
            wa[t, 4 * chan:] = gate_ref[t].astype(jnp.float32).T.astype(jnp.bfloat16)
            wo[t] = out_ref[t].astype(jnp.float32).T.astype(jnp.bfloat16)
        fb[:odim * odim, :] = oout_ref[...].astype(jnp.float32)

        @pl.loop(0, odim * odim // LANES)
        def _(b):
            m = LANES // odim
            v = jnp.concatenate([fb[pl.ds(b * m + k, odim, stride=odim), :] for k in range(m)], axis=0)
            wt[:, pl.ds(pl.multiple_of(b * LANES, LANES), LANES)] = v.T.astype(jnp.bfloat16)

    def piece_rows(u, steps, pieces):
        @pl.loop(0, steps)
        def _(i):
            at = [(r0 + i, h * lanes) for r0, h, _, _ in pieces]
            z = jnp.concatenate([zb[r, :, h:h + lanes] for r, h in at], axis=1)
            m = jnp.concatenate([mk[pl.ds(r, 1), :][:, h:h + lanes] for r, h in at], axis=1)
            scale = jnp.concatenate([nc[u, 0]] * 2, axis=1)
            shift = jnp.concatenate([nc[u, 1]] * 2, axis=1)
            q = jnp.dot(wa[u], _norm_rows(z, scale, shift), preferred_element_type=jnp.float32)
            ab = (m * jax.nn.sigmoid(q[chan:2 * chan]) * q[:chan], m * jax.nn.sigmoid(q[3 * chan:4 * chan]) * q[2 * chan:3 * chan])
            g = jax.nn.sigmoid(q[4 * chan:])
            for s, (r, h) in enumerate(at):
                gb[r, :, h:h + lanes] = g[:, s * lanes:(s + 1) * lanes]
                for t in range(2):
                    row = pl.multiple_of((t * 2 + pieces[s][2]) * (jrows * pst) + (i + pieces[s][3]) * pst, 8)
                    st[pl.ds(row, chan), :] = ab[t][:, s * lanes:(s + 1) * lanes]

    def turn(p, which=(0, 1)):
        @pl.loop(0, chan, unroll=8)
        def _(c):
            for t in range(2):
                for s in which:
                    snd[t, p, s, c] = st[pl.ds((t * 2 + s) * (jrows * pst) + c, jrows, stride=pst), :].astype(jnp.bfloat16)

    own = pl.ds(pl.multiple_of(me * cown, cown), cown)

    chip, core = me // 2, lax.rem(me, 2)
    first, second = chip + 1 - 2 * lax.rem(chip, 2), n // 2 - 1 - chip
    gchan, cslice = chan // 2, chan // 4
    sides = (lax.rem((chip + 1) // 2, 2), chip // 2)

    def mate(t, g):
        return first if t == g else second

    def o_copy(t, p, s, g, far, src_core, dst_core, sending):
        other = 2 * (mate(t, g) if far else chip) + (dst_core if sending else src_core)
        src = me if sending else other
        buf = rb if t else ra
        k = (2 if far else 0)
        return pltpu.make_async_remote_copy(
            src_ref=snd.at[t, p, s, pl.ds(pl.multiple_of(g * gchan + (dst_core if sending else core) * cslice, cslice), cslice)],
            dst_ref=buf.at[g, p, slot(s, src)],
            send_sem=ss_o.at[t, p, s, g, k + (dst_core if sending else 0)], recv_sem=rs_o.at[t, p, s, g, k + (core if sending else src_core)],
            device_id={"dap": other}, device_id_type=MESH)

    def o_send(t, p, s):
        for g in range(2):
            for c in range(2):
                o_copy(t, p, s, g, True, core, c, True).start()
            o_copy(t, p, s, g, False, core, 1 - core, True).start()
            buf = rb if t else ra
            buf[g, p, slot(s, me)] = snd[t, p, s, pl.ds(pl.multiple_of(g * gchan + core * cslice, cslice), cslice)]

    def o_wait(t, p, s):
        for g in range(2):
            o_copy(t, p, s, g, False, 1 - core, core, False).wait_recv()
            for c in range(2):
                o_copy(t, p, s, g, True, c, core, False).wait_recv()

    def o_sent():
        for t in range(2):
            for p in range(2):
                for s in range(2):
                    for g in range(2):
                        for c in range(2):
                            o_copy(t, p, s, g, True, core, c, True).wait_send()
                        o_copy(t, p, s, g, False, core, 1 - core, True).wait_send()

    def xo_copy(p, g, far, src_core, dst_core, sending):
        other = 2 * (mate(0, g) if far else chip) + (dst_core if sending else src_core)
        dst = other if sending else me
        k = 2 if far else 0
        return pltpu.make_async_remote_copy(
            src_ref=xs.at[g, :, slot(p, dst)],
            dst_ref=xr.at[p, sides[g], pl.ds((g * 2 + (core if sending else src_core)) * 2, 2)],
            send_sem=ss_xo.at[p, g, k + (dst_core if sending else 0)], recv_sem=rs_xo.at[p, g, k + (core if sending else src_core)],
            device_id={"dap": other}, device_id_type=MESH)

    def xo_send(p):
        for g in range(2):
            for c in range(2):
                xo_copy(p, g, True, core, c, True).start()
            xo_copy(p, g, False, core, 1 - core, True).start()
            xr[p, sides[g], pl.ds((g * 2 + core) * 2, 2)] = xs[g, :, slot(p, me)]

    def xo_wait(p):
        for g in range(2):
            xo_copy(p, g, False, 1 - core, core, False).wait_recv()
            for c in range(2):
                xo_copy(p, g, True, c, core, False).wait_recv()

    def xo_sent():
        for p in range(2):
            for g in range(2):
                for c in range(2):
                    xo_copy(p, g, True, core, c, True).wait_send()
                xo_copy(p, g, False, core, 1 - core, True).wait_send()

    def x_out(p):
        for g in range(2):
            at = [slot(p, 2 * w + c) for w in (chip, mate(0, g)) for c in range(2)]
            for e in range(cslice // cown):
                @pl.loop(0, cown, unroll=2)
                def _(c, g=g, e=e, at=at):
                    k = e * cown + c
                    a = jnp.concatenate([jnp.concatenate([ra[g, h, d, k] for d in at], axis=0) for h in range(2)], axis=1)
                    b = jnp.concatenate([rb[g, h, :, k].reshape(lanes, lanes) for h in range(2)], axis=1)
                    x = lax.dot_general(a, b, (((1,), (1,)), ((), ())), preferred_element_type=jnp.float32).astype(jnp.bfloat16)
                    for m, d in enumerate(at):
                        xs[g, e, d, c] = x[m * jrows:(m + 1) * jrows]

    def parts(p):
        return ((0, cown),) if p == 0 else ((0, cown // 2), (cown // 2, cown // 2))

    def landing(t, p, s, src, e):
        lo, m = parts(p)[e]
        return obuf.at[t * 4 + p * 2 + s, pl.ds(pl.multiple_of(src * cown, cown) + lo, m)]

    def ab_copy(t, p, s, e, src, dst):
        lo, m = parts(p)[e]
        return pltpu.make_async_remote_copy(
            src_ref=snd.at[t, p, s, pl.ds(pl.multiple_of(dst * cown, cown) + lo, m)], dst_ref=landing(t, p, s, src, e),
            send_sem=ss_ab.at[t, p, s, e, dst], recv_sem=rs_ab.at[t, p, s, e, src],
            device_id={"dap": dst}, device_id_type=MESH)

    def ab_send(p, e, which=(0, 1)):
        lo, m = parts(p)[e]
        for s in which:
            for t in range(2):
                for d in range(1, n):
                    ab_copy(t, p, s, e, me, lax.rem(me + d, n)).start()
                obuf[t * 4 + p * 2 + s, pl.ds(pl.multiple_of(me * cown, cown) + lo, m)] = snd[t, p, s, pl.ds(pl.multiple_of(me * cown, cown) + lo, m)]

    def ab_wait(p, e):
        for t in range(2):
            for s in range(2):
                for d in range(1, n):
                    ab_copy(t, p, s, e, lax.rem(me + d, n), me).wait_recv()

    def ab_sent():
        for p in range(2):
            for e in range(len(parts(p))):
                for t in range(2):
                    for s in range(2):
                        for d in range(1, n):
                            ab_copy(t, p, s, e, me, lax.rem(me + d, n)).wait_send()

    hown = cown // 2

    def x_copy(p, e, h, src, dst):
        at = pl.ds(e * hown, hown)
        return pltpu.make_async_remote_copy(
            src_ref=xs.at[p, h, dst, at], dst_ref=xr.at[p, h, src, at],
            send_sem=ss_x.at[p, e, h, dst], recv_sem=rs_x.at[p, e, h, src],
            device_id={"dap": dst}, device_id_type=MESH)

    def x_send(p, e):
        for h in range(2):
            for d in range(1, n):
                x_copy(p, e, h, me, lax.rem(me + d, n)).start()
        at = slice(e * hown, (e + 1) * hown)
        xr[p, :, me, at] = xs[p, :, me, at]

    def x_wait(p, h):
        for e in range(2):
            for d in range(1, n):
                x_copy(p, e, h, lax.rem(me + d, n), me).wait_recv()

    def x_sent():
        for p in range(2):
            for e in range(2):
                for h in range(2):
                    for d in range(1, n):
                        x_copy(p, e, h, me, lax.rem(me + d, n)).wait_send()

    def x_in(e):
        @pl.loop(e * hown, (e + 1) * hown)
        def _(c):
            a, b = (jnp.concatenate([
                jnp.concatenate([obuf[t * 4 + p * 2 + s, src * cown + c] for p in range(2) for src in range(n)], axis=0)
                for s in range(2)], axis=1) for t in range(2))
            x = lax.dot_general(a, b, (((0,), (0,)), ((), ())), preferred_element_type=jnp.float32)
            x = x.astype(jnp.bfloat16).reshape(2, n, jrows, cols)
            for p in range(2):
                v = turned(x[p], p)
                for h in range(2):
                    xs[p, h, :, c] = v[:, :, h * lanes:(h + 1) * lanes]

    half = chan * pxt

    def stage(u, p, which=(0, 1)):
        lane = lax.broadcasted_iota(jnp.int32, (jrows, lanes), 1) // (lanes // 4)
        for k in range(n):
            take = ((lane == 0) | (lane == 3)) if k < n // 2 else (lane < 2)

            @pl.loop(0, cown, unroll=8)
            def _(c, k=k, take=take):
                x = [xr[p, h, k, c].astype(jnp.float32) for h in which]
                if u == 0:
                    x = [jnp.where(take, x[0], x[1]), jnp.where(take, x[1], x[0])]
                for h, x in zip(which, x):
                    fb[pl.ds(pl.multiple_of(h * half + (k * cown + c) * pxt, 8), jrows), :] = x

    def finish(u, p, steps, pieces):
        @pl.loop(0, steps)
        def _(i):
            at = [(p * jrows + r0 + i, h * lanes) for r0, h in pieces]
            x = jnp.concatenate([fb[pl.ds(h * half + r0 + i, chan, stride=pxt), :] for r0, h in pieces], axis=1)
            xscale = jnp.concatenate([nc[u, 2]] * 2, axis=1)
            xshift = jnp.concatenate([nc[u, 3]] * 2, axis=1)
            upd = jnp.dot(wo[u], _norm_rows(x, xscale, xshift), preferred_element_type=jnp.float32)
            new = [zb[r, :, h:h + lanes] + gb[r, :, h:h + lanes] * upd[:, k * lanes:(k + 1) * lanes] for k, (r, h) in enumerate(at)]
            if u == 0:
                for (r, h), v in zip(at, new):
                    zb[r, :, h:h + lanes] = v
            else:
                for (r, h), v in zip(at, new):
                    c = h // lanes
                    zi[r, :, c] = turned(v.T.reshape(n, jrows, chan), c)

    def ocopy(p, h):
        at = pl.ds(p * jrows, jrows)
        return pltpu.make_async_copy(zi.at[at, :, h], o_hbm.at[at, :, h], osem.at[p * 2 + h])

    project(0, 0)
    pl.semaphore_wait(barrier, n - 1)
    send_own(0, 0)
    project(0, 1)
    send_own(0, 1)
    zcopy.start()
    project(1, 0)
    forward_far(0, 0)
    project(1, 1)
    prepare()
    forward_far(0, 1)
    send_own(1, 0)
    send_own(1, 1)
    forward_opp(0)
    partner_all(0)
    outer(0, 0, blocks * 3 // 8)
    forward_far(1, 0)
    outer(0, blocks * 3 // 8, blocks)
    zcopy.wait()
    hr = jrows // 2
    for s in range(2):
        mix(0, s * jrows, (s + 1) * jrows)
        if s == 0:
            forward_far(1, 1)
        piece_rows(0, hr, ((s * jrows, 0, s, 0), (s * jrows + hr, 0, s, hr)))
        turn(0, (s,))
        for t in (1, 0):
            o_send(t, 0, s)
    forward_opp(1)
    partner_all(1)
    outer(1, 0, blocks)
    for s in range(2):
        mix(1, s * jrows, (s + 1) * jrows)
        piece_rows(0, hr, ((s * jrows, 1, s, 0), (s * jrows + hr, 1, s, hr)))
        turn(1, (s,))
        o_send(1, 1, s)
    for s in range(2):
        o_send(0, 1, s)
    for p in range(2):
        for s in range(2):
            o_wait(1, p, s)
    for p in range(2):
        o_wait(0, 0, p)
        o_wait(0, 1, p)
        x_out(p)
        xo_send(p)
    o_sent()
    for p in range(2):
        xo_wait(p)
        stage(0, p)
        for h in range(2):
            finish(0, p, hr, ((0, h), (hr, h)))
            piece_rows(1, hr, ((p * jrows, h, h, 0), (p * jrows + hr, h, h, hr)))
            turn(p, (h,))
            if p == 0:
                ab_send(0, 0, (h,))
    for e in range(2):
        ab_send(1, e)
    xo_sent()
    ab_wait(0, 0)
    for e in range(2):
        ab_wait(1, e)
        x_in(e)
        for p in range(2):
            x_send(p, e)
    for p in range(2):
        for h in range(2):
            x_wait(p, h)
            stage(1, p, (h,))
            finish(1, p, hr, ((0, h), (hr, h)))
            ocopy(p, h).start()
    for p in range(2):
        for h in range(2):
            ocopy(p, h).wait()
    ab_sent()
    x_sent()
    for c in range(chunks):
        for h in (0, 1):
            for k, src in enumerate((me, me, me, left, right, opp)):
                send(c, h, src, k, part).wait_send()
            far(c, h, left, 0, right).wait_send()
            far(c, h, right, 1, left).wait_send()


def _carry_kernel(src_hbm, dst_hbm, buf, in_sem, out_sem):
    pieces = in_sem.shape[0]
    step = buf.shape[0] // pieces
    at = [pl.ds(k * step, step) for k in range(pieces)]
    reads = [pltpu.make_async_copy(src_hbm.at[a], buf.at[a], in_sem.at[k]) for k, a in enumerate(at)]
    writes = [pltpu.make_async_copy(buf.at[a], dst_hbm.at[a], out_sem.at[k]) for k, a in enumerate(at)]
    for copy in reads:
        copy.start()
    for read, write in zip(reads, writes):
        read.wait()
        write.start()
    for copy in writes:
        copy.wait()


def _carry(v):
    hbm = pl.BlockSpec(memory_space=pl.ANY)
    pieces = 16
    return pl.pallas_call(
        _carry_kernel,
        out_shape=jax.ShapeDtypeStruct(v.shape, v.dtype),
        in_specs=[hbm],
        out_specs=hbm,
        scratch_shapes=[pltpu.VMEM(v.shape, v.dtype), pltpu.SemaphoreType.DMA((pieces,)), pltpu.SemaphoreType.DMA((pieces,))],
        compiler_params=pltpu.CompilerParams(vmem_limit_bytes=60 * 1024 * 1024),
        name="carry",
    )(v)


def solution(mesh):
    row_spec = P(("data", "dap"), None, None)
    mask_spec = P(("data", "dap"), None)
    msa_spec = P(None, ("data", "dap"), None)
    replicated = P()

    def local_program(pair_loc, mask_loc, msa_loc, opm_norm, opm_proj, opm_out, opm_bias, tri_norm, tri_proj, tri_gate, tri_xnorm, tri_out):
        n = lax.axis_size("dap")
        rows, cols, chan = pair_loc.shape
        depth, _, mdim = msa_loc.shape
        odim = opm_proj.shape[1] // 2
        chunks = 2
        lanes = cols // chunks
        jrows = rows // chunks
        cown = chan // n
        hbm = pl.BlockSpec(memory_space=pl.ANY)
        f32, bf16 = jnp.float32, jnp.bfloat16
        dma = pltpu.SemaphoreType.DMA
        staged = max(4 * jrows * (chan + 8), depth // LANES * jrows * (odim + 8))
        block = (rows, n, chunks, jrows, chan)
        smalls = (mask_loc, opm_norm, opm_proj.T, opm_out, opm_bias.reshape(1, chan), tri_norm, tri_proj, tri_gate, tri_xnorm, tri_out)
        out = pl.pallas_call(
            functools.partial(_kernel, n),
            out_shape=jax.ShapeDtypeStruct(block, f32),
            in_specs=[hbm] * 12,
            out_specs=hbm,
            scratch_shapes=[pltpu.VMEM(a.shape, a.dtype) for a in smalls] + [
                pltpu.VMEM((depth, rows, mdim), bf16),
                pltpu.VMEM((max(depth // 2 * jrows, 2 * chan * (jrows + 8)), LANES), f32),
                pltpu.VMEM((rows * odim, depth), bf16),
                pltpu.VMEM((chunks, 2, n, odim, jrows, depth // 2), bf16),
                pltpu.VMEM((odim // 2, 2 * rows * odim // TILE, TILE, lanes), bf16),
                pltpu.VMEM(block, f32),
                pltpu.VMEM((rows, chan, cols), f32),
                pltpu.VMEM((rows, chan, cols), f32),
                pltpu.VMEM((staged, LANES), f32),
                pltpu.VMEM((2, 2, 2, chan, jrows, lanes), bf16),
                pltpu.VMEM((2, 2, n, chan // 4, jrows, lanes), bf16),
                pltpu.VMEM((2, 2, n, chan // 4, jrows, lanes), bf16),
                pltpu.VMEM((2, 2, n, cown, jrows, lanes), bf16),
                pltpu.VMEM((2, 2, n, cown, jrows, lanes), bf16),
                pltpu.VMEM((rows, cols), f32),
                pltpu.VMEM((chan, odim * odim), bf16),
                pltpu.VMEM((2, 5 * chan, chan), bf16),
                pltpu.VMEM((2, chan, chan), bf16),
                pltpu.VMEM((2, 4, chan, lanes), f32),
                pltpu.VMEM((chan, lanes), f32),
                dma((10,)), dma((depth // 32,)), dma((1,)), dma((4,)),
                dma((chunks, 2, 8)), dma((chunks, 2, n)), dma((chunks, 2, 2)),
                dma((2, 2, 2, 2, 4)), dma((2, 2, 2, 2, 4)), dma((2, 2, 4)), dma((2, 2, 4)),
                dma((2, 2, 2, 2, n)), dma((2, 2, 2, 2, n)), dma((2, 2, 2, n)), dma((2, 2, 2, n)),
            ],
            compiler_params=pltpu.CompilerParams(collective_id=0, has_side_effects=True, vmem_limit_bytes=67043328),
            name="pair_stack",
        )(pair_loc.reshape(block), mask_loc, msa_loc, *smalls[1:])
        return _carry(out).reshape(pair_loc.shape)

    return jax.shard_map(local_program, mesh=mesh, in_specs=(row_spec, mask_spec, msa_spec) + (replicated,) * 9, out_specs=row_spec, check_vma=False)
```

```python
import functools

import jax
import jax.numpy as jnp
from jax import lax
from jax.experimental import pallas as pl
from jax.experimental.pallas import tpu as pltpu
from jax.sharding import PartitionSpec as P

LN_EPS = 1e-5
LANES = 128
TILE = 16
MESH = pl.DeviceIdType.MESH


def _norm_rows(v, scale, shift):
    mean = jnp.mean(v, axis=0, keepdims=True)
    cen = v - mean
    var = jnp.mean(cen * cen, axis=0, keepdims=True)
    return (cen * lax.rsqrt(var + LN_EPS) * scale + shift).astype(jnp.bfloat16)


def _column(row, n):
    return jnp.broadcast_to(row, (n, row.shape[1])).T


def _kernel(n, z_hbm, mask_hbm, msa_hbm, onrm_hbm, oproj_hbm, oout_hbm, obias_hbm, nrm_hbm, proj_hbm, gate_hbm, xnrm_hbm, out_hbm, o_hbm,
            mask_ref, onrm_ref, oproj_ref, oout_ref, obias_ref, nrm_ref, proj_ref, gate_ref, xnrm_ref, out_ref,
            mb, fb, at_b, ball, obuf, zi, zb, gb, st, snd, ra, rb, xs, xr, mk, wt, wa, wo, nc, bc,
            wsem, msem, zsem, osem, ss, rs, rf, ss_o, rs_o, ss_xo, rs_xo, ss_ab, rs_ab, ss_x, rs_x):
    me = lax.axis_index("dap")
    depth, _, mdim = mb.shape
    rows, chan, cols = zb.shape
    chunks, lanes, jrows, odim = 2, cols // 2, rows // 2, ball.shape[3]
    grp = 8
    per = jrows // grp
    mblocks = msem.shape[0]
    qh = odim // 2
    cown = chan // n
    blocks = odim // 2
    bst, pst, pxt = odim + 8, chan + 8, jrows + 8
    part = me + 1 - 2 * lax.rem(me, 2)
    right, left, opp = lax.rem(me + 2, n), lax.rem(me + n - 2, n), lax.rem(me + 4, n)

    def mcopy(g):
        at = pl.ds(g * (depth // mblocks), depth // mblocks)
        return pltpu.make_async_copy(msa_hbm.at[at], mb.at[at], msem.at[g])

    smalls = [pltpu.make_async_copy(a, b, wsem.at[k]) for k, (a, b) in enumerate((
        (onrm_hbm, onrm_ref), (oproj_hbm, oproj_ref), (mask_hbm, mask_ref), (oout_hbm, oout_ref), (obias_hbm, obias_ref),
        (nrm_hbm, nrm_ref), (proj_hbm, proj_ref), (gate_hbm, gate_ref), (xnrm_hbm, xnrm_ref), (out_hbm, out_ref)))]
    for copy in smalls[:2]:
        copy.start()
    for g in range(mblocks):
        mcopy(g).start()
    for copy in smalls[2:]:
        copy.start()
    zcopy = pltpu.make_async_copy(z_hbm, zi, zsem.at[0])
    barrier = pltpu.get_barrier_semaphore()
    for s in range(1, n):
        pl.semaphore_signal(barrier, inc=1, device_id={"dap": lax.rem(me + s, n)}, device_id_type=MESH)
    for copy in smalls[:2]:
        copy.wait()

    def slot(c, dev):
        return lax.rem(dev + c * (n // 2), n)

    def turned(v, c):
        return v if c == 0 else jnp.concatenate([v[n // 2:], v[:n // 2]], axis=0)

    def block(c, h, src):
        return ball.at[c, h, slot(c, src)]

    def send(c, h, src, k, dst):
        return pltpu.make_async_remote_copy(
            src_ref=block(c, h, src), dst_ref=block(c, h, src), send_sem=ss.at[c, h, k], recv_sem=rs.at[c, h, src],
            device_id={"dap": dst}, device_id_type=MESH)

    def arrived(c, h, src):
        send(c, h, src, 0, part).wait_recv()

    def far(c, h, src, k, dst):
        at = ball.at[c, h, slot(c, src), k * qh:(k + 1) * qh]
        return pltpu.make_async_remote_copy(
            src_ref=at, dst_ref=at, send_sem=ss.at[c, h, 6 + k], recv_sem=rf.at[c, h, k],
            device_id={"dap": dst}, device_id_type=MESH)

    oscale, oshift = onrm_ref[0:1, :], onrm_ref[1:2, :]
    sb = 32
    hdep = depth // 2
    tiles = hdep // LANES

    def project(c, h):
        section = hdep * grp
        @pl.loop(0, hdep // sb)
        def _(b):
            if c == 0:
                mcopy(h * (hdep // sb) + b).wait()
            x = mb[pl.ds(h * hdep + b * sb, sb), c * jrows:(c + 1) * jrows].astype(jnp.float32).reshape(sb * jrows, mdim)
            mean = jnp.mean(x, axis=1, keepdims=True)
            cen = x - mean
            var = jnp.mean(cen * cen, axis=1, keepdims=True)
            y = (cen * lax.rsqrt(var + LN_EPS) * oscale + oshift).astype(jnp.bfloat16)
            v = lax.dot_general(y, oproj_ref[...], (((1,), (1,)), ((), ())), preferred_element_type=jnp.float32)
            v = v.reshape(sb, per, grp, 2 * odim)
            for k in range(per):
                at = pl.ds(pl.multiple_of(k * section + b * (sb * grp), sb * grp), sb * grp)
                fb[at, :2 * odim] = v[:, k].reshape(sb * grp, 2 * odim)

        for k in range(per):
            @pl.loop(0, grp)
            def _(i, k=k):
                v = fb[pl.ds(k * section + i, hdep, stride=grp), :].T
                r = (c * per + k) * grp + i
                at_b[pl.ds(pl.multiple_of(r * odim, odim), odim), h * hdep:(h + 1) * hdep] = v[:odim].astype(jnp.bfloat16)
                for t in range(tiles):
                    row = pl.multiple_of(t * (jrows * bst) + (k * grp + i) * bst, 8)
                    st[pl.ds(row, odim), :] = v[odim:2 * odim, t * LANES:(t + 1) * LANES]

        @pl.loop(0, odim, unroll=4)
        def _(q):
            for t in range(tiles):
                ball[c, h, slot(c, me), q, :, t * LANES:(t + 1) * LANES] = (
                    st[pl.ds(t * (jrows * bst) + q, jrows, stride=bst), :].astype(jnp.bfloat16))

    def send_own(c, h):
        for k, dst in enumerate((right, left, part)):
            send(c, h, me, k, dst).start()

    def forward_far(c, h):
        for k, (src, dst) in enumerate(((left, right), (right, left))):
            arrived(c, h, src)
            far(c, h, src, k, dst).start()
            send(c, h, src, 3 + k, part).start()

    def forward_opp(c):
        for h in (0, 1):
            for k in (0, 1):
                far(c, h, opp, k, part).wait_recv()
            send(c, h, opp, 5, part).start()

    def partner_all(c):
        for d in (0, 2, 4, 6):
            for h in (0, 1):
                arrived(c, h, lax.rem(part + d, n))

    def outer(c, lo, hi, r0=0, nr=rows):
        @pl.loop(lo, hi)
        def _(b):
            rhs = jnp.concatenate([jnp.concatenate([ball[c, h, :, b * 2 + t].reshape(lanes, hdep) for h in range(2)], axis=1) for t in range(2)], axis=0)
            o = lax.dot_general(at_b[r0 * odim:(r0 + nr) * odim], rhs, (((1,), (1,)), ((), ())), preferred_element_type=jnp.float32)
            o = (o * (1.0 / depth)).astype(jnp.bfloat16)
            nt, w = rows * odim // TILE, odim // TILE
            for t in range(2):
                obuf[b, t * nt + r0 * w:t * nt + (r0 + nr) * w] = o[:, t * lanes:(t + 1) * lanes].reshape(nr * w, TILE, lanes)

    def mix(c, lo, hi):
        @pl.loop(lo, hi, unroll=2)
        def _(i):
            nt, w = rows * odim // TILE, odim // TILE
            rhs = jnp.stack([obuf[:, pl.ds(t * nt + i * w, w)] for t in range(2)], axis=1).reshape(odim * odim, lanes)
            upd = jnp.dot(wt[...], rhs, preferred_element_type=jnp.float32)
            zt = turned(zi[i, :, c], c).reshape(lanes, chan).T
            zb[i, :, c * lanes:(c + 1) * lanes] = zt + (upd + bc[...])

    def prepare():
        for copy in smalls[2:]:
            copy.wait()
        rid = lax.broadcasted_iota(jnp.int32, (cols, cols), 0)
        cid = lax.broadcasted_iota(jnp.int32, (cols, cols), 1)
        two = chunks * jrows
        piece = (rid // jrows) % chunks
        place = piece * lanes + ((rid // two + piece * (n // 2)) % n) * jrows + rid % jrows
        perm = (cid == place).astype(jnp.float32).astype(jnp.bfloat16)
        mk[...] = jnp.dot(mask_ref[...].astype(jnp.float32).astype(jnp.bfloat16), perm, preferred_element_type=jnp.float32)
        bc[...] = _column(obias_ref[...], lanes)
        for t in range(2):
            for k in range(2):
                nc[t, k] = _column(nrm_ref[t, k:k + 1, :], lanes)
                nc[t, 2 + k] = _column(xnrm_ref[t, k:k + 1, :], lanes)
            for k in range(4):
                wa[t, k * chan:(k + 1) * chan] = proj_ref[t, :, k * chan:(k + 1) * chan].astype(jnp.float32).T.astype(jnp.bfloat16)
            wa[t, 4 * chan:] = gate_ref[t].astype(jnp.float32).T.astype(jnp.bfloat16)
            wo[t] = out_ref[t].astype(jnp.float32).T.astype(jnp.bfloat16)
        fb[:odim * odim, :] = oout_ref[...].astype(jnp.float32)

        @pl.loop(0, odim * odim // LANES)
        def _(b):
            m = LANES // odim
            v = jnp.concatenate([fb[pl.ds(b * m + k, odim, stride=odim), :] for k in range(m)], axis=0)
            wt[:, pl.ds(pl.multiple_of(b * LANES, LANES), LANES)] = v.T.astype(jnp.bfloat16)

    def piece_rows(u, steps, pieces):
        @pl.loop(0, steps)
        def _(i):
            at = [(r0 + i, h * lanes) for r0, h, _, _ in pieces]
            z = jnp.concatenate([zb[r, :, h:h + lanes] for r, h in at], axis=1)
            m = jnp.concatenate([mk[pl.ds(r, 1), :][:, h:h + lanes] for r, h in at], axis=1)
            scale = jnp.concatenate([nc[u, 0]] * 2, axis=1)
            shift = jnp.concatenate([nc[u, 1]] * 2, axis=1)
            q = jnp.dot(wa[u], _norm_rows(z, scale, shift), preferred_element_type=jnp.float32)
            ab = (m * jax.nn.sigmoid(q[chan:2 * chan]) * q[:chan], m * jax.nn.sigmoid(q[3 * chan:4 * chan]) * q[2 * chan:3 * chan])
            g = jax.nn.sigmoid(q[4 * chan:])
            for s, (r, h) in enumerate(at):
                gb[r, :, h:h + lanes] = g[:, s * lanes:(s + 1) * lanes]
                for t in range(2):
                    row = pl.multiple_of((t * 2 + pieces[s][2]) * (jrows * pst) + (i + pieces[s][3]) * pst, 8)
                    st[pl.ds(row, chan), :] = ab[t][:, s * lanes:(s + 1) * lanes]

    def turn(p, which=(0, 1)):
        @pl.loop(0, chan, unroll=8)
        def _(c):
            for t in range(2):
                for s in which:
                    snd[t, p, s, c] = st[pl.ds((t * 2 + s) * (jrows * pst) + c, jrows, stride=pst), :].astype(jnp.bfloat16)

    own = pl.ds(pl.multiple_of(me * cown, cown), cown)

    chip, core = me // 2, lax.rem(me, 2)
    first, second = chip + 1 - 2 * lax.rem(chip, 2), n // 2 - 1 - chip
    gchan, cslice = chan // 2, chan // 4
    sides = (lax.rem((chip + 1) // 2, 2), chip // 2)

    def mate(t, g):
        return first if t == g else second

    def o_copy(t, p, s, g, far, src_core, dst_core, sending):
        other = 2 * (mate(t, g) if far else chip) + (dst_core if sending else src_core)
        src = me if sending else other
        buf = rb if t else ra
        k = (2 if far else 0)
        return pltpu.make_async_remote_copy(
            src_ref=snd.at[t, p, s, pl.ds(pl.multiple_of(g * gchan + (dst_core if sending else core) * cslice, cslice), cslice)],
            dst_ref=buf.at[g, p, slot(s, src)],
            send_sem=ss_o.at[t, p, s, g, k + (dst_core if sending else 0)], recv_sem=rs_o.at[t, p, s, g, k + (core if sending else src_core)],
            device_id={"dap": other}, device_id_type=MESH)

    def o_send(t, p, s):
        for g in range(2):
            for c in range(2):
                o_copy(t, p, s, g, True, core, c, True).start()
            o_copy(t, p, s, g, False, core, 1 - core, True).start()
            buf = rb if t else ra
            buf[g, p, slot(s, me)] = snd[t, p, s, pl.ds(pl.multiple_of(g * gchan + core * cslice, cslice), cslice)]

    def o_wait(t, p, s):
        for g in range(2):
            o_copy(t, p, s, g, False, 1 - core, core, False).wait_recv()
            for c in range(2):
                o_copy(t, p, s, g, True, c, core, False).wait_recv()

    def o_sent():
        for t in range(2):
            for p in range(2):
                for s in range(2):
                    for g in range(2):
                        for c in range(2):
                            o_copy(t, p, s, g, True, core, c, True).wait_send()
                        o_copy(t, p, s, g, False, core, 1 - core, True).wait_send()

    def xo_copy(p, g, far, src_core, dst_core, sending):
        other = 2 * (mate(0, g) if far else chip) + (dst_core if sending else src_core)
        dst = other if sending else me
        k = 2 if far else 0
        return pltpu.make_async_remote_copy(
            src_ref=xs.at[g, :, slot(p, dst)],
            dst_ref=xr.at[p, sides[g], pl.ds((g * 2 + (core if sending else src_core)) * 2, 2)],
            send_sem=ss_xo.at[p, g, k + (dst_core if sending else 0)], recv_sem=rs_xo.at[p, g, k + (core if sending else src_core)],
            device_id={"dap": other}, device_id_type=MESH)

    def xo_send(p):
        for g in range(2):
            for c in range(2):
                xo_copy(p, g, True, core, c, True).start()
            xo_copy(p, g, False, core, 1 - core, True).start()
            xr[p, sides[g], pl.ds((g * 2 + core) * 2, 2)] = xs[g, :, slot(p, me)]

    def xo_wait(p):
        for g in range(2):
            xo_copy(p, g, False, 1 - core, core, False).wait_recv()
            for c in range(2):
                xo_copy(p, g, True, c, core, False).wait_recv()

    def xo_sent():
        for p in range(2):
            for g in range(2):
                for c in range(2):
                    xo_copy(p, g, True, core, c, True).wait_send()
                xo_copy(p, g, False, core, 1 - core, True).wait_send()

    def x_out(p):
        for g in range(2):
            at = [slot(p, 2 * w + c) for w in (chip, mate(0, g)) for c in range(2)]
            for e in range(cslice // cown):
                @pl.loop(0, cown, unroll=2)
                def _(c, g=g, e=e, at=at):
                    k = e * cown + c
                    a = jnp.concatenate([jnp.concatenate([ra[g, h, d, k] for d in at], axis=0) for h in range(2)], axis=1)
                    b = jnp.concatenate([rb[g, h, :, k].reshape(lanes, lanes) for h in range(2)], axis=1)
                    x = lax.dot_general(a, b, (((1,), (1,)), ((), ())), preferred_element_type=jnp.float32).astype(jnp.bfloat16)
                    for m, d in enumerate(at):
                        xs[g, e, d, c] = x[m * jrows:(m + 1) * jrows]

    def parts(p):
        return ((0, cown),) if p == 0 else ((0, cown // 2), (cown // 2, cown // 2))

    def landing(t, p, s, src, e):
        lo, m = parts(p)[e]
        return obuf.at[t * 4 + p * 2 + s, pl.ds(pl.multiple_of(src * cown, cown) + lo, m)]

    def ab_copy(t, p, s, e, src, dst):
        lo, m = parts(p)[e]
        return pltpu.make_async_remote_copy(
            src_ref=snd.at[t, p, s, pl.ds(pl.multiple_of(dst * cown, cown) + lo, m)], dst_ref=landing(t, p, s, src, e),
            send_sem=ss_ab.at[t, p, s, e, dst], recv_sem=rs_ab.at[t, p, s, e, src],
            device_id={"dap": dst}, device_id_type=MESH)

    def ab_send(p, e, which=(0, 1)):
        lo, m = parts(p)[e]
        for s in which:
            for t in range(2):
                for d in range(1, n):
                    ab_copy(t, p, s, e, me, lax.rem(me + d, n)).start()
                obuf[t * 4 + p * 2 + s, pl.ds(pl.multiple_of(me * cown, cown) + lo, m)] = snd[t, p, s, pl.ds(pl.multiple_of(me * cown, cown) + lo, m)]

    def ab_wait(p, e):
        for t in range(2):
            for s in range(2):
                for d in range(1, n):
                    ab_copy(t, p, s, e, lax.rem(me + d, n), me).wait_recv()

    def ab_sent():
        for p in range(2):
            for e in range(len(parts(p))):
                for t in range(2):
                    for s in range(2):
                        for d in range(1, n):
                            ab_copy(t, p, s, e, me, lax.rem(me + d, n)).wait_send()

    hown = cown // 2

    def x_copy(p, e, h, src, dst):
        at = pl.ds(e * hown, hown)
        return pltpu.make_async_remote_copy(
            src_ref=xs.at[p, h, dst, at], dst_ref=xr.at[p, h, src, at],
            send_sem=ss_x.at[p, e, h, dst], recv_sem=rs_x.at[p, e, h, src],
            device_id={"dap": dst}, device_id_type=MESH)

    def x_send(p, e):
        for h in range(2):
            for d in range(1, n):
                x_copy(p, e, h, me, lax.rem(me + d, n)).start()
        at = slice(e * hown, (e + 1) * hown)
        xr[p, :, me, at] = xs[p, :, me, at]

    def x_wait(p, h):
        for e in range(2):
            for d in range(1, n):
                x_copy(p, e, h, lax.rem(me + d, n), me).wait_recv()

    def x_sent():
        for p in range(2):
            for e in range(2):
                for h in range(2):
                    for d in range(1, n):
                        x_copy(p, e, h, me, lax.rem(me + d, n)).wait_send()

    def x_in(e):
        @pl.loop(e * hown, (e + 1) * hown)
        def _(c):
            a, b = (jnp.concatenate([
                jnp.concatenate([obuf[t * 4 + p * 2 + s, src * cown + c] for p in range(2) for src in range(n)], axis=0)
                for s in range(2)], axis=1) for t in range(2))
            x = lax.dot_general(a, b, (((0,), (0,)), ((), ())), preferred_element_type=jnp.float32)
            x = x.astype(jnp.bfloat16).reshape(2, n, jrows, cols)
            for p in range(2):
                v = turned(x[p], p)
                for h in range(2):
                    xs[p, h, :, c] = v[:, :, h * lanes:(h + 1) * lanes]

    half = chan * pxt

    def stage(u, p, which=(0, 1)):
        lane = lax.broadcasted_iota(jnp.int32, (jrows, lanes), 1) // (lanes // 4)
        for k in range(n):
            take = ((lane == 0) | (lane == 3)) if k < n // 2 else (lane < 2)

            @pl.loop(0, cown, unroll=8)
            def _(c, k=k, take=take):
                x = [xr[p, h, k, c].astype(jnp.float32) for h in which]
                if u == 0:
                    x = [jnp.where(take, x[0], x[1]), jnp.where(take, x[1], x[0])]
                for h, x in zip(which, x):
                    fb[pl.ds(pl.multiple_of(h * half + (k * cown + c) * pxt, 8), jrows), :] = x

    def finish(u, p, steps, pieces):
        @pl.loop(0, steps)
        def _(i):
            at = [(p * jrows + r0 + i, h * lanes) for r0, h in pieces]
            x = jnp.concatenate([fb[pl.ds(h * half + r0 + i, chan, stride=pxt), :] for r0, h in pieces], axis=1)
            xscale = jnp.concatenate([nc[u, 2]] * 2, axis=1)
            xshift = jnp.concatenate([nc[u, 3]] * 2, axis=1)
            upd = jnp.dot(wo[u], _norm_rows(x, xscale, xshift), preferred_element_type=jnp.float32)
            new = [zb[r, :, h:h + lanes] + gb[r, :, h:h + lanes] * upd[:, k * lanes:(k + 1) * lanes] for k, (r, h) in enumerate(at)]
            if u == 0:
                for (r, h), v in zip(at, new):
                    zb[r, :, h:h + lanes] = v
            else:
                for (r, h), v in zip(at, new):
                    c = h // lanes
                    zi[r, :, c] = turned(v.T.reshape(n, jrows, chan), c)

    def ocopy(p, h):
        at = pl.ds(p * jrows, jrows)
        return pltpu.make_async_copy(zi.at[at, :, h], o_hbm.at[at, :, h], osem.at[p * 2 + h])

    project(0, 0)
    pl.semaphore_wait(barrier, n - 1)
    send_own(0, 0)
    project(0, 1)
    send_own(0, 1)
    zcopy.start()
    project(1, 0)
    forward_far(0, 0)
    project(1, 1)
    prepare()
    forward_far(0, 1)
    send_own(1, 0)
    send_own(1, 1)
    forward_opp(0)
    partner_all(0)
    outer(0, 0, blocks * 3 // 8)
    forward_far(1, 0)
    outer(0, blocks * 3 // 8, blocks)
    zcopy.wait()
    hr = jrows // 2
    for s in range(2):
        mix(0, s * jrows, (s + 1) * jrows)
        if s == 0:
            forward_far(1, 1)
        piece_rows(0, hr, ((s * jrows, 0, s, 0), (s * jrows + hr, 0, s, hr)))
        turn(0, (s,))
        for t in (1, 0):
            o_send(t, 0, s)
    forward_opp(1)
    partner_all(1)
    for s in range(2):
        outer(1, 0, blocks, s * jrows, jrows)
        mix(1, s * jrows, (s + 1) * jrows)
        piece_rows(0, hr, ((s * jrows, 1, s, 0), (s * jrows + hr, 1, s, hr)))
        turn(1, (s,))
        for t in (1, 0):
            o_send(t, 1, s)
    for p in range(2):
        for s in range(2):
            o_wait(1, p, s)
    for p in range(2):
        o_wait(0, 0, p)
        o_wait(0, 1, p)
        x_out(p)
        xo_send(p)
    o_sent()
    for p in range(2):
        xo_wait(p)
        stage(0, p)
        for h in range(2):
            finish(0, p, hr, ((0, h), (hr, h)))
            piece_rows(1, hr, ((p * jrows, h, h, 0), (p * jrows + hr, h, h, hr)))
            turn(p, (h,))
            if p == 0:
                ab_send(0, 0, (h,))
    for e in range(2):
        ab_send(1, e)
    xo_sent()
    ab_wait(0, 0)
    for e in range(2):
        ab_wait(1, e)
        x_in(e)
        for p in range(2):
            x_send(p, e)
    for p in range(2):
        for h in range(2):
            x_wait(p, h)
            stage(1, p, (h,))
            finish(1, p, hr, ((0, h), (hr, h)))
            ocopy(p, h).start()
    for p in range(2):
        for h in range(2):
            ocopy(p, h).wait()
    ab_sent()
    x_sent()
    for c in range(chunks):
        for h in (0, 1):
            for k, src in enumerate((me, me, me, left, right, opp)):
                send(c, h, src, k, part).wait_send()
            far(c, h, left, 0, right).wait_send()
            far(c, h, right, 1, left).wait_send()


def _carry_kernel(src_hbm, dst_hbm, buf, in_sem, out_sem):
    pieces = in_sem.shape[0]
    step = buf.shape[0] // pieces
    at = [pl.ds(k * step, step) for k in range(pieces)]
    reads = [pltpu.make_async_copy(src_hbm.at[a], buf.at[a], in_sem.at[k]) for k, a in enumerate(at)]
    writes = [pltpu.make_async_copy(buf.at[a], dst_hbm.at[a], out_sem.at[k]) for k, a in enumerate(at)]
    for copy in reads:
        copy.start()
    for read, write in zip(reads, writes):
        read.wait()
        write.start()
    for copy in writes:
        copy.wait()


def _carry(v):
    hbm = pl.BlockSpec(memory_space=pl.ANY)
    pieces = 16
    return pl.pallas_call(
        _carry_kernel,
        out_shape=jax.ShapeDtypeStruct(v.shape, v.dtype),
        in_specs=[hbm],
        out_specs=hbm,
        scratch_shapes=[pltpu.VMEM(v.shape, v.dtype), pltpu.SemaphoreType.DMA((pieces,)), pltpu.SemaphoreType.DMA((pieces,))],
        compiler_params=pltpu.CompilerParams(vmem_limit_bytes=60 * 1024 * 1024),
        name="carry",
    )(v)


def solution(mesh):
    row_spec = P(("data", "dap"), None, None)
    mask_spec = P(("data", "dap"), None)
    msa_spec = P(None, ("data", "dap"), None)
    replicated = P()

    def local_program(pair_loc, mask_loc, msa_loc, opm_norm, opm_proj, opm_out, opm_bias, tri_norm, tri_proj, tri_gate, tri_xnorm, tri_out):
        n = lax.axis_size("dap")
        rows, cols, chan = pair_loc.shape
        depth, _, mdim = msa_loc.shape
        odim = opm_proj.shape[1] // 2
        chunks = 2
        lanes = cols // chunks
        jrows = rows // chunks
        cown = chan // n
        hbm = pl.BlockSpec(memory_space=pl.ANY)
        f32, bf16 = jnp.float32, jnp.bfloat16
        dma = pltpu.SemaphoreType.DMA
        staged = max(4 * jrows * (chan + 8), depth // LANES * jrows * (odim + 8))
        block = (rows, n, chunks, jrows, chan)
        smalls = (mask_loc, opm_norm, opm_proj.T, opm_out, opm_bias.reshape(1, chan), tri_norm, tri_proj, tri_gate, tri_xnorm, tri_out)
        out = pl.pallas_call(
            functools.partial(_kernel, n),
            out_shape=jax.ShapeDtypeStruct(block, f32),
            in_specs=[hbm] * 12,
            out_specs=hbm,
            scratch_shapes=[pltpu.VMEM(a.shape, a.dtype) for a in smalls] + [
                pltpu.VMEM((depth, rows, mdim), bf16),
                pltpu.VMEM((max(depth // 2 * jrows, 2 * chan * (jrows + 8)), LANES), f32),
                pltpu.VMEM((rows * odim, depth), bf16),
                pltpu.VMEM((chunks, 2, n, odim, jrows, depth // 2), bf16),
                pltpu.VMEM((odim // 2, 2 * rows * odim // TILE, TILE, lanes), bf16),
                pltpu.VMEM(block, f32),
                pltpu.VMEM((rows, chan, cols), f32),
                pltpu.VMEM((rows, chan, cols), f32),
                pltpu.VMEM((staged, LANES), f32),
                pltpu.VMEM((2, 2, 2, chan, jrows, lanes), bf16),
                pltpu.VMEM((2, 2, n, chan // 4, jrows, lanes), bf16),
                pltpu.VMEM((2, 2, n, chan // 4, jrows, lanes), bf16),
                pltpu.VMEM((2, 2, n, cown, jrows, lanes), bf16),
                pltpu.VMEM((2, 2, n, cown, jrows, lanes), bf16),
                pltpu.VMEM((rows, cols), f32),
                pltpu.VMEM((chan, odim * odim), bf16),
                pltpu.VMEM((2, 5 * chan, chan), bf16),
                pltpu.VMEM((2, chan, chan), bf16),
                pltpu.VMEM((2, 4, chan, lanes), f32),
                pltpu.VMEM((chan, lanes), f32),
                dma((10,)), dma((depth // 32,)), dma((1,)), dma((4,)),
                dma((chunks, 2, 8)), dma((chunks, 2, n)), dma((chunks, 2, 2)),
                dma((2, 2, 2, 2, 4)), dma((2, 2, 2, 2, 4)), dma((2, 2, 4)), dma((2, 2, 4)),
                dma((2, 2, 2, 2, n)), dma((2, 2, 2, 2, n)), dma((2, 2, 2, n)), dma((2, 2, 2, n)),
            ],
            compiler_params=pltpu.CompilerParams(collective_id=0, has_side_effects=True, vmem_limit_bytes=67043328),
            name="pair_stack",
        )(pair_loc.reshape(block), mask_loc, msa_loc, *smalls[1:])
        return _carry(out).reshape(pair_loc.shape)

    return jax.shard_map(local_program, mesh=mesh, in_specs=(row_spec, mask_spec, msa_spec) + (replicated,) * 9, out_specs=row_spec, check_vma=False)
```
